8 devices in a mesh: dp: 1 (over z), ey: 2 (over y), ex: 2 (over x), ec: 2 (over core).
Axes of the slice: x: 2, y: 2, z: 1, core: 2. Of those that a mesh axis runs over, the one named last changes fastest.
Arguments:
- x: bfloat16 [2048, 2048], P(('dp', 'ey', 'ex', 'ec'))
- ids: int32 [2048, 6], P(('dp', 'ey', 'ex', 'ec'))
- gates: float32 [2048, 6], P(('dp', 'ey', 'ex', 'ec'))
- w1: bfloat16 [64, 2048, 1408], P(('ey', 'ex', 'ec'))
- w3: bfloat16 [64, 2048, 1408], P(('ey', 'ex', 'ec'))
- w2: bfloat16 [64, 1408, 2048], P(('ey', 'ex', 'ec'))
- ws1: bfloat16 [2048, 2816], replicated
- ws3: bfloat16 [2048, 2816], replicated
- ws2: bfloat16 [2816, 2048], replicated
Outputs:
- output: bfloat16 [2048, 2048], P(('dp', 'ey', 'ex', 'ec'))
All inputs are finite; a program needn't handle non-finite values.
Results may differ from the reference program's by a relative error of at most 0.00579921.
Values are sent between devices in bfloat16 or wider.
A program may use at most 1 GiB of HBM per device.

```python
import jax
import jax.numpy as jnp
from jax import lax

DEVS = 8
T = 256
H = 2048
F = 1408
E = 64
TOP = 6
NG = 1
TOPG = 1
FS = 2816

CAP = min(T, 2 * ((T * TOP + E - 1) // E))
EG = E // NG
KG = TOP // TOPG


def route_ids(kgrp, kexp, ktok, kslot, wheel):
    gperm = jnp.argsort(jax.random.uniform(kgrp, (DEVS, NG)), axis=-1)
    q = jnp.arange(T * TOPG)
    grp = gperm[:, q % NG]
    slot = ((q // NG)[:, None] * KG + jnp.arange(KG)[None, :]) % wheel
    eperm = jnp.argsort(jax.random.uniform(kexp, (DEVS, NG, EG)), axis=-1)
    rows = eperm[jnp.arange(DEVS)[:, None], grp]
    loc = jnp.take_along_axis(rows, jnp.broadcast_to(slot[None], (DEVS, T * TOPG, KG)), axis=2)
    ids = (grp[:, :, None] * EG + loc).reshape(DEVS, T, TOP)
    tperm = jnp.argsort(jax.random.uniform(ktok, (DEVS, T)), axis=-1)
    ids = jnp.take_along_axis(ids, jnp.broadcast_to(tperm[:, :, None], (DEVS, T, TOP)), axis=1)
    sperm = jnp.argsort(jax.random.uniform(kslot, (DEVS, T, TOP)), axis=-1)
    ids = jnp.take_along_axis(ids, sperm, axis=2)
    return ids.reshape(DEVS * T, TOP).astype(jnp.int32)


def setup_inputs(seed: int = 0, part: int = 0) -> dict:
    key = jax.random.fold_in(jax.random.key(seed), part)
    kx, kg, kgr, kex, ktk, ksl = jax.random.split(key, 6)
    wk = jax.random.split(jax.random.key(seed + 1), 6)
    x = jax.random.normal(kx, (DEVS * T, H), jnp.float32).astype(jnp.bfloat16)
    ids = route_ids(kgr, kex, ktk, ksl, EG)
    u = jax.random.uniform(kg, (DEVS * T, TOP), jnp.float32, 0.5, 1.5)
    gates = u / jnp.sum(u, axis=1, keepdims=True)
    w1 = (jax.random.normal(wk[0], (E, H, F), jnp.float32) * H ** -0.5).astype(jnp.bfloat16)
    w3 = (jax.random.normal(wk[1], (E, H, F), jnp.float32) * H ** -0.5).astype(jnp.bfloat16)
    w2 = (jax.random.normal(wk[2], (E, F, H), jnp.float32) * (2.0 * F ** -0.5)).astype(jnp.bfloat16)
    ws1 = (jax.random.normal(wk[3], (H, FS), jnp.float32) * H ** -0.5).astype(jnp.bfloat16)
    ws3 = (jax.random.normal(wk[4], (H, FS), jnp.float32) * H ** -0.5).astype(jnp.bfloat16)
    ws2 = (jax.random.normal(wk[5], (FS, H), jnp.float32) * FS ** -0.5).astype(jnp.bfloat16)
    return dict(x=x, ids=ids, gates=gates, w1=w1, w3=w3, w2=w2, ws1=ws1, ws3=ws3, ws2=ws2)


def reference(x, ids, gates, w1, w3, w2, ws1, ws3, ws2):
    n = x.shape[0]
    m = n * TOP
    flat = ids.reshape(m)
    gflat = gates.reshape(m)
    capp = DEVS * CAP

    def body(acc, inp):
        w1e, w3e, w2e, e = inp
        sel = jnp.nonzero(flat == e, size=capp, fill_value=m)[0]
        valid = sel < m
        idx = jnp.minimum(sel, m - 1)
        tok = idx // TOP
        u = x[tok]
        a = jnp.dot(u, w1e, preferred_element_type=jnp.float32)
        b = jnp.dot(u, w3e, preferred_element_type=jnp.float32)
        h = (jax.nn.silu(a) * b).astype(jnp.bfloat16)
        o = jnp.dot(h, w2e, preferred_element_type=jnp.float32).astype(jnp.bfloat16)
        wgt = jnp.where(valid, gflat[idx], 0.0)
        return acc.at[tok].add(wgt[:, None] * o.astype(jnp.float32)), None

    acc, _ = lax.scan(body, jnp.zeros((n, H), jnp.float32), (w1, w3, w2, jnp.arange(E)))
    sa = jnp.dot(x, ws1, preferred_element_type=jnp.float32)
    sb = jnp.dot(x, ws3, preferred_element_type=jnp.float32)
    sh = (jax.nn.silu(sa) * sb).astype(jnp.bfloat16)
    s = jnp.dot(sh, ws2, preferred_element_type=jnp.float32).astype(jnp.bfloat16)
    y = x.astype(jnp.float32) + s.astype(jnp.float32) + acc
    return y.astype(jnp.bfloat16)
```

```python
import jax
import jax.numpy as jnp
from jax import lax
from jax.sharding import PartitionSpec as P

EXP = ("ey", "ex", "ec")
ALL = ("dp", "ey", "ex", "ec")


def split3(g):
    g1 = lax.reduce_precision(g, 8, 7)
    r = g - g1
    g2 = lax.reduce_precision(r, 8, 7)
    g3 = r - g2
    return [v.astype(jnp.bfloat16) for v in (g1, g2, g3)]


def solution(mesh):
    pg = mesh.shape["ey"] * mesh.shape["ex"] * mesh.shape["ec"]

    def local(x, ids, gates, w1, w3, w2, ws1, ws3, ws2):
        t, hd = x.shape
        top = ids.shape[1]
        el = w1.shape[0]
        ne = el * pg
        cap = min(t, 2 * ((t * top + ne - 1) // ne))
        me = lax.axis_index(EXP)
        xg = lax.all_gather(x, EXP, axis=0, tiled=True).reshape(pg, t, hd)
        idg = lax.all_gather(ids, EXP, axis=0, tiled=True).reshape(pg, t, top)
        gg = lax.all_gather(gates, EXP, axis=0, tiled=True).reshape(pg, t, top)
        mine = me * el + jnp.arange(el)
        hit = idg[:, :, :, None] == mine
        c = jnp.any(hit, axis=2)
        g = jnp.sum(jnp.where(hit, gg[:, :, :, None], 0.0), axis=2)
        tri = (jnp.arange(t)[None, :] < jnp.arange(t)[:, None]).astype(jnp.bfloat16)
        cnt = jnp.einsum("ab,sbe->sae", tri, c.astype(jnp.bfloat16), preferred_element_type=jnp.float32).astype(jnp.int32)
        sel = (cnt[:, :, :, None] == jnp.arange(cap)) & c[:, :, :, None]
        disp = sel.astype(jnp.bfloat16).reshape(pg, t, el * cap)
        rows = jnp.einsum("std,sth->sdh", disp, xg, preferred_element_type=jnp.float32).astype(jnp.bfloat16)
        recv = rows.reshape(pg, el, cap, hd).transpose(1, 0, 2, 3).reshape(el, pg * cap, hd)
        a = jnp.einsum("erh,ehf->erf", recv, w1, preferred_element_type=jnp.float32)
        b = jnp.einsum("erh,ehf->erf", recv, w3, preferred_element_type=jnp.float32)
        hid = (jax.nn.silu(a) * b).astype(jnp.bfloat16)
        out = jnp.einsum("erf,efh->erh", hid, w2, preferred_element_type=jnp.float32).astype(jnp.bfloat16)
        out = out.reshape(el, pg, cap, hd).transpose(1, 0, 2, 3).reshape(pg, el * cap, hd)
        wg = jnp.where(sel, g[:, :, :, None], 0.0).reshape(pg, t, el * cap)
        part = sum(jnp.einsum("std,sdh->sth", v, out, preferred_element_type=jnp.float32) for v in split3(wg))
        moe = lax.psum_scatter(part.reshape(pg * t, hd), EXP, scatter_dimension=0, tiled=True)
        sa = jnp.dot(x, ws1, preferred_element_type=jnp.float32)
        sb = jnp.dot(x, ws3, preferred_element_type=jnp.float32)
        sh = (jax.nn.silu(sa) * sb).astype(jnp.bfloat16)
        s = jnp.dot(sh, ws2, preferred_element_type=jnp.float32).astype(jnp.bfloat16)
        return (x.astype(jnp.float32) + s.astype(jnp.float32) + moe).astype(jnp.bfloat16)

    return jax.shard_map(local, mesh=mesh,
                         in_specs=(P(ALL), P(ALL), P(ALL), P(EXP), P(EXP), P(EXP), P(), P(), P()),
                         out_specs=P(ALL), check_vma=False)
```

```python
import functools

import jax
import jax.numpy as jnp
from jax import lax
from jax.experimental import pallas as pl
from jax.experimental.pallas import tpu as pltpu
from jax.sharding import PartitionSpec as P

EXP = ("ey", "ex", "ec")
ALL = ("dp", "ey", "ex", "ec")
MESH = pl.DeviceIdType.MESH
ANY = pl.BlockSpec(memory_space=pl.ANY)
VM = pl.BlockSpec(memory_space=pltpu.VMEM)
BF = jnp.bfloat16
F32 = jnp.float32
VLIM = 67043328

NK = 4
NS = 3
CW = 256
NW = 4


def place():
    ey, ex, ec = (lax.axis_index(a) for a in EXP)
    dev = {"x": dict(ey=ey, ex=1 - ex, ec=ec), "y": dict(ey=1 - ey, ex=ex, ec=ec), "p": dict(ey=ey, ex=ex, ec=1 - ec)}
    chip = {"o": ey * 2 + ex, "x": ey * 2 + 1 - ex, "y": (1 - ey) * 2 + ex, "d": (1 - ey) * 2 + 1 - ex}
    return ey, ex, ec, dev, chip


def silu_mul(a, b):
    return (a * jax.nn.sigmoid(a) * b).astype(BF)


def first(el, cap, ids_ref, gates_ref, x_ref, w1_ref, w3_ref, ws1_ref, ws3_ref, h_ref, sh_ref, wc_ref,
          xg, acc, wb, disp, xe, hst, wst, mout, meta,
          xsem, wsem, osem, csem, msend, mrecv, ssem, rsem):
    ey, ex, ec, dev, chip = place()
    t = x_ref.shape[0]
    kw = x_ref.shape[1] // NK
    f = w1_ref.shape[2]
    half = t // 2
    lo, hi, full = pl.ds(0, half), pl.ds(half, half), pl.ds(0, t)
    mine = {c: ec * 4 + chip[c] for c in "oxyd"}
    theirs = {c: (1 - ec) * 4 + chip[c] for c in "oxyd"}
    nsh = 2 * NK
    nb = nsh + NK * el

    def block(b, go):
        slot = lax.rem(b, NS)

        @pl.when(b < nsh)
        def _():
            rows = pl.ds(pl.multiple_of(lax.rem(b, NK) * kw, kw), kw)
            cols = pl.ds(pl.multiple_of((b // NK) * f, 128), f)
            for i, w in enumerate((ws1_ref, ws3_ref)):
                go(pltpu.make_async_copy(w.at[rows, cols], wb.at[slot, :, pl.ds(i * f, f)], wsem.at[slot, i]))

        @pl.when((b >= nsh) & (b < nb))
        def _():
            q = b - nsh
            rows = pl.ds(pl.multiple_of((q // el) * kw, kw), kw)
            for i, w in enumerate((w1_ref, w3_ref)):
                go(pltpu.make_async_copy(w.at[lax.rem(q, el), rows], wb.at[slot, :, pl.ds(i * f, f)], wsem.at[slot, i]))

    def fetch(b):
        block(b, lambda c: c.start())

    def ready(b):
        block(b, lambda c: c.wait())

    for b in range(NS - 1):
        fetch(b)
    for k in range(NK):
        pltpu.make_async_copy(x_ref.at[:, pl.ds(k * kw, kw)], xg.at[k, mine["o"]], xsem.at[k]).start()

    ne = el * 8
    row = lax.broadcasted_iota(jnp.int32, (ne, t), 0)
    chosen = jnp.zeros((ne, t), F32)
    gate = jnp.zeros((ne, t), F32)
    for j in range(6):
        hit = ids_ref[j:j + 1, :] == row
        chosen = jnp.where(hit, 1.0, chosen)
        gate = jnp.where(hit, gates_ref[j:j + 1, :], gate)
    before = (lax.broadcasted_iota(jnp.int32, (t, t), 0) < lax.broadcasted_iota(jnp.int32, (t, t), 1))
    rank = jnp.dot(chosen.astype(BF), before.astype(F32).astype(BF), preferred_element_type=F32)
    rank = jnp.where(chosen > 0.0, rank, -1.0)
    for d in range(8):
        mout[d, 0:el, :] = rank[d * el:(d + 1) * el]
        mout[d, el:2 * el, :] = gate[d * el:(d + 1) * el]

    barrier = pltpu.get_barrier_semaphore()
    others = [(a, b, c) for a in (0, 1) for b in (0, 1) for c in (0, 1) if a + b + c]

    def flip(o):
        return [lax.rem(v + s, 2) for v, s in zip((ey, ex, ec), o)]

    for o in others:
        y2, x2, c2 = flip(o)
        pl.semaphore_signal(barrier, inc=1, device_id=dict(ey=y2, ex=x2, ec=c2), device_id_type=MESH)
    pl.semaphore_wait(barrier, len(others))

    for k in range(NK):
        pltpu.make_async_copy(x_ref.at[:, pl.ds(k * kw, kw)], xg.at[k, mine["o"]], xsem.at[k]).wait()

    def remote(k, src, rows, chan, to):
        ref = xg.at[k, src, rows]
        return pltpu.make_async_remote_copy(ref, ref, ssem.at[k, chan], rsem.at[k, chan], device_id=dev[to],
                                            device_id_type=MESH)

    def direct(k):
        for chan, to in enumerate("xyp"):
            remote(k, mine["o"], full, chan, to).start()

    def relay(k):
        remote(k, mine["x"], full, 0, "x").wait_recv()
        remote(k, mine["x"], lo, 3, "y").start()
        remote(k, mine["x"], full, 5, "p").start()
        remote(k, mine["y"], full, 1, "y").wait_recv()
        remote(k, mine["y"], hi, 4, "x").start()
        remote(k, mine["y"], full, 6, "p").start()

    def corner(k):
        remote(k, mine["d"], lo, 3, "y").wait_recv()
        remote(k, mine["d"], lo, 7, "p").start()
        remote(k, mine["d"], hi, 4, "x").wait_recv()
        remote(k, mine["d"], hi, 8, "p").start()

    def arrived(k):
        remote(k, theirs["o"], full, 2, "p").wait_recv()
        remote(k, theirs["x"], full, 5, "p").wait_recv()
        remote(k, theirs["y"], full, 6, "p").wait_recv()
        remote(k, theirs["d"], lo, 7, "p").wait_recv()
        remote(k, theirs["d"], hi, 8, "p").wait_recv()

    def sent(k):
        for src, rows, chan, to in ((mine["o"], full, 0, "x"), (mine["o"], full, 1, "y"), (mine["o"], full, 2, "p"),
                                    (mine["x"], lo, 3, "y"), (mine["y"], hi, 4, "x"), (mine["x"], full, 5, "p"),
                                    (mine["y"], full, 6, "p"), (mine["d"], lo, 7, "p"), (mine["d"], hi, 8, "p")):
            remote(k, src, rows, chan, to).wait_send()

    def mcopy(o, back=False):
        y2, x2, c2 = flip(o)
        num = c2 * 4 + y2 * 2 + x2
        idx = y2 * 4 + x2 * 2 + c2
        src, dst = (meta.at[num], num) if back else (mout.at[idx], mine["o"])
        return pltpu.make_async_remote_copy(src, meta.at[dst], msend.at[num], mrecv.at[dst],
                                            device_id=dict(ey=y2, ex=x2, ec=c2), device_id_type=MESH)

    for o in others:
        mcopy(o).start()
    direct(0)
    direct(1)

    for hf in range(2):
        acc[0, 0:t, :] = jnp.zeros((t, 2 * f), F32)

        def body(k, _):
            b = hf * NK + k
            fetch(b + NS - 1)
            ready(b)
            acc[0, 0:t, :] += jnp.dot(xg[k, mine["o"]], wb[lax.rem(b, NS)], preferred_element_type=F32)
            return 0

        lax.fori_loop(0, NK, body, 0)
        hst[hf, 0:t, :] = silu_mul(acc[0, 0:t, 0:f], acc[0, 0:t, f:2 * f])
        pltpu.make_async_copy(hst.at[hf, 0:t], sh_ref.at[hf], osem.at[hf]).start()

    relay(0)
    direct(2)

    meta[mine["o"]] = mout[ey * 4 + ex * 2 + ec]
    for o in others:
        mcopy(o, True).wait_recv()
    slots = lax.broadcasted_iota(jnp.int32, (cap, t), 0).astype(F32)

    def build(s, _):
        parts = []
        for e in range(el):
            sel = meta[s, e:e + 1, :] == slots
            disp[s, e * cap:(e + 1) * cap, :] = jnp.where(sel, 1.0, 0.0).astype(BF)
            parts.append(jnp.where(sel, meta[s, el + e:el + e + 1, :], 0.0))
        w = jnp.concatenate(parts, axis=0).T
        n = el * cap
        slot = lax.rem(s, 2)

        @pl.when(s >= 2)
        def _():
            pltpu.make_async_copy(wst.at[slot], wc_ref.at[s - 2], csem.at[slot]).wait()

        for i in range(3):
            p = w.astype(BF)
            wst[slot, :, i * n:(i + 1) * n] = p
            w = w - p.astype(F32)
        pltpu.make_async_copy(wst.at[slot], wc_ref.at[s], csem.at[slot]).start()
        return 0

    lax.fori_loop(0, 8, build, 0)
    relay(1)
    direct(3)

    def gather(k):
        def body(s, _):
            r = jnp.dot(disp[s], xg[k, s], preferred_element_type=F32).astype(BF)
            for e in range(el):
                xe[e, s] = r[e * cap:(e + 1) * cap]
            return 0

        lax.fori_loop(0, 8, body, 0)

    def product(k, e):
        b = nsh + k * el + e
        fetch(b + NS - 1)
        ready(b)
        return jnp.dot(xe[e].reshape(8 * cap, kw), wb[lax.rem(b, NS)], preferred_element_type=F32)

    def start_acc(e, _):
        acc[e] = product(0, e)
        return 0

    corner(0)
    arrived(0)
    gather(0)
    lax.fori_loop(0, el // 2, start_acc, 0)
    relay(2)
    corner(1)
    lax.fori_loop(el // 2, el, start_acc, 0)

    def more(k, _):
        arrived(k)
        gather(k)

        def add(e, _):
            acc[e] += product(k, e)
            return 0

        lax.fori_loop(0, el // 2, add, 0)

        @pl.when(k == 1)
        def _():
            relay(3)
        corner(k + 1)
        lax.fori_loop(el // 2, el, add, 0)
        return 0

    lax.fori_loop(1, NK - 1, more, 0)

    arrived(NK - 1)
    gather(NK - 1)
    for hf in range(2):
        pltpu.make_async_copy(hst.at[hf, 0:t], sh_ref.at[hf], osem.at[hf]).wait()

    def last(e, _):
        slot = lax.rem(e, 2)
        acc[e] += product(NK - 1, e)

        @pl.when(e >= 2)
        def _():
            pltpu.make_async_copy(hst.at[slot], h_ref.at[e - 2], osem.at[slot]).wait()
        hst[slot] = silu_mul(acc[e, :, 0:f], acc[e, :, f:2 * f])
        pltpu.make_async_copy(hst.at[slot], h_ref.at[e], osem.at[slot]).start()
        return 0

    lax.fori_loop(0, el, last, 0)

    for s in (6, 7):
        pltpu.make_async_copy(wst.at[s % 2], wc_ref.at[s], csem.at[s % 2]).wait()
    for e in (el - 2, el - 1):
        pltpu.make_async_copy(hst.at[e % 2], h_ref.at[e], osem.at[e % 2]).wait()
    for o in others:
        mcopy(o).wait_send()
    for k in range(NK):
        sent(k)


def second(el, cap, h_ref, sh_ref, wc_ref, x_ref, w2_ref, ws2_ref, y_ref,
           hv, shv, wcv, xv, wb, o3, part, pr, dr, fr, res, yst,
           hsem, csem, xsem, wsem, ysem, psend, precv, dsend, drecv, fsend, frecv):
    ey, ex, ec, dev, chip = place()
    t, hd = x_ref.shape
    nc = hd // CW
    f = w2_ref.shape[1]
    half = t // 2
    lo, hi = pl.ds(0, half), pl.ds(half, half)
    per = el + 2
    nb = nc * per
    n = el * cap

    def block(b, go):
        c, j = b // per, lax.rem(b, per)
        cols = pl.ds(pl.multiple_of(c * CW, CW), CW)
        slot = lax.rem(b, NW)

        @pl.when((j < el) & (b < nb))
        def _():
            go(pltpu.make_async_copy(w2_ref.at[j, :, cols], wb.at[slot], wsem.at[slot]))

        @pl.when((j >= el) & (b < nb))
        def _():
            rows = pl.ds(pl.multiple_of((j - el) * f, 128), f)
            go(pltpu.make_async_copy(ws2_ref.at[rows, cols], wb.at[slot], wsem.at[slot]))

    def fetch(b):
        block(b, lambda c: c.start())

    def ready(b):
        block(b, lambda c: c.wait())

    def hcopy(e):
        return pltpu.make_async_copy(h_ref.at[e], hv.at[e], hsem.at[e])

    hcopy(0).start()
    for b in range(NW - 1):
        fetch(b)
    for e in range(1, el):
        hcopy(e).start()
    loads = [pltpu.make_async_copy(sh_ref, shv, xsem.at[0]), pltpu.make_async_copy(x_ref, xv, xsem.at[1]),
             pltpu.make_async_copy(wc_ref, wcv, csem)]
    for c in loads:
        c.start()

    barrier = pltpu.get_barrier_semaphore()
    for to in "xyp":
        pl.semaphore_signal(barrier, inc=1, device_id=dev[to], device_id_type=MESH)
    pl.semaphore_wait(barrier, 3)

    def swap(c):
        return pltpu.make_async_remote_copy(part.at[1, c], pr.at[c], psend.at[c], precv.at[c], device_id=dev["p"],
                                            device_id_type=MESH)

    def corner(c, i):
        src = part.at[0, c, chip["d"], (lo, hi)[i]]
        return pltpu.make_async_remote_copy(src, dr.at[c, i], dsend.at[c, i], drecv.at[c, i], device_id=dev["xy"[i]],
                                            device_id_type=MESH)

    def final(c, i, rows):
        src = part.at[0, c, chip["xy"[i]], (lo, hi)[rows]]
        return pltpu.make_async_remote_copy(src, fr.at[c, i, (lo, hi)[rows]], fsend.at[c, i, rows], frecv.at[c, i, rows],
                                            device_id=dev["xy"[i]], device_id_type=MESH)

    def weigh(c, g):
        core = ec if g == 0 else 1 - ec

        def body(ch, _):
            s = core * 4 + ch
            part[g, c, ch] = jnp.dot(wcv[s], o3[s], preferred_element_type=F32)
            return 0

        lax.fori_loop(0, 4, body, 0)

    def compute(c):
        def expert(e, _):
            b = c * per + e
            fetch(b + NW - 1)

            @pl.when(c == 0)
            def _():
                hcopy(e).wait()
            ready(b)
            o = jnp.dot(hv[e], wb[lax.rem(b, NW)], preferred_element_type=F32).astype(BF)
            for s in range(8):
                for i in range(3):
                    o3[s, pl.ds(pl.multiple_of(i * n + e * cap, 16), cap), :] = o[s * cap:(s + 1) * cap]
            return 0

        lax.fori_loop(0, el, expert, 0)

        @pl.when(c == 0)
        def _():
            for d in loads:
                d.wait()
        weigh(c, 1)
        swap(c).start()
        weigh(c, 0)
        s = None
        for i in range(2):
            b = c * per + el + i
            fetch(b + NW - 1)
            ready(b)
            p = jnp.dot(shv[i], wb[lax.rem(b, NW)], preferred_element_type=F32)
            s = p if s is None else s + p
        cols = pl.ds(pl.multiple_of(c * CW, CW), CW)
        res[c] = xv[:, cols].astype(F32) + s.astype(BF).astype(F32)

    def stage1(c):
        swap(c).wait_recv()
        for ch in "dxyo":
            part[0, c, chip[ch]] += pr[c, chip[ch]]
        corner(c, 0).start()
        corner(c, 1).start()
        final(c, 0, 0).start()
        final(c, 1, 1).start()

    def stage2(c):
        corner(c, 0).wait_recv()
        part[0, c, chip["y"], 0:half] += dr[c, 0]
        corner(c, 1).wait_recv()
        part[0, c, chip["x"], half:t] += dr[c, 1]
        final(c, 1, 0).start()
        final(c, 0, 1).start()

    def ycopy(c):
        cols = pl.ds(pl.multiple_of(c * CW, CW), CW)
        return pltpu.make_async_copy(yst.at[lax.rem(c, 2)], y_ref.at[:, cols], ysem.at[lax.rem(c, 2)])

    def stage3(c):
        for i in range(2):
            for rows in range(2):
                final(c, i, rows).wait_recv()

        @pl.when(c >= 2)
        def _():
            ycopy(c - 2).wait()
        yst[lax.rem(c, 2)] = (res[c] + (part[0, c, chip["o"]] + fr[c, 0] + fr[c, 1])).astype(BF)
        ycopy(c).start()

    def step(c, _):
        @pl.when(c < nc)
        def _():
            compute(c)
            stage1(c)

        @pl.when((c >= 1) & (c < nc + 1))
        def _():
            stage2(c - 1)

        @pl.when(c >= 2)
        def _():
            stage3(c - 2)
        return 0

    lax.fori_loop(0, nc + 2, step, 0)
    for c in (nc - 2, nc - 1):
        ycopy(c).wait()

    def drain(c, _):
        swap(c).wait_send()
        for i in range(2):
            corner(c, i).wait_send()
            for rows in range(2):
                final(c, i, rows).wait_send()
        return 0

    lax.fori_loop(0, nc, drain, 0)


def solution(mesh):
    pg = mesh.shape["ey"] * mesh.shape["ex"] * mesh.shape["ec"]

    def local(x, ids, gates, w1, w3, w2, ws1, ws3, ws2):
        t, hd = x.shape
        top = ids.shape[1]
        el, _, f = w1.shape
        ne = el * pg
        cap = min(t, 2 * ((t * top + ne - 1) // ne))
        n = el * cap
        kw = hd // NK
        nc = hd // CW
        idt = jnp.pad(ids.T, ((0, 8 - top), (0, 0)), constant_values=-1)
        gt = jnp.pad(gates.T, ((0, 8 - top), (0, 0)))
        dma = pltpu.SemaphoreType.DMA
        h, sh, wc = pl.pallas_call(
            functools.partial(first, el, cap),
            out_shape=(jax.ShapeDtypeStruct((el, pg * cap, f), BF), jax.ShapeDtypeStruct((2, t, f), BF),
                       jax.ShapeDtypeStruct((pg, t, 3 * n), BF)),
            in_specs=[VM, VM] + [ANY] * 5, out_specs=(ANY,) * 3,
            scratch_shapes=[
                pltpu.VMEM((NK, pg, t, kw), BF), pltpu.VMEM((el, pg * cap, 2 * f), F32), pltpu.VMEM((NS, kw, 2 * f), BF),
                pltpu.VMEM((pg, n, t), BF), pltpu.VMEM((el, pg, cap, kw), BF), pltpu.VMEM((2, pg * cap, f), BF),
                pltpu.VMEM((2, t, 3 * n), BF), pltpu.VMEM((pg, 2 * el, t), F32), pltpu.VMEM((pg, 2 * el, t), F32),
                dma((NK,)), dma((NS, 2)), dma((2,)), dma((2,)), dma((8,)), dma((8,)), dma((NK, 9)), dma((NK, 9))],
            compiler_params=pltpu.CompilerParams(collective_id=0, has_side_effects=True, vmem_limit_bytes=VLIM),
        )(idt, gt, x, w1, w3, ws1, ws3)
        return pl.pallas_call(
            functools.partial(second, el, cap),
            out_shape=jax.ShapeDtypeStruct((t, hd), BF),
            in_specs=[ANY] * 6, out_specs=ANY,
            scratch_shapes=[
                pltpu.VMEM((el, pg * cap, f), BF), pltpu.VMEM((2, t, f), BF), pltpu.VMEM((pg, t, 3 * n), BF),
                pltpu.VMEM((t, hd), BF), pltpu.VMEM((NW, f, CW), BF), pltpu.VMEM((pg, 3 * n, CW), BF),
                pltpu.VMEM((2, nc, 4, t, CW), F32), pltpu.VMEM((nc, 4, t, CW), F32), pltpu.VMEM((nc, 2, t // 2, CW), F32),
                pltpu.VMEM((nc, 2, t, CW), F32), pltpu.VMEM((nc, t, CW), F32), pltpu.VMEM((2, t, CW), BF),
                dma((el,)), dma, dma((2,)), dma((NW,)), dma((2,)), dma((nc,)), dma((nc,)), dma((nc, 2)), dma((nc, 2)),
                dma((nc, 2, 2)), dma((nc, 2, 2))],
            compiler_params=pltpu.CompilerParams(collective_id=1, has_side_effects=True, vmem_limit_bytes=VLIM),
        )(h, sh, wc, x, w2, ws2)

    return jax.shard_map(local, mesh=mesh,
                         in_specs=(P(ALL), P(ALL), P(ALL), P(EXP), P(EXP), P(EXP), P(), P(), P()),
                         out_specs=P(ALL), check_vma=False)
```

```python
import functools

import jax
import jax.numpy as jnp
from jax import lax
from jax.experimental import pallas as pl
from jax.experimental.pallas import tpu as pltpu
from jax.sharding import PartitionSpec as P

EXP = ("ey", "ex", "ec")
ALL = ("dp", "ey", "ex", "ec")
MESH = pl.DeviceIdType.MESH
ANY = pl.BlockSpec(memory_space=pl.ANY)
VM = pl.BlockSpec(memory_space=pltpu.VMEM)
BF = jnp.bfloat16
F32 = jnp.float32
VLIM = 67043328

NK = 4
NS = 3
CW = 256
NW = 4
LAG = 3


def place():
    ey, ex, ec = (lax.axis_index(a) for a in EXP)
    dev = {"x": dict(ey=ey, ex=1 - ex, ec=ec), "y": dict(ey=1 - ey, ex=ex, ec=ec), "p": dict(ey=ey, ex=ex, ec=1 - ec)}
    chip = {"o": ey * 2 + ex, "x": ey * 2 + 1 - ex, "y": (1 - ey) * 2 + ex, "d": (1 - ey) * 2 + 1 - ex}
    return ey, ex, ec, dev, chip


def silu_mul(a, b):
    return (a * jax.nn.sigmoid(a) * b).astype(BF)


def first(el, cap, ids_ref, gates_ref, x_ref, ws1_ref, ws3_ref, ws2_ref, xe_ref, res_ref, wc_ref, cnt_ref,
          xg, acc, sh, wb, wd, disp, xst, rst, wst, cst, mout, meta,
          xsem, wsem, dsem, gsem, osem, csem, nsem, msend, mrecv, ssem, rsem):
    ey, ex, ec, dev, chip = place()
    t, hd = x_ref.shape
    top = ids_ref.shape[1]
    kw = hd // NK
    f = ws1_ref.shape[1] // 2
    nc = hd // CW
    half = t // 2
    n = el * cap
    lo, hi, full = pl.ds(0, half), pl.ds(half, half), pl.ds(0, t)
    mine = {c: ec * 4 + chip[c] for c in "oxyd"}
    theirs = {c: (1 - ec) * 4 + chip[c] for c in "oxyd"}
    nb = 2 * NK

    def block(b, go):
        @pl.when(b < nb)
        def _():
            slot = lax.rem(b, NS)
            rows = pl.ds(pl.multiple_of(lax.rem(b, NK) * kw, kw), kw)
            cols = pl.ds(pl.multiple_of((b // NK) * f, 128), f)
            for i, w in enumerate((ws1_ref, ws3_ref)):
                go(pltpu.make_async_copy(w.at[rows, cols], wb.at[slot, :, pl.ds(i * f, f)], wsem.at[slot, i]))

    def down(c, go):
        @pl.when(c < nc)
        def _():
            slot = lax.rem(c, NS)
            cols = pl.ds(pl.multiple_of(c * CW, CW), CW)
            go(pltpu.make_async_copy(ws2_ref.at[:, cols], wd.at[slot], dsem.at[slot]))

    def go_start(c):
        c.start()

    def go_wait(c):
        c.wait()

    for k in range(NK):
        pltpu.make_async_copy(x_ref.at[:, pl.ds(k * kw, kw)], xg.at[k, mine["o"]], xsem.at[k]).start()
    for b in range(NS - 1):
        block(b, go_start)
    for c in range(NS - 1):
        down(c, go_start)

    col = lax.broadcasted_iota(jnp.int32, (t, 128), 1)
    chosen = jnp.zeros((t, 128), F32)
    gate = jnp.zeros((t, 128), F32)
    for j in range(top):
        hit = ids_ref[:, j:j + 1] == col
        chosen = jnp.where(hit, 1.0, chosen)
        gate = jnp.where(hit, gates_ref[:, j:j + 1], gate)
    before = lax.broadcasted_iota(jnp.int32, (t, t), 1) < lax.broadcasted_iota(jnp.int32, (t, t), 0)
    rank = jnp.dot(jnp.where(before, 1.0, 0.0).astype(BF), chosen.astype(BF), preferred_element_type=F32)
    rank = jnp.where(chosen > 0.0, rank, -1.0).T
    gate = gate.T
    for d in range(8):
        mout[d, 0:el, :] = rank[d * el:(d + 1) * el]
        mout[d, el:2 * el, :] = gate[d * el:(d + 1) * el]

    barrier = pltpu.get_barrier_semaphore()
    others = [(a, b, c) for a in (0, 1) for b in (0, 1) for c in (0, 1) if a + b + c]

    def flip(o):
        return [lax.rem(v + s, 2) for v, s in zip((ey, ex, ec), o)]

    for o in others:
        y2, x2, c2 = flip(o)
        pl.semaphore_signal(barrier, inc=1, device_id=dict(ey=y2, ex=x2, ec=c2), device_id_type=MESH)
    pl.semaphore_wait(barrier, len(others))

    def remote(k, src, rows, chan, to):
        ref = xg.at[k, src, rows]
        return pltpu.make_async_remote_copy(ref, ref, ssem.at[k, chan], rsem.at[k, chan], device_id=dev[to],
                                            device_id_type=MESH)

    def direct(k):
        pltpu.make_async_copy(x_ref.at[:, pl.ds(k * kw, kw)], xg.at[k, mine["o"]], xsem.at[k]).wait()
        for chan, to in enumerate("xyp"):
            remote(k, mine["o"], full, chan, to).start()

    def relay(k):
        remote(k, mine["x"], full, 0, "x").wait_recv()
        remote(k, mine["x"], lo, 3, "y").start()
        remote(k, mine["x"], full, 5, "p").start()
        remote(k, mine["y"], full, 1, "y").wait_recv()
        remote(k, mine["y"], hi, 4, "x").start()
        remote(k, mine["y"], full, 6, "p").start()

    def corner(k):
        remote(k, mine["d"], lo, 3, "y").wait_recv()
        remote(k, mine["d"], lo, 7, "p").start()
        remote(k, mine["d"], hi, 4, "x").wait_recv()
        remote(k, mine["d"], hi, 8, "p").start()

    def arrived(k):
        remote(k, theirs["o"], full, 2, "p").wait_recv()
        remote(k, theirs["x"], full, 5, "p").wait_recv()
        remote(k, theirs["y"], full, 6, "p").wait_recv()
        remote(k, theirs["d"], lo, 7, "p").wait_recv()
        remote(k, theirs["d"], hi, 8, "p").wait_recv()

    def sent(k):
        for src, rows, chan, to in ((mine["o"], full, 0, "x"), (mine["o"], full, 1, "y"), (mine["o"], full, 2, "p"),
                                    (mine["x"], lo, 3, "y"), (mine["y"], hi, 4, "x"), (mine["x"], full, 5, "p"),
                                    (mine["y"], full, 6, "p"), (mine["d"], lo, 7, "p"), (mine["d"], hi, 8, "p")):
            remote(k, src, rows, chan, to).wait_send()

    def mcopy(o, back=False):
        y2, x2, c2 = flip(o)
        num = c2 * 4 + y2 * 2 + x2
        idx = y2 * 4 + x2 * 2 + c2
        src, dst = (meta.at[num], num) if back else (mout.at[idx], mine["o"])
        return pltpu.make_async_remote_copy(src, meta.at[dst], msend.at[num], mrecv.at[dst],
                                            device_id=dict(ey=y2, ex=x2, ec=c2), device_id_type=MESH)

    direct(0)
    for o in others:
        mcopy(o).start()
    direct(1)
    for k in range(2, NK):
        pltpu.make_async_copy(x_ref.at[:, pl.ds(k * kw, kw)], xg.at[k, mine["o"]], xsem.at[k]).wait()

    for hf in range(2):
        acc[...] = jnp.zeros((t, 2 * f), F32)

        def body(k, _):
            b = hf * NK + k
            block(b + NS - 1, go_start)
            block(b, go_wait)
            acc[...] += jnp.dot(xg[k, mine["o"]], wb[lax.rem(b, NS)], preferred_element_type=F32)
            return 0

        lax.fori_loop(0, NK, body, 0)
        sh[:, hf * f:(hf + 1) * f] = silu_mul(acc[:, 0:f], acc[:, f:2 * f])

    relay(0)
    for k in range(2, NK):
        for chan, to in enumerate("xyp"):
            if k == 2:
                remote(k, mine["o"], full, chan, to).start()

    meta[mine["o"]] = mout[ey * 4 + ex * 2 + ec]
    for o in others:
        mcopy(o, True).wait_recv()
    slots = lax.broadcasted_iota(jnp.int32, (cap, t), 0).astype(F32)

    def build(s, _):
        parts = []
        for e in range(el):
            sel = meta[s, e:e + 1, :] == slots
            disp[s, e * cap:(e + 1) * cap, :] = jnp.where(sel, 1.0, 0.0).astype(BF)
            parts.append(jnp.where(sel, meta[s, el + e:el + e + 1, :], 0.0))
        w = jnp.concatenate(parts, axis=0).T
        slot = lax.rem(s, 2)
        most = jnp.max(meta[s, 0:el, :], axis=1, keepdims=True).astype(jnp.int32) + 1
        cst[pl.ds(pl.multiple_of(s * el, 8), el), :] = jnp.broadcast_to(most, (el, 128))

        @pl.when(s >= 2)
        def _():
            pltpu.make_async_copy(wst.at[slot], wc_ref.at[s - 2], csem.at[slot]).wait()

        for i in range(3):
            p = w.astype(BF)
            wst[slot, :, i * n:(i + 1) * n] = p
            w = w - p.astype(F32)
        pltpu.make_async_copy(wst.at[slot], wc_ref.at[s], csem.at[slot]).start()
        return 0

    lax.fori_loop(0, 8, build, 0)
    counts = pltpu.make_async_copy(cst, cnt_ref, nsem)
    counts.start()

    def rcopy(c):
        return pltpu.make_async_copy(rst.at[lax.rem(c, 2)], res_ref.at[c], osem.at[lax.rem(c, 2)])

    def shared_down(c, _):
        down(c + NS - 1, go_start)
        down(c, go_wait)

        @pl.when(c >= 2)
        def _():
            rcopy(c - 2).wait()
        v = jnp.dot(sh[...], wd[lax.rem(c, NS)], preferred_element_type=F32).astype(BF).astype(F32)
        per = kw // CW
        cols = pl.ds(pl.multiple_of(lax.rem(c, per) * CW, CW), CW)
        rst[lax.rem(c, 2)] = xg[c // per, mine["o"], :, cols].astype(F32) + v
        rcopy(c).start()
        return 0

    lax.fori_loop(0, nc // 2, shared_down, 0)
    relay(1)
    for chan, to in enumerate("xyp"):
        remote(3, mine["o"], full, chan, to).start()
    lax.fori_loop(nc // 2, nc, shared_down, 0)

    def gcopy(k, s):
        slot = lax.rem(s, 2)
        return pltpu.make_async_copy(xst.at[slot], xe_ref.at[:, s, :, pl.ds(pl.multiple_of(k * kw, kw), kw)], gsem.at[slot])

    def gather(k):
        def body(s, _):
            r = jnp.dot(disp[s], xg[k, s], preferred_element_type=F32).astype(BF)
            if isinstance(k, int) and k == 0:
                @pl.when(s >= 2)
                def _():
                    gcopy(k, s - 2).wait()
            else:
                @pl.when(s < 2)
                def _():
                    gcopy(k - 1, s + 6).wait()

                @pl.when(s >= 2)
                def _():
                    gcopy(k, s - 2).wait()
            for e in range(el):
                xst[lax.rem(s, 2), e] = r[e * cap:(e + 1) * cap]
            gcopy(k, s).start()
            return 0

        lax.fori_loop(0, 8, body, 0)

    corner(0)
    arrived(0)
    gather(0)
    relay(2)
    corner(1)
    arrived(1)
    gather(1)
    relay(3)
    corner(2)
    arrived(2)
    gather(2)
    corner(3)
    arrived(3)
    gather(3)

    for s in (6, 7):
        gcopy(NK - 1, s).wait()
        pltpu.make_async_copy(wst.at[s % 2], wc_ref.at[s], csem.at[s % 2]).wait()
    for c in (nc - 2, nc - 1):
        rcopy(c).wait()
    counts.wait()
    for o in others:
        mcopy(o).wait_send()

    def drain(k, _):
        sent(k)
        return 0

    lax.fori_loop(0, NK, drain, 0)


def middle(el, cap, cnt_ref, xe_ref, w1_ref, w3_ref, h_ref, xc, wb, hs, zero, wsem, xsem, osem):
    f = w1_ref.shape[2]
    hd = w1_ref.shape[1]
    pc = 16
    rows = 8 * cap

    def pieces(e, go, skip=None):
        off = 0
        for s in range(8):
            n = cnt_ref[s * el + e, 0]
            for r in range(cap // pc):
                at = pl.ds(r * pc, pc)
                if skip is None:
                    pl.when(n > r * pc)(functools.partial(go, s, at, off + r * pc))
                else:
                    pl.when(n > r * pc)(functools.partial(go, s, at, off + r * pc))
                    pl.when(n <= r * pc)(functools.partial(skip, s, at))
            off += (n + pc - 1) // pc * pc
        return off

    def rows_in(e, op):
        slot = lax.rem(e, 2)

        def go(s, at, off):
            op(pltpu.make_async_copy(xe_ref.at[e, s, at], xc.at[slot, pl.ds(pl.multiple_of(off, pc), pc)], xsem.at[slot]))
        return pieces(e, go)

    def rows_out(e, op):
        slot = lax.rem(e, 2)

        def go(s, at, off):
            op(pltpu.make_async_copy(hs.at[slot, pl.ds(pl.multiple_of(off, pc), pc)], h_ref.at[e, s, at], osem.at[slot]))

        def skip(s, at):
            op(pltpu.make_async_copy(zero, h_ref.at[e, s, at], osem.at[slot]))
        pieces(e, go, skip)

    def weights(e, op):
        slot = lax.rem(e, 2)
        q = hd // 2
        for i, w in enumerate((w1_ref, w3_ref)):
            for j in range(2):
                at = pl.ds(j * q, q)
                op(pltpu.make_async_copy(w.at[e, at], wb.at[slot, at, pl.ds(i * f, f)], wsem.at[slot]))

    def start(c):
        c.start()

    def wait(c):
        c.wait()

    rows_in(0, start)
    weights(0, start)
    rows_in(1, start)
    weights(1, start)
    zero[...] = jnp.zeros_like(zero)

    def body(e, _):
        slot = lax.rem(e, 2)
        total = rows_in(e, wait)
        weights(e, wait)

        @pl.when(e >= 2)
        def _():
            rows_out(e - 2, wait)

        def go(m):
            d = jnp.dot(xc[slot, 0:m], wb[slot], preferred_element_type=F32)
            hs[slot, 0:m] = silu_mul(d[:, 0:f], d[:, f:2 * f])

        step = rows // 3
        for i in range(1, 4):
            pl.when((total <= i * step) & (total > (i - 1) * step))(functools.partial(go, i * step))
        rows_out(e, start)

        @pl.when(e + 2 < el)
        def _():
            rows_in(e + 2, start)
            weights(e + 2, start)
        return 0

    lax.fori_loop(0, el, body, 0)
    rows_out(el - 2, wait)
    rows_out(el - 1, wait)


def second(el, cap, h_ref, wc_ref, res_ref, w2_ref, y_ref,
           hv, wcv, wb, o3, part, pr, dr, fr, res, yst,
           hsem, csem, xsem, wsem, ysem, psend, precv, dsend, drecv, fsend, frecv):
    ey, ex, ec, dev, chip = place()
    t, hd = y_ref.shape
    nc = hd // CW
    half = t // 2
    lo, hi = pl.ds(0, half), pl.ds(half, half)
    per = el
    nb = nc * per
    n = el * cap

    def block(b, go):
        c, j = b // per, lax.rem(b, per)
        cols = pl.ds(pl.multiple_of(c * CW, CW), CW)
        slot = lax.rem(b, NW)

        @pl.when(b < nb)
        def _():
            go(pltpu.make_async_copy(w2_ref.at[j, :, cols], wb.at[slot], wsem.at[slot]))

    def fetch(b):
        block(b, lambda c: c.start())

    def ready(b):
        block(b, lambda c: c.wait())

    def hcopy(e):
        return pltpu.make_async_copy(h_ref.at[e], hv.at[e], hsem.at[e])

    hcopy(0).start()
    for b in range(NW - 1):
        fetch(b)
    for e in range(1, el):
        hcopy(e).start()
    loads = [pltpu.make_async_copy(wc_ref, wcv, csem), pltpu.make_async_copy(res_ref, res, xsem)]
    for c in loads:
        c.start()

    barrier = pltpu.get_barrier_semaphore()
    for to in "xyp":
        pl.semaphore_signal(barrier, inc=1, device_id=dev[to], device_id_type=MESH)
    pl.semaphore_wait(barrier, 3)

    def swap(c):
        return pltpu.make_async_remote_copy(part.at[1, c], pr.at[c], psend.at[c], precv.at[c], device_id=dev["p"],
                                            device_id_type=MESH)

    def corner(c, i):
        src = part.at[0, c, chip["d"], (lo, hi)[i]]
        return pltpu.make_async_remote_copy(src, dr.at[c, i], dsend.at[c, i], drecv.at[c, i], device_id=dev["xy"[i]],
                                            device_id_type=MESH)

    def final(c, i, rows):
        src = part.at[0, c, chip["xy"[i]], (lo, hi)[rows]]
        return pltpu.make_async_remote_copy(src, fr.at[c, i, (lo, hi)[rows]], fsend.at[c, i, rows], frecv.at[c, i, rows],
                                            device_id=dev["xy"[i]], device_id_type=MESH)

    def weigh(c, g):
        core = ec if g == 0 else 1 - ec

        def body(ch, _):
            s = core * 4 + ch
            part[g, c, ch] = jnp.dot(wcv[s], o3[s], preferred_element_type=F32)
            return 0

        lax.fori_loop(0, 4, body, 0)

    def compute(c):
        def expert(e, _):
            b = c * per + e
            fetch(b + NW - 1)

            @pl.when(c == 0)
            def _():
                hcopy(e).wait()
            ready(b)
            o = jnp.dot(hv[e], wb[lax.rem(b, NW)], preferred_element_type=F32).astype(BF)
            for s in range(8):
                for i in range(3):
                    o3[s, pl.ds(pl.multiple_of(i * n + e * cap, 16), cap), :] = o[s * cap:(s + 1) * cap]
            return 0

        lax.fori_loop(0, el, expert, 0)

        @pl.when(c == 0)
        def _():
            for d in loads:
                d.wait()
        weigh(c, 1)
        swap(c).start()
        weigh(c, 0)

    def stage1(c):
        swap(c).wait_recv()
        for ch in "dxyo":
            part[0, c, chip[ch]] += pr[c, chip[ch]]
        corner(c, 0).start()
        corner(c, 1).start()
        final(c, 0, 0).start()
        final(c, 1, 1).start()

    def stage2(c):
        corner(c, 0).wait_recv()
        part[0, c, chip["y"], 0:half] += dr[c, 0]
        corner(c, 1).wait_recv()
        part[0, c, chip["x"], half:t] += dr[c, 1]
        final(c, 1, 0).start()
        final(c, 0, 1).start()

    def ycopy(c):
        cols = pl.ds(pl.multiple_of(c * CW, CW), CW)
        return pltpu.make_async_copy(yst.at[lax.rem(c, 2)], y_ref.at[:, cols], ysem.at[lax.rem(c, 2)])

    def stage3(c):
        for i in range(2):
            for rows in range(2):
                final(c, i, rows).wait_recv()

        @pl.when(c >= 2)
        def _():
            ycopy(c - 2).wait()
        yst[lax.rem(c, 2)] = (res[c] + (part[0, c, chip["o"]] + fr[c, 0] + fr[c, 1])).astype(BF)
        ycopy(c).start()

    def step(c, _):
        @pl.when(c < nc)
        def _():
            compute(c)
            stage1(c)

        @pl.when((c >= 1) & (c < nc + 1))
        def _():
            stage2(c - 1)

        @pl.when(c >= LAG)
        def _():
            stage3(c - LAG)
        return 0

    lax.fori_loop(0, nc + LAG, step, 0)
    for c in (nc - 2, nc - 1):
        ycopy(c).wait()

    def drain(c, _):
        swap(c).wait_send()
        for i in range(2):
            corner(c, i).wait_send()
            for rows in range(2):
                final(c, i, rows).wait_send()
        return 0

    lax.fori_loop(0, nc, drain, 0)


def solution(mesh):
    pg = mesh.shape["ey"] * mesh.shape["ex"] * mesh.shape["ec"]

    def local(x, ids, gates, w1, w3, w2, ws1, ws3, ws2):
        t, hd = x.shape
        top = ids.shape[1]
        el, _, f = w1.shape
        ne = el * pg
        cap = min(t, 2 * ((t * top + ne - 1) // ne))
        n = el * cap
        kw = hd // NK
        nc = hd // CW
        dma = pltpu.SemaphoreType.DMA
        xe, res, wc, cnt = pl.pallas_call(
            functools.partial(first, el, cap),
            out_shape=(jax.ShapeDtypeStruct((el, pg, cap, hd), BF), jax.ShapeDtypeStruct((nc, t, CW), F32),
                       jax.ShapeDtypeStruct((pg, t, 3 * n), BF), jax.ShapeDtypeStruct((pg * el, 128), jnp.int32)),
            in_specs=[VM, VM] + [ANY] * 4, out_specs=(ANY,) * 4,
            scratch_shapes=[
                pltpu.VMEM((NK, pg, t, kw), BF), pltpu.VMEM((t, 2 * f), F32), pltpu.VMEM((t, 2 * f), BF),
                pltpu.VMEM((NS, kw, 2 * f), BF), pltpu.VMEM((NS, 2 * f, CW), BF), pltpu.VMEM((pg, n, t), BF),
                pltpu.VMEM((2, el, cap, kw), BF), pltpu.VMEM((2, t, CW), F32), pltpu.VMEM((2, t, 3 * n), BF),
                pltpu.VMEM((pg * el, 128), jnp.int32), pltpu.VMEM((pg, 2 * el, t), F32), pltpu.VMEM((pg, 2 * el, t), F32),
                dma((NK,)), dma((NS, 2)), dma((NS,)), dma((2,)), dma((2,)), dma((2,)), dma, dma((8,)), dma((8,)),
                dma((NK, 9)), dma((NK, 9))],
            compiler_params=pltpu.CompilerParams(collective_id=0, has_side_effects=True, vmem_limit_bytes=VLIM),
        )(ids, gates, x, ws1, ws3, ws2)
        h = pl.pallas_call(
            functools.partial(middle, el, cap),
            out_shape=jax.ShapeDtypeStruct((el, pg, cap, f), BF),
            in_specs=[pl.BlockSpec(memory_space=pltpu.SMEM)] + [ANY] * 3, out_specs=ANY,
            scratch_shapes=[
                pltpu.VMEM((2, pg * cap, hd), BF), pltpu.VMEM((2, hd, 2 * f), BF), pltpu.VMEM((2, pg * cap, f), BF),
                pltpu.VMEM((16, f), BF), dma((2,)), dma((2,)), dma((2,))],
            compiler_params=pltpu.CompilerParams(vmem_limit_bytes=VLIM),
        )(cnt, xe, w1, w3)
        return pl.pallas_call(
            functools.partial(second, el, cap),
            out_shape=jax.ShapeDtypeStruct((t, hd), BF),
            in_specs=[ANY] * 4, out_specs=ANY,
            scratch_shapes=[
                pltpu.VMEM((el, pg * cap, f), BF), pltpu.VMEM((pg, t, 3 * n), BF),
                pltpu.VMEM((NW, f, CW), BF), pltpu.VMEM((pg, 3 * n, CW), BF),
                pltpu.VMEM((2, nc, 4, t, CW), F32), pltpu.VMEM((nc, 4, t, CW), F32), pltpu.VMEM((nc, 2, t // 2, CW), F32),
                pltpu.VMEM((nc, 2, t, CW), F32), pltpu.VMEM((nc, t, CW), F32), pltpu.VMEM((2, t, CW), BF),
                dma((el,)), dma, dma, dma((NW,)), dma((2,)), dma((nc,)), dma((nc,)), dma((nc, 2)), dma((nc, 2)),
                dma((nc, 2, 2)), dma((nc, 2, 2))],
            compiler_params=pltpu.CompilerParams(collective_id=1, has_side_effects=True, vmem_limit_bytes=VLIM),
        )(h.reshape(el, pg * cap, f), wc, res, w2)

    return jax.shard_map(local, mesh=mesh,
                         in_specs=(P(ALL), P(ALL), P(ALL), P(EXP), P(EXP), P(EXP), P(), P(), P()),
                         out_specs=P(ALL), check_vma=False)
```

```python
import functools

import jax
import jax.numpy as jnp
from jax import lax
from jax.experimental import pallas as pl
from jax.experimental.pallas import tpu as pltpu
from jax.sharding import PartitionSpec as P

EXP = ("ey", "ex", "ec")
ALL = ("dp", "ey", "ex", "ec")
MESH = pl.DeviceIdType.MESH
ANY = pl.BlockSpec(memory_space=pl.ANY)
VM = pl.BlockSpec(memory_space=pltpu.VMEM)
BF = jnp.bfloat16
F32 = jnp.float32
VLIM = 67043328

NK = 4
NS = 3
CW = 256
NW = 4
LAG = 3
SLAB = 256


def place():
    ey, ex, ec = (lax.axis_index(a) for a in EXP)
    dev = {"x": dict(ey=ey, ex=1 - ex, ec=ec), "y": dict(ey=1 - ey, ex=ex, ec=ec), "p": dict(ey=ey, ex=ex, ec=1 - ec)}
    chip = {"o": ey * 2 + ex, "x": ey * 2 + 1 - ex, "y": (1 - ey) * 2 + ex, "d": (1 - ey) * 2 + 1 - ex}
    return ey, ex, ec, dev, chip


def silu_mul(a, b):
    return (a * jax.nn.sigmoid(a) * b).astype(BF)


def first(el, cap, ids_ref, gates_ref, x_ref, w1_ref, w3_ref, ws1_ref, ws3_ref, h_ref, sh_ref, meta_ref,
          xg, acc, wb, disp, xe, hst, mout, meta,
          xsem, wsem, osem, csem, msend, mrecv, ssem, rsem):
    ey, ex, ec, dev, chip = place()
    t = x_ref.shape[0]
    kw = x_ref.shape[1] // NK
    f = w1_ref.shape[2]
    half = t // 2
    lo, hi, full = pl.ds(0, half), pl.ds(half, half), pl.ds(0, t)
    mine = {c: ec * 4 + chip[c] for c in "oxyd"}
    theirs = {c: (1 - ec) * 4 + chip[c] for c in "oxyd"}
    nsh = 2 * NK
    nb = nsh + NK * el

    def block(b, go):
        slot = lax.rem(b, NS)

        @pl.when(b < nsh)
        def _():
            rows = pl.ds(pl.multiple_of(lax.rem(b, NK) * kw, kw), kw)
            cols = pl.ds(pl.multiple_of((b // NK) * f, 128), f)
            for i, w in enumerate((ws1_ref, ws3_ref)):
                go(pltpu.make_async_copy(w.at[rows, cols], wb.at[slot, :, pl.ds(i * f, f)], wsem.at[slot, i]))

        @pl.when((b >= nsh) & (b < nb))
        def _():
            q = b - nsh
            rows = pl.ds(pl.multiple_of((q // el) * kw, kw), kw)
            for i, w in enumerate((w1_ref, w3_ref)):
                go(pltpu.make_async_copy(w.at[lax.rem(q, el), rows], wb.at[slot, :, pl.ds(i * f, f)], wsem.at[slot, i]))

    def fetch(b):
        block(b, lambda c: c.start())

    def ready(b):
        block(b, lambda c: c.wait())

    for b in range(NS - 1):
        fetch(b)
    for k in range(NK):
        pltpu.make_async_copy(x_ref.at[:, pl.ds(k * kw, kw)], xg.at[k, mine["o"]], xsem.at[k]).start()

    ne = el * 8
    row = lax.broadcasted_iota(jnp.int32, (ne, t), 0)
    chosen = jnp.zeros((ne, t), F32)
    gate = jnp.zeros((ne, t), F32)
    for j in range(ids_ref.shape[0]):
        hit = ids_ref[j:j + 1, :] == row
        chosen = jnp.where(hit, 1.0, chosen)
        gate = jnp.where(hit, gates_ref[j:j + 1, :], gate)
    before = (lax.broadcasted_iota(jnp.int32, (t, t), 0) < lax.broadcasted_iota(jnp.int32, (t, t), 1))
    rank = jnp.dot(chosen.astype(BF), before.astype(F32).astype(BF), preferred_element_type=F32)
    rank = jnp.where(chosen > 0.0, rank, -1.0)
    for d in range(8):
        mout[d, 0:el, :] = rank[d * el:(d + 1) * el]
        mout[d, el:2 * el, :] = gate[d * el:(d + 1) * el]

    barrier = pltpu.get_barrier_semaphore()
    others = [(a, b, c) for a in (0, 1) for b in (0, 1) for c in (0, 1) if a + b + c]

    def flip(o):
        return [lax.rem(v + s, 2) for v, s in zip((ey, ex, ec), o)]

    for o in others:
        y2, x2, c2 = flip(o)
        pl.semaphore_signal(barrier, inc=1, device_id=dict(ey=y2, ex=x2, ec=c2), device_id_type=MESH)
    pl.semaphore_wait(barrier, len(others))

    for k in range(NK):
        pltpu.make_async_copy(x_ref.at[:, pl.ds(k * kw, kw)], xg.at[k, mine["o"]], xsem.at[k]).wait()

    def remote(k, src, rows, chan, to):
        ref = xg.at[k, src, rows]
        return pltpu.make_async_remote_copy(ref, ref, ssem.at[k, chan], rsem.at[k, chan], device_id=dev[to],
                                            device_id_type=MESH)

    def direct(k):
        for chan, to in enumerate("xyp"):
            remote(k, mine["o"], full, chan, to).start()

    def relay(k):
        remote(k, mine["x"], full, 0, "x").wait_recv()
        remote(k, mine["x"], lo, 3, "y").start()
        remote(k, mine["x"], full, 5, "p").start()
        remote(k, mine["y"], full, 1, "y").wait_recv()
        remote(k, mine["y"], hi, 4, "x").start()
        remote(k, mine["y"], full, 6, "p").start()

    def corner(k):
        remote(k, mine["d"], lo, 3, "y").wait_recv()
        remote(k, mine["d"], lo, 7, "p").start()
        remote(k, mine["d"], hi, 4, "x").wait_recv()
        remote(k, mine["d"], hi, 8, "p").start()

    def arrived(k):
        remote(k, theirs["o"], full, 2, "p").wait_recv()
        remote(k, theirs["x"], full, 5, "p").wait_recv()
        remote(k, theirs["y"], full, 6, "p").wait_recv()
        remote(k, theirs["d"], lo, 7, "p").wait_recv()
        remote(k, theirs["d"], hi, 8, "p").wait_recv()

    def sent(k):
        for src, rows, chan, to in ((mine["o"], full, 0, "x"), (mine["o"], full, 1, "y"), (mine["o"], full, 2, "p"),
                                    (mine["x"], lo, 3, "y"), (mine["y"], hi, 4, "x"), (mine["x"], full, 5, "p"),
                                    (mine["y"], full, 6, "p"), (mine["d"], lo, 7, "p"), (mine["d"], hi, 8, "p")):
            remote(k, src, rows, chan, to).wait_send()

    def mcopy(o, back=False):
        y2, x2, c2 = flip(o)
        num = c2 * 4 + y2 * 2 + x2
        idx = y2 * 4 + x2 * 2 + c2
        src, dst = (meta.at[num], num) if back else (mout.at[idx], mine["o"])
        return pltpu.make_async_remote_copy(src, meta.at[dst], msend.at[num], mrecv.at[dst],
                                            device_id=dict(ey=y2, ex=x2, ec=c2), device_id_type=MESH)

    for o in others:
        mcopy(o).start()
    direct(0)
    direct(1)

    for hf in range(2):
        acc[0, 0:t, :] = jnp.zeros((t, 2 * f), F32)

        def body(k, _):
            b = hf * NK + k
            fetch(b + NS - 1)
            ready(b)
            acc[0, 0:t, :] += jnp.dot(xg[k, mine["o"]], wb[lax.rem(b, NS)], preferred_element_type=F32)
            return 0

        lax.fori_loop(0, NK, body, 0)
        hst[hf, 0:t, :] = silu_mul(acc[0, 0:t, 0:f], acc[0, 0:t, f:2 * f])
        pltpu.make_async_copy(hst.at[hf, 0:t], sh_ref.at[hf], osem.at[hf]).start()

    relay(0)
    direct(2)

    meta[mine["o"]] = mout[ey * 4 + ex * 2 + ec]
    for o in others:
        mcopy(o, True).wait_recv()
    keep = pltpu.make_async_copy(meta, meta_ref, csem)
    keep.start()
    slots = lax.broadcasted_iota(jnp.int32, (cap, t), 0).astype(F32)

    def build(s, _):
        for e in range(el):
            sel = meta[s, e:e + 1, :] == slots
            disp[s, e * cap:(e + 1) * cap, :] = jnp.where(sel, 1.0, 0.0).astype(BF)
        return 0

    lax.fori_loop(0, 8, build, 0)
    relay(1)
    direct(3)

    def gather(k):
        def body(s, _):
            r = jnp.dot(disp[s], xg[k, s], preferred_element_type=F32).astype(BF)
            for e in range(el):
                xe[e, s] = r[e * cap:(e + 1) * cap]
            return 0

        lax.fori_loop(0, 8, body, 0)

    def product(k, e, use):
        b = nsh + k * el + e
        fetch(b + NS - 1)
        ready(b)
        slot = lax.rem(b, NS)
        u = xe[e].reshape(8 * cap, kw)

        def part(at):
            return jnp.dot(u, wb[slot, :, at], preferred_element_type=F32)
        use(part)

    def slabs(w):
        return [slice(i, min(i + w, 2 * f)) for i in range(0, 2 * f, w)]

    def start_acc(e, _):
        def use(part):
            for at in slabs(SLAB):
                acc[e, :, at] = part(at)
        product(0, e, use)
        return 0

    corner(0)
    arrived(0)
    gather(0)
    lax.fori_loop(0, el // 2, start_acc, 0)
    relay(2)
    corner(1)
    lax.fori_loop(el // 2, el, start_acc, 0)

    def more(k, _):
        arrived(k)
        gather(k)

        def add(e, _):
            def use(part):
                for at in slabs(SLAB):
                    acc[e, :, at] += part(at)
            product(k, e, use)
            return 0

        lax.fori_loop(0, el // 2, add, 0)

        @pl.when(k == 1)
        def _():
            relay(3)
        corner(k + 1)
        lax.fori_loop(el // 2, el, add, 0)
        return 0

    lax.fori_loop(1, NK - 1, more, 0)

    arrived(NK - 1)
    gather(NK - 1)
    for hf in range(2):
        pltpu.make_async_copy(hst.at[hf, 0:t], sh_ref.at[hf], osem.at[hf]).wait()

    def last(e, _):
        slot = lax.rem(e, 2)

        @pl.when(e >= 2)
        def _():
            pltpu.make_async_copy(hst.at[slot], h_ref.at[e - 2], osem.at[slot]).wait()

        def use(part):
            nt = f // 128
            live = {}
            order = [nt // 2] + [v for i in range(nt // 2) for v in (i, nt // 2 + 1 + i)]
            for i in order:
                at = slice(i * 256, i * 256 + 256)
                d = acc[e, :, at] + part(at)
                for j in (2 * i, 2 * i + 1):
                    live[j] = d[:, (j - 2 * i) * 128:(j - 2 * i) * 128 + 128]
                    if j == nt - 1:
                        acc[e, :, j * 128:j * 128 + 128] = live.pop(j)
                for j in [v for v in live if v < nt and v + nt in live]:
                    hst[slot, :, j * 128:j * 128 + 128] = silu_mul(live.pop(j), live.pop(j + nt))
                if 2 * nt - 1 in live:
                    j = nt - 1
                    hst[slot, :, j * 128:j * 128 + 128] = silu_mul(acc[e, :, j * 128:j * 128 + 128], live.pop(2 * nt - 1))
        product(NK - 1, e, use)
        pltpu.make_async_copy(hst.at[slot], h_ref.at[e], osem.at[slot]).start()
        return 0

    lax.fori_loop(0, el, last, 0)

    keep.wait()
    for e in (el - 2, el - 1):
        pltpu.make_async_copy(hst.at[e % 2], h_ref.at[e], osem.at[e % 2]).wait()
    for o in others:
        mcopy(o).wait_send()
    for k in range(NK):
        sent(k)


def second(el, cap, h_ref, sh_ref, meta_ref, x_ref, w2_ref, ws2_ref, y_ref,
           hv, shv, wcv, meta, xv, wb, o3, part, pr, dr, fr, res, yst,
           hsem, csem, xsem, wsem, ysem, psend, precv, dsend, drecv, fsend, frecv):
    ey, ex, ec, dev, chip = place()
    t, hd = x_ref.shape
    nc = hd // CW
    f = w2_ref.shape[1]
    half = t // 2
    lo, hi = pl.ds(0, half), pl.ds(half, half)
    per = el + 2
    nb = nc * per
    n = el * cap

    def block(b, go):
        c, j = b // per, lax.rem(b, per)
        cols = pl.ds(pl.multiple_of(c * CW, CW), CW)
        slot = lax.rem(b, NW)

        @pl.when((j < el) & (b < nb))
        def _():
            go(pltpu.make_async_copy(w2_ref.at[j, :, cols], wb.at[slot], wsem.at[slot]))

        @pl.when((j >= el) & (b < nb))
        def _():
            rows = pl.ds(pl.multiple_of((j - el) * f, 128), f)
            go(pltpu.make_async_copy(ws2_ref.at[rows, cols], wb.at[slot], wsem.at[slot]))

    def fetch(b):
        block(b, lambda c: c.start())

    def ready(b):
        block(b, lambda c: c.wait())

    def hcopy(e):
        return pltpu.make_async_copy(h_ref.at[e], hv.at[e], hsem.at[e])

    hcopy(0).start()
    for b in range(NW - 1):
        fetch(b)
    for e in range(1, el):
        hcopy(e).start()
    loads = [pltpu.make_async_copy(sh_ref, shv, xsem.at[0]), pltpu.make_async_copy(x_ref, xv, xsem.at[1]),
             ]
    m = pltpu.make_async_copy(meta_ref, meta, csem)
    m.start()
    for c in loads:
        c.start()

    barrier = pltpu.get_barrier_semaphore()
    for to in "xyp":
        pl.semaphore_signal(barrier, inc=1, device_id=dev[to], device_id_type=MESH)
    pl.semaphore_wait(barrier, 3)

    m.wait()
    slots = lax.broadcasted_iota(jnp.int32, (cap, t), 0).astype(F32)

    def build(s, _):
        parts = [jnp.where(meta[s, e:e + 1, :] == slots, meta[s, el + e:el + e + 1, :], 0.0) for e in range(el)]
        w = jnp.concatenate(parts, axis=0).T
        for i in range(3):
            p = w.astype(BF)
            wcv[s, :, i * n:(i + 1) * n] = p
            w = w - p.astype(F32)
        return 0

    lax.fori_loop(0, 8, build, 0)

    def swap(c):
        return pltpu.make_async_remote_copy(part.at[1, c], pr.at[c], psend.at[c], precv.at[c], device_id=dev["p"],
                                            device_id_type=MESH)

    def corner(c, i):
        src = part.at[0, c, chip["d"], (lo, hi)[i]]
        return pltpu.make_async_remote_copy(src, dr.at[c, i], dsend.at[c, i], drecv.at[c, i], device_id=dev["xy"[i]],
                                            device_id_type=MESH)

    def final(c, i, rows):
        src = part.at[0, c, chip["xy"[i]], (lo, hi)[rows]]
        return pltpu.make_async_remote_copy(src, fr.at[c, i, (lo, hi)[rows]], fsend.at[c, i, rows], frecv.at[c, i, rows],
                                            device_id=dev["xy"[i]], device_id_type=MESH)

    def weigh(c, g):
        core = ec if g == 0 else 1 - ec

        def body(ch, _):
            s = core * 4 + ch
            part[g, c, ch] = jnp.dot(wcv[s], o3[s], preferred_element_type=F32)
            return 0

        lax.fori_loop(0, 4, body, 0)

    def compute(c):
        def expert(e, _):
            b = c * per + e
            fetch(b + NW - 1)

            @pl.when(c == 0)
            def _():
                hcopy(e).wait()
            ready(b)
            o = jnp.dot(hv[e], wb[lax.rem(b, NW)], preferred_element_type=F32).astype(BF)
            for s in range(8):
                for i in range(3):
                    o3[s, pl.ds(pl.multiple_of(i * n + e * cap, 16), cap), :] = o[s * cap:(s + 1) * cap]
            return 0

        lax.fori_loop(0, el, expert, 0)

        weigh(c, 1)
        swap(c).start()
        weigh(c, 0)

    def shared(c):
        @pl.when(c == 0)
        def _():
            for d in loads:
                d.wait()
        s = None
        for i in range(2):
            b = c * per + el + i
            fetch(b + NW - 1)
            ready(b)
            p = jnp.dot(shv[i], wb[lax.rem(b, NW)], preferred_element_type=F32)
            s = p if s is None else s + p
        cols = pl.ds(pl.multiple_of(c * CW, CW), CW)
        res[c] = xv[:, cols].astype(F32) + s.astype(BF).astype(F32)

    def stage1(c):
        swap(c).wait_recv()
        for ch in "dxyo":
            part[0, c, chip[ch]] += pr[c, chip[ch]]
        corner(c, 0).start()
        corner(c, 1).start()
        final(c, 0, 0).start()
        final(c, 1, 1).start()

    def stage2(c):
        corner(c, 0).wait_recv()
        part[0, c, chip["y"], 0:half] += dr[c, 0]
        corner(c, 1).wait_recv()
        part[0, c, chip["x"], half:t] += dr[c, 1]
        final(c, 1, 0).start()
        final(c, 0, 1).start()

    def ycopy(c):
        cols = pl.ds(pl.multiple_of(c * CW, CW), CW)
        return pltpu.make_async_copy(yst.at[lax.rem(c, 2)], y_ref.at[:, cols], ysem.at[lax.rem(c, 2)])

    def stage3(c):
        for i in range(2):
            for rows in range(2):
                final(c, i, rows).wait_recv()

        @pl.when(c >= 2)
        def _():
            ycopy(c - 2).wait()
        yst[lax.rem(c, 2)] = (res[c] + (part[0, c, chip["o"]] + fr[c, 0] + fr[c, 1])).astype(BF)
        ycopy(c).start()

    def step(c, _):
        @pl.when(c < nc)
        def _():
            compute(c)
            stage1(c)
            shared(c)

        @pl.when((c >= 1) & (c < nc + 1))
        def _():
            stage2(c - 1)

        @pl.when(c >= LAG)
        def _():
            stage3(c - LAG)
        return 0

    lax.fori_loop(0, nc + LAG, step, 0)
    for c in (nc - 2, nc - 1):
        ycopy(c).wait()

    def drain(c, _):
        swap(c).wait_send()
        for i in range(2):
            corner(c, i).wait_send()
            for rows in range(2):
                final(c, i, rows).wait_send()
        return 0

    lax.fori_loop(0, nc, drain, 0)


def solution(mesh):
    pg = mesh.shape["ey"] * mesh.shape["ex"] * mesh.shape["ec"]

    def local(x, ids, gates, w1, w3, w2, ws1, ws3, ws2):
        t, hd = x.shape
        top = ids.shape[1]
        el, _, f = w1.shape
        ne = el * pg
        cap = min(t, 2 * ((t * top + ne - 1) // ne))
        n = el * cap
        kw = hd // NK
        nc = hd // CW
        dma = pltpu.SemaphoreType.DMA
        h, sh, meta = pl.pallas_call(
            functools.partial(first, el, cap),
            out_shape=(jax.ShapeDtypeStruct((el, pg * cap, f), BF), jax.ShapeDtypeStruct((2, t, f), BF),
                       jax.ShapeDtypeStruct((pg, 2 * el, t), F32)),
            in_specs=[VM, VM] + [ANY] * 5, out_specs=(ANY,) * 3,
            scratch_shapes=[
                pltpu.VMEM((NK, pg, t, kw), BF), pltpu.VMEM((el, pg * cap, 2 * f), F32), pltpu.VMEM((NS, kw, 2 * f), BF),
                pltpu.VMEM((pg, n, t), BF), pltpu.VMEM((el, pg, cap, kw), BF), pltpu.VMEM((2, pg * cap, f), BF),
                pltpu.VMEM((pg, 2 * el, t), F32), pltpu.VMEM((pg, 2 * el, t), F32),
                dma((NK,)), dma((NS, 2)), dma((2,)), dma, dma((8,)), dma((8,)), dma((NK, 9)), dma((NK, 9))],
            compiler_params=pltpu.CompilerParams(collective_id=0, has_side_effects=True, vmem_limit_bytes=VLIM),
        )(ids.T, gates.T, x, w1, w3, ws1, ws3)
        return pl.pallas_call(
            functools.partial(second, el, cap),
            out_shape=jax.ShapeDtypeStruct((t, hd), BF),
            in_specs=[ANY] * 6, out_specs=ANY,
            scratch_shapes=[
                pltpu.VMEM((el, pg * cap, f), BF), pltpu.VMEM((2, t, f), BF), pltpu.VMEM((pg, t, 3 * n), BF), pltpu.VMEM((pg, 2 * el, t), F32),
                pltpu.VMEM((t, hd), BF), pltpu.VMEM((NW, f, CW), BF), pltpu.VMEM((pg, 3 * n, CW), BF),
                pltpu.VMEM((2, nc, 4, t, CW), F32), pltpu.VMEM((nc, 4, t, CW), F32), pltpu.VMEM((nc, 2, t // 2, CW), F32),
                pltpu.VMEM((nc, 2, t, CW), F32), pltpu.VMEM((nc, t, CW), F32), pltpu.VMEM((2, t, CW), BF),
                dma((el,)), dma, dma((2,)), dma((NW,)), dma((2,)), dma((nc,)), dma((nc,)), dma((nc, 2)), dma((nc, 2)),
                dma((nc, 2, 2)), dma((nc, 2, 2))],
            compiler_params=pltpu.CompilerParams(collective_id=1, has_side_effects=True, vmem_limit_bytes=VLIM),
        )(h, sh, meta, x, w2, ws2)

    return jax.shard_map(local, mesh=mesh,
                         in_specs=(P(ALL), P(ALL), P(ALL), P(EXP), P(EXP), P(EXP), P(), P(), P()),
                         out_specs=P(ALL), check_vma=False)
```

```python
import functools

import jax
import jax.numpy as jnp
from jax import lax
from jax.experimental import pallas as pl
from jax.experimental.pallas import tpu as pltpu
from jax.sharding import PartitionSpec as P

EXP = ("ey", "ex", "ec")
ALL = ("dp", "ey", "ex", "ec")
MESH = pl.DeviceIdType.MESH
ANY = pl.BlockSpec(memory_space=pl.ANY)
VM = pl.BlockSpec(memory_space=pltpu.VMEM)
BF = jnp.bfloat16
F32 = jnp.float32
VLIM = 67043328

NK = 4
NS = 4
CW = 256
NW = 12
LAG = 3
SLAB = 256


def place():
    ey, ex, ec = (lax.axis_index(a) for a in EXP)
    dev = {"x": dict(ey=ey, ex=1 - ex, ec=ec), "y": dict(ey=1 - ey, ex=ex, ec=ec), "p": dict(ey=ey, ex=ex, ec=1 - ec)}
    chip = {"o": ey * 2 + ex, "x": ey * 2 + 1 - ex, "y": (1 - ey) * 2 + ex, "d": (1 - ey) * 2 + 1 - ex}
    return ey, ex, ec, dev, chip


def silu_mul(a, b):
    return (a * jax.nn.sigmoid(a) * b).astype(BF)


def first(el, cap, ids_ref, gates_ref, x_ref, w1_ref, w3_ref, ws1_ref, ws3_ref, h_ref, sh_ref, meta_ref,
          xg, acc, wb, disp, xe, hst, mout, meta,
          xsem, wsem, osem, csem, msend, mrecv, ssem, rsem):
    ey, ex, ec, dev, chip = place()
    t = x_ref.shape[0]
    kw = x_ref.shape[1] // NK
    f = w1_ref.shape[2]
    half = t // 2
    lo, hi, full = pl.ds(0, half), pl.ds(half, half), pl.ds(0, t)
    mine = {c: ec * 4 + chip[c] for c in "oxyd"}
    theirs = {c: (1 - ec) * 4 + chip[c] for c in "oxyd"}
    nsh = 2 * NK
    nb = nsh + NK * el

    def block(b, go):
        slot = lax.rem(b, NS)

        @pl.when(b < nsh)
        def _():
            rows = pl.ds(pl.multiple_of(lax.rem(b, NK) * kw, kw), kw)
            cols = pl.ds(pl.multiple_of((b // NK) * f, 128), f)
            for i, w in enumerate((ws1_ref, ws3_ref)):
                go(pltpu.make_async_copy(w.at[rows, cols], wb.at[slot, :, pl.ds(i * f, f)], wsem.at[slot, i]))

        @pl.when((b >= nsh) & (b < nb))
        def _():
            q = b - nsh
            rows = pl.ds(pl.multiple_of((q // el) * kw, kw), kw)
            for i, w in enumerate((w1_ref, w3_ref)):
                go(pltpu.make_async_copy(w.at[lax.rem(q, el), rows], wb.at[slot, :, pl.ds(i * f, f)], wsem.at[slot, i]))

    def fetch(b):
        block(b, lambda c: c.start())

    def ready(b):
        block(b, lambda c: c.wait())

    for b in range(NS - 1):
        fetch(b)
    for k in range(NK):
        pltpu.make_async_copy(x_ref.at[:, pl.ds(k * kw, kw)], xg.at[k, mine["o"]], xsem.at[k]).start()

    ne = el * 8
    row = lax.broadcasted_iota(jnp.int32, (ne, t), 0)
    chosen = jnp.zeros((ne, t), F32)
    gate = jnp.zeros((ne, t), F32)
    for j in range(ids_ref.shape[0]):
        hit = ids_ref[j:j + 1, :] == row
        chosen = jnp.where(hit, 1.0, chosen)
        gate = jnp.where(hit, gates_ref[j:j + 1, :], gate)
    before = (lax.broadcasted_iota(jnp.int32, (t, t), 0) < lax.broadcasted_iota(jnp.int32, (t, t), 1))
    rank = jnp.dot(chosen.astype(BF), before.astype(F32).astype(BF), preferred_element_type=F32)
    rank = jnp.where(chosen > 0.0, rank, -1.0)
    for d in range(8):
        mout[d, 0:el, :] = rank[d * el:(d + 1) * el]
        mout[d, el:2 * el, :] = gate[d * el:(d + 1) * el]

    barrier = pltpu.get_barrier_semaphore()
    others = [(a, b, c) for a in (0, 1) for b in (0, 1) for c in (0, 1) if a + b + c]

    def flip(o):
        return [lax.rem(v + s, 2) for v, s in zip((ey, ex, ec), o)]

    for o in others:
        y2, x2, c2 = flip(o)
        pl.semaphore_signal(barrier, inc=1, device_id=dict(ey=y2, ex=x2, ec=c2), device_id_type=MESH)
    pl.semaphore_wait(barrier, len(others))

    for k in range(NK):
        pltpu.make_async_copy(x_ref.at[:, pl.ds(k * kw, kw)], xg.at[k, mine["o"]], xsem.at[k]).wait()

    def remote(k, src, rows, chan, to):
        ref = xg.at[k, src, rows]
        return pltpu.make_async_remote_copy(ref, ref, ssem.at[k, chan], rsem.at[k, chan], device_id=dev[to],
                                            device_id_type=MESH)

    def direct(k):
        for chan, to in enumerate("xyp"):
            remote(k, mine["o"], full, chan, to).start()

    def relay(k):
        remote(k, mine["x"], full, 0, "x").wait_recv()
        remote(k, mine["x"], lo, 3, "y").start()
        remote(k, mine["x"], full, 5, "p").start()
        remote(k, mine["y"], full, 1, "y").wait_recv()
        remote(k, mine["y"], hi, 4, "x").start()
        remote(k, mine["y"], full, 6, "p").start()

    def corner(k):
        remote(k, mine["d"], lo, 3, "y").wait_recv()
        remote(k, mine["d"], lo, 7, "p").start()
        remote(k, mine["d"], hi, 4, "x").wait_recv()
        remote(k, mine["d"], hi, 8, "p").start()

    def arrived(k):
        remote(k, theirs["o"], full, 2, "p").wait_recv()
        remote(k, theirs["x"], full, 5, "p").wait_recv()
        remote(k, theirs["y"], full, 6, "p").wait_recv()
        remote(k, theirs["d"], lo, 7, "p").wait_recv()
        remote(k, theirs["d"], hi, 8, "p").wait_recv()

    def sent(k):
        for src, rows, chan, to in ((mine["o"], full, 0, "x"), (mine["o"], full, 1, "y"), (mine["o"], full, 2, "p"),
                                    (mine["x"], lo, 3, "y"), (mine["y"], hi, 4, "x"), (mine["x"], full, 5, "p"),
                                    (mine["y"], full, 6, "p"), (mine["d"], lo, 7, "p"), (mine["d"], hi, 8, "p")):
            remote(k, src, rows, chan, to).wait_send()

    def mcopy(o, back=False):
        y2, x2, c2 = flip(o)
        num = c2 * 4 + y2 * 2 + x2
        idx = y2 * 4 + x2 * 2 + c2
        src, dst = (meta.at[num], num) if back else (mout.at[idx], mine["o"])
        return pltpu.make_async_remote_copy(src, meta.at[dst], msend.at[num], mrecv.at[dst],
                                            device_id=dict(ey=y2, ex=x2, ec=c2), device_id_type=MESH)

    for o in others:
        mcopy(o).start()
    direct(0)

    for hf in range(2):
        acc[0, 0:t, :] = jnp.zeros((t, 2 * f), F32)

        def body(k, _):
            b = hf * NK + k
            fetch(b + NS - 1)
            ready(b)
            acc[0, 0:t, :] += jnp.dot(xg[k, mine["o"]], wb[lax.rem(b, NS)], preferred_element_type=F32)
            return 0

        lax.fori_loop(0, NK, body, 0)
        hst[hf, 0:t, :] = silu_mul(acc[0, 0:t, 0:f], acc[0, 0:t, f:2 * f])
        pltpu.make_async_copy(hst.at[hf, 0:t], sh_ref.at[hf], osem.at[hf]).start()
        if hf == 0:
            relay(0)
            direct(1)


    meta[mine["o"]] = mout[ey * 4 + ex * 2 + ec]
    for o in others:
        mcopy(o, True).wait_recv()
    keep = pltpu.make_async_copy(meta, meta_ref, csem)
    keep.start()
    slots = lax.broadcasted_iota(jnp.int32, (cap, t), 0).astype(F32)

    def build(s, _):
        for e in range(el):
            sel = meta[s, e:e + 1, :] == slots
            disp[s, e * cap:(e + 1) * cap, :] = jnp.where(sel, 1.0, 0.0).astype(BF)
        return 0

    lax.fori_loop(0, 8, build, 0)

    def gather(k):
        def body(s, _):
            r = jnp.dot(disp[s], xg[k, s], preferred_element_type=F32).astype(BF)
            for e in range(el):
                xe[e, s] = r[e * cap:(e + 1) * cap]
            return 0

        lax.fori_loop(0, 8, body, 0)

    def product(k, e, use):
        b = nsh + k * el + e
        fetch(b + NS - 1)
        ready(b)
        slot = lax.rem(b, NS)
        u = xe[e].reshape(8 * cap, kw)

        def part(at):
            return jnp.dot(u, wb[slot, :, at], preferred_element_type=F32)
        use(part)

    def slabs(w):
        return [slice(i, min(i + w, 2 * f)) for i in range(0, 2 * f, w)]

    def start_acc(e, _):
        def use(part):
            for at in slabs(SLAB):
                acc[e, :, at] = part(at)
        product(0, e, use)
        return 0

    corner(0)
    arrived(0)
    gather(0)
    lax.fori_loop(0, el // 4, start_acc, 0)
    relay(1)
    direct(2)
    lax.fori_loop(el // 4, el - el // 4, start_acc, 0)
    corner(1)
    lax.fori_loop(el - el // 4, el, start_acc, 0)

    def more(k, _):
        arrived(k)
        gather(k)

        def add(e, _):
            def use(part):
                for at in slabs(SLAB):
                    acc[e, :, at] += part(at)
            product(k, e, use)
            return 0

        lax.fori_loop(0, el // 4, add, 0)
        relay(k + 1)

        @pl.when(k < NK - 2)
        def _():
            direct(k + 2)
        lax.fori_loop(el // 4, el - el // 4, add, 0)
        corner(k + 1)
        lax.fori_loop(el - el // 4, el, add, 0)
        return 0

    lax.fori_loop(1, NK - 1, more, 0)

    arrived(NK - 1)
    gather(NK - 1)
    for hf in range(2):
        pltpu.make_async_copy(hst.at[hf, 0:t], sh_ref.at[hf], osem.at[hf]).wait()

    def last(e, _):
        slot = lax.rem(e, 2)

        @pl.when(e >= 2)
        def _():
            pltpu.make_async_copy(hst.at[slot], h_ref.at[e - 2], osem.at[slot]).wait()

        def use(part):
            nt = f // 128
            live = {}
            order = [nt // 2] + [v for i in range(nt // 2) for v in (i, nt // 2 + 1 + i)]
            for i in order:
                at = slice(i * 256, i * 256 + 256)
                d = acc[e, :, at] + part(at)
                for j in (2 * i, 2 * i + 1):
                    live[j] = d[:, (j - 2 * i) * 128:(j - 2 * i) * 128 + 128]
                    if j == nt - 1:
                        acc[e, :, j * 128:j * 128 + 128] = live.pop(j)
                for j in [v for v in live if v < nt and v + nt in live]:
                    hst[slot, :, j * 128:j * 128 + 128] = silu_mul(live.pop(j), live.pop(j + nt))
                if 2 * nt - 1 in live:
                    j = nt - 1
                    hst[slot, :, j * 128:j * 128 + 128] = silu_mul(acc[e, :, j * 128:j * 128 + 128], live.pop(2 * nt - 1))
        product(NK - 1, e, use)
        pltpu.make_async_copy(hst.at[slot], h_ref.at[e], osem.at[slot]).start()
        return 0

    lax.fori_loop(0, el, last, 0)

    keep.wait()
    for e in (el - 2, el - 1):
        pltpu.make_async_copy(hst.at[e % 2], h_ref.at[e], osem.at[e % 2]).wait()
    for o in others:
        mcopy(o).wait_send()
    for k in range(NK):
        sent(k)


def second(el, cap, h_ref, sh_ref, meta_ref, x_ref, w2_ref, ws2_ref, y_ref,
           hv, shv, wcv, meta, xv, wb, o3, part, pr, dr, fr, res, yst,
           hsem, csem, xsem, wsem, ysem, psend, precv, dsend, drecv, fsend, frecv):
    ey, ex, ec, dev, chip = place()
    t, hd = x_ref.shape
    nc = hd // CW
    f = w2_ref.shape[1]
    half = t // 2
    lo, hi = pl.ds(0, half), pl.ds(half, half)
    per = el + 2
    nb = nc * per
    n = el * cap

    def block(b, go):
        c, j = b // per, lax.rem(b, per)
        cols = pl.ds(pl.multiple_of(c * CW, CW), CW)
        slot = lax.rem(b, NW)

        @pl.when((j < el) & (b < nb))
        def _():
            go(pltpu.make_async_copy(w2_ref.at[j, :, cols], wb.at[slot], wsem.at[slot]))

        @pl.when((j >= el) & (b < nb))
        def _():
            rows = pl.ds(pl.multiple_of((j - el) * f, 128), f)
            go(pltpu.make_async_copy(ws2_ref.at[rows, cols], wb.at[slot], wsem.at[slot]))

    def fetch(b):
        block(b, lambda c: c.start())

    def ready(b):
        block(b, lambda c: c.wait())

    def hcopy(e):
        return pltpu.make_async_copy(h_ref.at[e], hv.at[e], hsem.at[e])

    hcopy(0).start()
    for b in range(NW - 1):
        fetch(b)
    for e in range(1, el):
        hcopy(e).start()
    loads = [pltpu.make_async_copy(sh_ref, shv, xsem.at[0]), pltpu.make_async_copy(x_ref, xv, xsem.at[1]),
             ]
    m = pltpu.make_async_copy(meta_ref, meta, csem)
    m.start()
    for c in loads:
        c.start()

    barrier = pltpu.get_barrier_semaphore()
    for to in "xyp":
        pl.semaphore_signal(barrier, inc=1, device_id=dev[to], device_id_type=MESH)
    pl.semaphore_wait(barrier, 3)

    m.wait()
    slots = lax.broadcasted_iota(jnp.int32, (cap, t), 0).astype(F32)

    def build(s, _):
        parts = [jnp.where(meta[s, e:e + 1, :] == slots, meta[s, el + e:el + e + 1, :], 0.0) for e in range(el)]
        w = jnp.concatenate(parts, axis=0).T
        for i in range(3):
            p = w.astype(BF)
            wcv[s, :, i * n:(i + 1) * n] = p
            w = w - p.astype(F32)
        return 0

    lax.fori_loop(0, 8, build, 0)

    def swap(c):
        return pltpu.make_async_remote_copy(part.at[1, c], pr.at[c], psend.at[c], precv.at[c], device_id=dev["p"],
                                            device_id_type=MESH)

    def corner(c, i):
        src = part.at[0, c, chip["d"], (lo, hi)[i]]
        return pltpu.make_async_remote_copy(src, dr.at[c, i], dsend.at[c, i], drecv.at[c, i], device_id=dev["xy"[i]],
                                            device_id_type=MESH)

    def final(c, i, rows):
        src = part.at[0, c, chip["xy"[i]], (lo, hi)[rows]]
        return pltpu.make_async_remote_copy(src, fr.at[c, i, (lo, hi)[rows]], fsend.at[c, i, rows], frecv.at[c, i, rows],
                                            device_id=dev["xy"[i]], device_id_type=MESH)

    def weigh(c, g):
        core = ec if g == 0 else 1 - ec

        def body(ch, _):
            s = core * 4 + ch
            part[g, c, ch] = jnp.dot(wcv[s], o3[s], preferred_element_type=F32)
            return 0

        lax.fori_loop(0, 4, body, 0)

    def compute(c):
        def expert(e, _):
            b = c * per + e
            fetch(b + NW - 1)

            @pl.when(c == 0)
            def _():
                hcopy(e).wait()
            ready(b)
            o = jnp.dot(hv[e], wb[lax.rem(b, NW)], preferred_element_type=F32).astype(BF)
            for s in range(8):
                for i in range(3):
                    o3[s, pl.ds(pl.multiple_of(i * n + e * cap, 16), cap), :] = o[s * cap:(s + 1) * cap]
            return 0

        lax.fori_loop(0, el, expert, 0)

        weigh(c, 1)
        swap(c).start()
        weigh(c, 0)

    def shared(c):
        @pl.when(c == 0)
        def _():
            for d in loads:
                d.wait()
        s = None
        for i in range(2):
            b = c * per + el + i
            fetch(b + NW - 1)
            ready(b)
            p = jnp.dot(shv[i], wb[lax.rem(b, NW)], preferred_element_type=F32)
            s = p if s is None else s + p
        cols = pl.ds(pl.multiple_of(c * CW, CW), CW)
        res[c] = xv[:, cols].astype(F32) + s.astype(BF).astype(F32)

    def stage1(c):
        swap(c).wait_recv()
        for ch in "dxyo":
            part[0, c, chip[ch]] += pr[c, chip[ch]]
        corner(c, 0).start()
        corner(c, 1).start()
        final(c, 0, 0).start()
        final(c, 1, 1).start()

    def stage2(c):
        corner(c, 0).wait_recv()
        part[0, c, chip["y"], 0:half] += dr[c, 0]
        corner(c, 1).wait_recv()
        part[0, c, chip["x"], half:t] += dr[c, 1]
        final(c, 1, 0).start()
        final(c, 0, 1).start()

    def ycopy(c):
        cols = pl.ds(pl.multiple_of(c * CW, CW), CW)
        return pltpu.make_async_copy(yst.at[lax.rem(c, 2)], y_ref.at[:, cols], ysem.at[lax.rem(c, 2)])

    def stage3(c):
        for i in range(2):
            for rows in range(2):
                final(c, i, rows).wait_recv()

        @pl.when(c >= 2)
        def _():
            ycopy(c - 2).wait()
        yst[lax.rem(c, 2)] = (res[c] + (part[0, c, chip["o"]] + fr[c, 0] + fr[c, 1])).astype(BF)
        ycopy(c).start()

    def step(c, _):
        @pl.when(c < nc)
        def _():
            compute(c)
            shared(c)
            stage1(c)

        @pl.when((c >= 1) & (c < nc + 1))
        def _():
            stage2(c - 1)

        @pl.when(c >= LAG)
        def _():
            stage3(c - LAG)
        return 0

    lax.fori_loop(0, nc + LAG, step, 0)
    for c in (nc - 2, nc - 1):
        ycopy(c).wait()

    def drain(c, _):
        swap(c).wait_send()
        for i in range(2):
            corner(c, i).wait_send()
            for rows in range(2):
                final(c, i, rows).wait_send()
        return 0

    lax.fori_loop(0, nc, drain, 0)


def solution(mesh):
    pg = mesh.shape["ey"] * mesh.shape["ex"] * mesh.shape["ec"]

    def local(x, ids, gates, w1, w3, w2, ws1, ws3, ws2):
        t, hd = x.shape
        top = ids.shape[1]
        el, _, f = w1.shape
        ne = el * pg
        cap = min(t, 2 * ((t * top + ne - 1) // ne))
        n = el * cap
        kw = hd // NK
        nc = hd // CW
        dma = pltpu.SemaphoreType.DMA
        h, sh, meta = pl.pallas_call(
            functools.partial(first, el, cap),
            out_shape=(jax.ShapeDtypeStruct((el, pg * cap, f), BF), jax.ShapeDtypeStruct((2, t, f), BF),
                       jax.ShapeDtypeStruct((pg, 2 * el, t), F32)),
            in_specs=[VM, VM] + [ANY] * 5, out_specs=(ANY,) * 3,
            scratch_shapes=[
                pltpu.VMEM((NK, pg, t, kw), BF), pltpu.VMEM((el, pg * cap, 2 * f), F32), pltpu.VMEM((NS, kw, 2 * f), BF),
                pltpu.VMEM((pg, n, t), BF), pltpu.VMEM((el, pg, cap, kw), BF), pltpu.VMEM((2, pg * cap, f), BF),
                pltpu.VMEM((pg, 2 * el, t), F32), pltpu.VMEM((pg, 2 * el, t), F32),
                dma((NK,)), dma((NS, 2)), dma((2,)), dma, dma((8,)), dma((8,)), dma((NK, 9)), dma((NK, 9))],
            compiler_params=pltpu.CompilerParams(collective_id=0, has_side_effects=True, vmem_limit_bytes=VLIM),
        )(ids.T, gates.T, x, w1, w3, ws1, ws3)
        return pl.pallas_call(
            functools.partial(second, el, cap),
            out_shape=jax.ShapeDtypeStruct((t, hd), BF),
            in_specs=[ANY] * 6, out_specs=ANY,
            scratch_shapes=[
                pltpu.VMEM((el, pg * cap, f), BF), pltpu.VMEM((2, t, f), BF), pltpu.VMEM((pg, t, 3 * n), BF), pltpu.VMEM((pg, 2 * el, t), F32),
                pltpu.VMEM((t, hd), BF), pltpu.VMEM((NW, f, CW), BF), pltpu.VMEM((pg, 3 * n, CW), BF),
                pltpu.VMEM((2, nc, 4, t, CW), F32), pltpu.VMEM((nc, 4, t, CW), F32), pltpu.VMEM((nc, 2, t // 2, CW), F32),
                pltpu.VMEM((nc, 2, t, CW), F32), pltpu.VMEM((nc, t, CW), F32), pltpu.VMEM((2, t, CW), BF),
                dma((el,)), dma, dma((2,)), dma((NW,)), dma((2,)), dma((nc,)), dma((nc,)), dma((nc, 2)), dma((nc, 2)),
                dma((nc, 2, 2)), dma((nc, 2, 2))],
            compiler_params=pltpu.CompilerParams(collective_id=1, has_side_effects=True, vmem_limit_bytes=VLIM),
        )(h, sh, meta, x, w2, ws2)

    return jax.shard_map(local, mesh=mesh,
                         in_specs=(P(ALL), P(ALL), P(ALL), P(EXP), P(EXP), P(EXP), P(), P(), P()),
                         out_specs=P(ALL), check_vma=False)
```

```python
import functools

import jax
import jax.numpy as jnp
from jax import lax
from jax.experimental import pallas as pl
from jax.experimental.pallas import tpu as pltpu
from jax.sharding import PartitionSpec as P

EXP = ("ey", "ex", "ec")
ALL = ("dp", "ey", "ex", "ec")
MESH = pl.DeviceIdType.MESH
ANY = pl.BlockSpec(memory_space=pl.ANY)
VM = pl.BlockSpec(memory_space=pltpu.VMEM)
BF = jnp.bfloat16
F32 = jnp.float32
VLIM = 67043328

NK = 4
NS = 5
CW = 256
NW = 8
SLAB = 256


def place():
    ey, ex, ec = (lax.axis_index(a) for a in EXP)
    dev = {"x": dict(ey=ey, ex=1 - ex, ec=ec), "y": dict(ey=1 - ey, ex=ex, ec=ec), "p": dict(ey=ey, ex=ex, ec=1 - ec)}
    chip = {"o": ey * 2 + ex, "x": ey * 2 + 1 - ex, "y": (1 - ey) * 2 + ex, "d": (1 - ey) * 2 + 1 - ex}
    return ey, ex, ec, dev, chip


def silu_mul(a, b):
    return (a * jax.nn.sigmoid(a) * b).astype(BF)


def first(el, cap, ids_ref, gates_ref, x_ref, w1_ref, w3_ref, ws1_ref, ws3_ref, h_ref, sh_ref, meta_ref,
          xg, acc, wb, disp, xe, hst, mout, meta,
          xsem, wsem, osem, csem, msend, mrecv, ssem, rsem):
    ey, ex, ec, dev, chip = place()
    t = x_ref.shape[0]
    kw = x_ref.shape[1] // NK
    f = w1_ref.shape[2]
    half = t // 2
    lo, hi, full = pl.ds(0, half), pl.ds(half, half), pl.ds(0, t)
    mine = {c: ec * 4 + chip[c] for c in "oxyd"}
    theirs = {c: (1 - ec) * 4 + chip[c] for c in "oxyd"}
    nsh = 2 * NK
    nb = nsh + NK * el

    def block(b, go):
        slot = lax.rem(b, NS)

        @pl.when(b < nsh)
        def _():
            rows = pl.ds(pl.multiple_of(lax.rem(b, NK) * kw, kw), kw)
            cols = pl.ds(pl.multiple_of((b // NK) * f, 128), f)
            for i, w in enumerate((ws1_ref, ws3_ref)):
                go(pltpu.make_async_copy(w.at[rows, cols], wb.at[slot, :, pl.ds(i * f, f)], wsem.at[slot, i]))

        @pl.when((b >= nsh) & (b < nb))
        def _():
            q = b - nsh
            rows = pl.ds(pl.multiple_of((q // el) * kw, kw), kw)
            for i, w in enumerate((w1_ref, w3_ref)):
                go(pltpu.make_async_copy(w.at[lax.rem(q, el), rows], wb.at[slot, :, pl.ds(i * f, f)], wsem.at[slot, i]))

    def fetch(b):
        block(b, lambda c: c.start())

    def ready(b):
        block(b, lambda c: c.wait())

    def pair(b):
        for j in range(2):
            fetch(b + NS - 2 + j)
        for j in range(2):
            ready(b + j)

    for b in range(NS - 2):
        fetch(b)
    for k in range(NK):
        pltpu.make_async_copy(x_ref.at[:, pl.ds(k * kw, kw)], xg.at[k, mine["o"]], xsem.at[k]).start()

    ne = el * 8
    row = lax.broadcasted_iota(jnp.int32, (ne, t), 0)
    chosen = jnp.zeros((ne, t), F32)
    gate = jnp.zeros((ne, t), F32)
    for j in range(ids_ref.shape[0]):
        hit = ids_ref[j:j + 1, :] == row
        chosen = jnp.where(hit, 1.0, chosen)
        gate = jnp.where(hit, gates_ref[j:j + 1, :], gate)
    before = (lax.broadcasted_iota(jnp.int32, (t, t), 0) < lax.broadcasted_iota(jnp.int32, (t, t), 1))
    rank = jnp.dot(chosen.astype(BF), before.astype(F32).astype(BF), preferred_element_type=F32)
    rank = jnp.where(chosen > 0.0, rank, -1.0)
    for d in range(8):
        mout[d, 0:el, :] = rank[d * el:(d + 1) * el]
        mout[d, el:2 * el, :] = gate[d * el:(d + 1) * el]

    barrier = pltpu.get_barrier_semaphore()
    others = [(a, b, c) for a in (0, 1) for b in (0, 1) for c in (0, 1) if a + b + c]

    def flip(o):
        return [lax.rem(v + s, 2) for v, s in zip((ey, ex, ec), o)]

    for o in others:
        y2, x2, c2 = flip(o)
        pl.semaphore_signal(barrier, inc=1, device_id=dict(ey=y2, ex=x2, ec=c2), device_id_type=MESH)
    pl.semaphore_wait(barrier, len(others))

    for k in range(NK):
        pltpu.make_async_copy(x_ref.at[:, pl.ds(k * kw, kw)], xg.at[k, mine["o"]], xsem.at[k]).wait()

    def remote(k, src, rows, chan, to):
        ref = xg.at[k, src, rows]
        return pltpu.make_async_remote_copy(ref, ref, ssem.at[k, chan], rsem.at[k, chan], device_id=dev[to],
                                            device_id_type=MESH)

    def direct(k):
        for chan, to in enumerate("xyp"):
            remote(k, mine["o"], full, chan, to).start()

    def relay(k):
        remote(k, mine["x"], full, 0, "x").wait_recv()
        remote(k, mine["x"], lo, 3, "y").start()
        remote(k, mine["x"], full, 5, "p").start()
        remote(k, mine["y"], full, 1, "y").wait_recv()
        remote(k, mine["y"], hi, 4, "x").start()
        remote(k, mine["y"], full, 6, "p").start()

    def corner(k):
        remote(k, mine["d"], lo, 3, "y").wait_recv()
        remote(k, mine["d"], lo, 7, "p").start()
        remote(k, mine["d"], hi, 4, "x").wait_recv()
        remote(k, mine["d"], hi, 8, "p").start()

    def arrived(k):
        remote(k, theirs["o"], full, 2, "p").wait_recv()
        remote(k, theirs["x"], full, 5, "p").wait_recv()
        remote(k, theirs["y"], full, 6, "p").wait_recv()
        remote(k, theirs["d"], lo, 7, "p").wait_recv()
        remote(k, theirs["d"], hi, 8, "p").wait_recv()

    def sent(k):
        for src, rows, chan, to in ((mine["o"], full, 0, "x"), (mine["o"], full, 1, "y"), (mine["o"], full, 2, "p"),
                                    (mine["x"], lo, 3, "y"), (mine["y"], hi, 4, "x"), (mine["x"], full, 5, "p"),
                                    (mine["y"], full, 6, "p"), (mine["d"], lo, 7, "p"), (mine["d"], hi, 8, "p")):
            remote(k, src, rows, chan, to).wait_send()

    def mcopy(o, back=False):
        y2, x2, c2 = flip(o)
        num = c2 * 4 + y2 * 2 + x2
        idx = y2 * 4 + x2 * 2 + c2
        src, dst = (meta.at[num], num) if back else (mout.at[idx], mine["o"])
        return pltpu.make_async_remote_copy(src, meta.at[dst], msend.at[num], mrecv.at[dst],
                                            device_id=dict(ey=y2, ex=x2, ec=c2), device_id_type=MESH)

    for o in others:
        mcopy(o).start()
    direct(0)

    for hf in range(2):
        acc[0, 0:t, :] = jnp.zeros((t, 2 * f), F32)

        def body(i, _):
            b = hf * NK + 2 * i
            pair(b)
            for at in [slice(v, v + SLAB) for v in range(0, 2 * f, SLAB)]:
                d = [jnp.dot(xg[2 * i + j, mine["o"]], wb[lax.rem(b + j, NS), :, at], preferred_element_type=F32)
                     for j in range(2)]
                acc[0, 0:t, at] += d[0] + d[1]
            return 0

        lax.fori_loop(0, NK // 2, body, 0)
        for v in range(0, f, 128):
            hst[hf, 0:t, v:v + 128] = silu_mul(acc[0, 0:t, v:v + 128], acc[0, 0:t, f + v:f + v + 128])
        pltpu.make_async_copy(hst.at[hf, 0:t], sh_ref.at[hf], osem.at[hf]).start()
        if hf == 0:
            relay(0)
            direct(1)


    meta[mine["o"]] = mout[ey * 4 + ex * 2 + ec]
    for o in others:
        mcopy(o, True).wait_recv()
    keep = pltpu.make_async_copy(meta, meta_ref, csem)
    keep.start()
    slots = lax.broadcasted_iota(jnp.int32, (cap, t), 0).astype(F32)

    def build(s, _):
        for e in range(el):
            sel = meta[s, e:e + 1, :] == slots
            disp[s, e * cap:(e + 1) * cap, :] = jnp.where(sel, 1.0, 0.0).astype(BF)
        return 0

    lax.fori_loop(0, 8, build, 0)

    def gather(k):
        def body(s, _):
            r = jnp.dot(disp[s], xg[k, s], preferred_element_type=F32).astype(BF)
            for e in range(el):
                xe[e, s] = r[e * cap:(e + 1) * cap]
            return 0

        lax.fori_loop(0, 8, body, 0)

    def products(k, i, use):
        b = nsh + k * el + 2 * i
        pair(b)
        for j in range(2):
            slot = lax.rem(b + j, NS)
            u = xe[2 * i + j].reshape(8 * cap, kw)
            use(2 * i + j, lambda at, u=u, slot=slot: jnp.dot(u, wb[slot, :, at], preferred_element_type=F32))

    def slabs(w):
        return [slice(i, min(i + w, 2 * f)) for i in range(0, 2 * f, w)]

    def start_acc(i, _):
        def use(e, part):
            for at in slabs(SLAB):
                acc[e, :, at] = part(at)
        products(0, i, use)
        return 0

    corner(0)
    arrived(0)
    gather(0)
    lax.fori_loop(0, el // 8, start_acc, 0)
    relay(1)
    direct(2)
    lax.fori_loop(el // 8, el // 2 - el // 8, start_acc, 0)
    corner(1)
    lax.fori_loop(el // 2 - el // 8, el // 2, start_acc, 0)

    def more(k, _):
        arrived(k)
        gather(k)

        def add(i, _):
            def use(e, part):
                for at in slabs(SLAB):
                    acc[e, :, at] += part(at)
            products(k, i, use)
            return 0

        lax.fori_loop(0, el // 8, add, 0)
        relay(k + 1)

        @pl.when(k < NK - 2)
        def _():
            direct(k + 2)
        lax.fori_loop(el // 8, el // 2 - el // 8, add, 0)
        corner(k + 1)
        lax.fori_loop(el // 2 - el // 8, el // 2, add, 0)
        return 0

    lax.fori_loop(1, NK - 1, more, 0)

    arrived(NK - 1)
    gather(NK - 1)
    for hf in range(2):
        pltpu.make_async_copy(hst.at[hf, 0:t], sh_ref.at[hf], osem.at[hf]).wait()

    def last(i, _):
        @pl.when(i >= 1)
        def _():
            for j in range(2):
                pltpu.make_async_copy(hst.at[j], h_ref.at[2 * i - 2 + j], osem.at[j]).wait()

        def use(e, part):
            slot = lax.rem(e, 2)
            nt = f // 128
            live = {}
            order = [nt // 2] + [v for i in range(nt // 2) for v in (i, nt // 2 + 1 + i)]
            for i in order:
                at = slice(i * 256, i * 256 + 256)
                d = acc[e, :, at] + part(at)
                for j in (2 * i, 2 * i + 1):
                    live[j] = d[:, (j - 2 * i) * 128:(j - 2 * i) * 128 + 128]
                    if j == nt - 1:
                        acc[e, :, j * 128:j * 128 + 128] = live.pop(j)
                for j in [v for v in live if v < nt and v + nt in live]:
                    hst[slot, :, j * 128:j * 128 + 128] = silu_mul(live.pop(j), live.pop(j + nt))
                if 2 * nt - 1 in live:
                    j = nt - 1
                    hst[slot, :, j * 128:j * 128 + 128] = silu_mul(acc[e, :, j * 128:j * 128 + 128], live.pop(2 * nt - 1))
            pltpu.make_async_copy(hst.at[slot], h_ref.at[e], osem.at[slot]).start()
        products(NK - 1, i, use)
        return 0

    lax.fori_loop(0, el // 2, last, 0)

    keep.wait()
    for e in (el - 2, el - 1):
        pltpu.make_async_copy(hst.at[e % 2], h_ref.at[e], osem.at[e % 2]).wait()
    for o in others:
        mcopy(o).wait_send()
    for k in range(NK):
        sent(k)


def second(el, cap, h_ref, sh_ref, meta_ref, x_ref, w2_ref, ws2_ref, y_ref,
           hv, shv, wcv, meta, xv, wb, o3, part, give, pr, sb, rv, res, yst,
           hsem, csem, xsem, wsem, ysem, psend, precv, ssem, rsem, esend, erecv):
    ey, ex, ec, dev, chip = place()
    t, hd = x_ref.shape
    nc = hd // CW
    f = w2_ref.shape[1]
    half = t // 2
    lo, hi = pl.ds(0, half), pl.ds(half, half)
    per = el + 2
    nb = nc * per
    n = el * cap

    def block(b, go):
        c, j = b // per, lax.rem(b, per)
        cols = pl.ds(pl.multiple_of(c * CW, CW), CW)
        slot = lax.rem(b, NW)

        @pl.when((j < el) & (b < nb))
        def _():
            go(pltpu.make_async_copy(w2_ref.at[j, :, cols], wb.at[slot], wsem.at[slot]))

        @pl.when((j >= el) & (b < nb))
        def _():
            rows = pl.ds(pl.multiple_of((j - el) * f, 128), f)
            go(pltpu.make_async_copy(ws2_ref.at[rows, cols], wb.at[slot], wsem.at[slot]))

    def fetch(b):
        block(b, lambda c: c.start())

    def ready(b):
        block(b, lambda c: c.wait())

    def hcopy(e):
        return pltpu.make_async_copy(h_ref.at[e], hv.at[e], hsem.at[e])

    hcopy(0).start()
    for b in range(NW - 1):
        fetch(b)
    for e in range(1, el):
        hcopy(e).start()
    loads = [pltpu.make_async_copy(sh_ref, shv, xsem.at[0]), pltpu.make_async_copy(x_ref, xv, xsem.at[1]),
             ]
    m = pltpu.make_async_copy(meta_ref, meta, csem)
    m.start()

    barrier = pltpu.get_barrier_semaphore()
    for to in "xyp":
        pl.semaphore_signal(barrier, inc=1, device_id=dev[to], device_id_type=MESH)
    pl.semaphore_wait(barrier, 3)

    m.wait()
    slots = lax.broadcasted_iota(jnp.int32, (cap, t), 0).astype(F32)

    def build(s, _):
        parts = [jnp.where(meta[s, e:e + 1, :] == slots, meta[s, el + e:el + e + 1, :], 0.0) for e in range(el)]
        w = jnp.concatenate(parts, axis=0).T
        for i in range(3):
            p = w.astype(BF)
            wcv[s, :, i * n:(i + 1) * n] = p
            w = w - p.astype(F32)
        return 0

    lax.fori_loop(0, 8, build, 0)

    def swap(c, i):
        ch = chip["dxyo"[i]]
        return pltpu.make_async_remote_copy(give.at[lax.rem(c, 2), ch], pr.at[c, ch], psend.at[c, i], precv.at[c, i],
                                            device_id=dev["p"], device_id_type=MESH)

    def ship(c, i, a, b, k=None):
        send, recv = (ssem.at[c, i], rsem.at[c, i]) if k is None else (esend.at[k, i], erecv.at[k, i])
        at = pl.ds(a, b - a)
        return pltpu.make_async_remote_copy(sb.at[i, c, at], rv.at[i, c, at], send, recv, device_id=dev["xy"[i]],
                                            device_id_type=MESH)

    def dispatch(c, op):
        for i in range(2):
            pl.when(c < 2)(lambda: op(ship(c, i, 0, 2)))
            pl.when((c >= 2) & (c < nc - 1))(lambda: op(ship(c, i, 0, 3)))
            pl.when(c == nc - 1)(lambda: op(ship(c, i, 0, 1)))

    def weigh(c, ch, core):
        s = core * 4 + chip[ch]
        return jnp.dot(wcv[s], o3[s], preferred_element_type=F32)

    def compute(c):
        def expert(e, _):
            b = c * per + e
            fetch(b + NW - 1)

            @pl.when(c == 0)
            def _():
                hcopy(e).wait()
            ready(b)
            o = jnp.dot(hv[e], wb[lax.rem(b, NW)], preferred_element_type=F32).astype(BF)
            for s in range(8):
                for i in range(3):
                    o3[s, pl.ds(pl.multiple_of(i * n + e * cap, 16), cap), :] = o[s * cap:(s + 1) * cap]
            return 0

        lax.fori_loop(0, el, expert, 0)

        @pl.when(c == 0)
        def _():
            for d in loads:
                d.start()

        @pl.when(c >= 2)
        def _():
            for i in range(4):
                swap(c - 2, i).wait_send()
        for i, ch in enumerate("dxyo"):
            give[lax.rem(c, 2), chip[ch]] = weigh(c, ch, 1 - ec)
            swap(c, i).start()
        for ch in "dxyo":
            part[c, chip[ch]] = weigh(c, ch, ec)

    def shared(c):
        @pl.when(c == 0)
        def _():
            for d in loads:
                d.wait()
        s = None
        for i in range(2):
            b = c * per + el + i
            fetch(b + NW - 1)
            ready(b)
            p = jnp.dot(shv[i], wb[lax.rem(b, NW)], preferred_element_type=F32)
            s = p if s is None else s + p
        cols = pl.ds(pl.multiple_of(c * CW, CW), CW)
        res[c] = xv[:, cols].astype(F32) + s.astype(BF).astype(F32)

    def stage1(c):
        d, x, y, o = (chip[ch] for ch in "dxyo")
        swap(c, 0).wait_recv()
        sb[0, c, 0] = part[c, d, 0:half] + pr[c, d, 0:half]
        sb[1, c, 0] = part[c, d, half:t] + pr[c, d, half:t]
        swap(c, 1).wait_recv()
        sb[0, c, 1] = part[c, x, 0:half] + pr[c, x, 0:half]
        part[c, x, half:t] += pr[c, x, half:t]
        swap(c, 2).wait_recv()
        part[c, y, 0:half] += pr[c, y, 0:half]
        sb[1, c, 1] = part[c, y, half:t] + pr[c, y, half:t]
        swap(c, 3).wait_recv()
        part[c, o] += pr[c, o]

    def stage2(c, into):
        sb[1, into, 2] = part[c, chip["y"], 0:half] + rv[0, c, 0]
        sb[0, into, 2] = part[c, chip["x"], half:t] + rv[1, c, 0]

    def ycopy(c):
        cols = pl.ds(pl.multiple_of(c * CW, CW), CW)
        return pltpu.make_async_copy(yst.at[lax.rem(c, 2)], y_ref.at[:, cols], ysem.at[lax.rem(c, 2)])

    def stage3(c):
        n2 = lax.rem(c + 2, nc)

        @pl.when(c >= 2)
        def _():
            ycopy(c - 2).wait()
        own = res[c] + part[c, chip["o"]]
        yst[lax.rem(c, 2), 0:half] = (own[0:half] + rv[0, c, 1] + rv[1, n2, 2]).astype(BF)
        yst[lax.rem(c, 2), half:t] = (own[half:t] + rv[0, n2, 2] + rv[1, c, 1]).astype(BF)
        ycopy(c).start()

    def step(c, _):
        compute(c)

        @pl.when(c >= 2)
        def _():
            dispatch(c - 2, lambda d: d.wait_recv())
            stage2(c - 2, c)
        stage1(c)
        dispatch(c, lambda d: d.start())

        @pl.when(c == nc - 1)
        def _():
            for i in range(2):
                ship(nc - 1, i, 1, 3, 0).start()
        shared(c)

        @pl.when(c >= 4)
        def _():
            stage3(c - 4)
        return 0

    lax.fori_loop(0, nc, step, 0)
    for i in range(2):
        ship(nc - 2, i, 0, 3).wait_recv()
    stage2(nc - 2, 0)
    for i in range(2):
        ship(0, i, 2, 3, 1).start()
    stage3(nc - 4)
    for i in range(2):
        ship(nc - 1, i, 0, 1).wait_recv()
    stage2(nc - 1, 1)
    for i in range(2):
        ship(1, i, 2, 3, 2).start()
    for i in range(2):
        ship(nc - 1, i, 1, 3, 0).wait_recv()
    stage3(nc - 3)
    for k in range(2):
        for i in range(2):
            ship(k, i, 2, 3, k + 1).wait_recv()
        stage3(nc - 2 + k)
    for c in (nc - 2, nc - 1):
        ycopy(c).wait()
        for i in range(4):
            swap(c, i).wait_send()
    for i in range(2):
        ship(nc - 1, i, 1, 3, 0).wait_send()
        for k in range(2):
            ship(k, i, 2, 3, k + 1).wait_send()

    def drain(c, _):
        dispatch(c, lambda d: d.wait_send())
        return 0

    lax.fori_loop(0, nc, drain, 0)


def solution(mesh):
    pg = mesh.shape["ey"] * mesh.shape["ex"] * mesh.shape["ec"]

    def local(x, ids, gates, w1, w3, w2, ws1, ws3, ws2):
        t, hd = x.shape
        top = ids.shape[1]
        el, _, f = w1.shape
        ne = el * pg
        cap = min(t, 2 * ((t * top + ne - 1) // ne))
        n = el * cap
        kw = hd // NK
        nc = hd // CW
        dma = pltpu.SemaphoreType.DMA
        h, sh, meta = pl.pallas_call(
            functools.partial(first, el, cap),
            out_shape=(jax.ShapeDtypeStruct((el, pg * cap, f), BF), jax.ShapeDtypeStruct((2, t, f), BF),
                       jax.ShapeDtypeStruct((pg, 2 * el, t), F32)),
            in_specs=[VM, VM] + [ANY] * 5, out_specs=(ANY,) * 3,
            scratch_shapes=[
                pltpu.VMEM((NK, pg, t, kw), BF), pltpu.VMEM((el, pg * cap, 2 * f), F32), pltpu.VMEM((NS, kw, 2 * f), BF),
                pltpu.VMEM((pg, n, t), BF), pltpu.VMEM((el, pg, cap, kw), BF), pltpu.VMEM((2, pg * cap, f), BF),
                pltpu.VMEM((pg, 2 * el, t), F32), pltpu.VMEM((pg, 2 * el, t), F32),
                dma((NK,)), dma((NS, 2)), dma((2,)), dma, dma((8,)), dma((8,)), dma((NK, 9)), dma((NK, 9))],
            compiler_params=pltpu.CompilerParams(collective_id=0, has_side_effects=True, vmem_limit_bytes=VLIM),
        )(ids.T, gates.T, x, w1, w3, ws1, ws3)
        return pl.pallas_call(
            functools.partial(second, el, cap),
            out_shape=jax.ShapeDtypeStruct((t, hd), BF),
            in_specs=[ANY] * 6, out_specs=ANY,
            scratch_shapes=[
                pltpu.VMEM((el, pg * cap, f), BF), pltpu.VMEM((2, t, f), BF), pltpu.VMEM((pg, t, 3 * n), BF), pltpu.VMEM((pg, 2 * el, t), F32),
                pltpu.VMEM((t, hd), BF), pltpu.VMEM((NW, f, CW), BF), pltpu.VMEM((pg, 3 * n, CW), BF),
                pltpu.VMEM((nc, 4, t, CW), F32), pltpu.VMEM((2, 4, t, CW), F32), pltpu.VMEM((nc, 4, t, CW), F32),
                pltpu.VMEM((2, nc, 3, t // 2, CW), F32), pltpu.VMEM((2, nc, 3, t // 2, CW), F32),
                pltpu.VMEM((nc, t, CW), F32), pltpu.VMEM((2, t, CW), BF),
                dma((el,)), dma, dma((2,)), dma((NW,)), dma((2,)), dma((nc, 4)), dma((nc, 4)), dma((nc, 2)), dma((nc, 2)),
                dma((3, 2)), dma((3, 2))],
            compiler_params=pltpu.CompilerParams(collective_id=1, has_side_effects=True, vmem_limit_bytes=VLIM),
        )(h, sh, meta, x, w2, ws2)

    return jax.shard_map(local, mesh=mesh,
                         in_specs=(P(ALL), P(ALL), P(ALL), P(EXP), P(EXP), P(EXP), P(), P(), P()),
                         out_specs=P(ALL), check_vma=False)
```

```python
import functools

import jax
import jax.numpy as jnp
from jax import lax
from jax.experimental import pallas as pl
from jax.experimental.pallas import tpu as pltpu
from jax.sharding import PartitionSpec as P

EXP = ("ey", "ex", "ec")
ALL = ("dp", "ey", "ex", "ec")
MESH = pl.DeviceIdType.MESH
ANY = pl.BlockSpec(memory_space=pl.ANY)
VM = pl.BlockSpec(memory_space=pltpu.VMEM)
BF = jnp.bfloat16
F32 = jnp.float32
VLIM = 67043328

NK = 4
NS = 5
CW = 256
NW = 8
SLAB = 256


def place():
    ey, ex, ec = (lax.axis_index(a) for a in EXP)
    dev = {"x": dict(ey=ey, ex=1 - ex, ec=ec), "y": dict(ey=1 - ey, ex=ex, ec=ec), "p": dict(ey=ey, ex=ex, ec=1 - ec)}
    chip = {"o": ey * 2 + ex, "x": ey * 2 + 1 - ex, "y": (1 - ey) * 2 + ex, "d": (1 - ey) * 2 + 1 - ex}
    return ey, ex, ec, dev, chip


def silu_mul(a, b):
    return (a * jax.nn.sigmoid(a) * b).astype(BF)


def first(el, cap, ids_ref, gates_ref, x_ref, w1_ref, w3_ref, ws1_ref, ws3_ref, h_ref, sh_ref, meta_ref,
          xg, acc, wb, disp, xe, hst, mout, meta,
          xsem, wsem, osem, csem, msend, mrecv, ssem, rsem):
    ey, ex, ec, dev, chip = place()
    t = x_ref.shape[0]
    kw = x_ref.shape[1] // NK
    f = w1_ref.shape[2]
    half = t // 2
    lo, hi, full = pl.ds(0, half), pl.ds(half, half), pl.ds(0, t)
    mine = {c: ec * 4 + chip[c] for c in "oxyd"}
    theirs = {c: (1 - ec) * 4 + chip[c] for c in "oxyd"}
    nsh = 2 * NK
    nb = nsh + NK * el

    def block(b, go):
        slot = lax.rem(b, NS)

        @pl.when(b < nsh)
        def _():
            rows = pl.ds(pl.multiple_of(lax.rem(b, NK) * kw, kw), kw)
            cols = pl.ds(pl.multiple_of((b // NK) * f, 128), f)
            for i, w in enumerate((ws1_ref, ws3_ref)):
                go(pltpu.make_async_copy(w.at[rows, cols], wb.at[slot, :, pl.ds(i * f, f)], wsem.at[slot, i]))

        @pl.when((b >= nsh) & (b < nb))
        def _():
            q = b - nsh
            rows = pl.ds(pl.multiple_of((q // el) * kw, kw), kw)
            for i, w in enumerate((w1_ref, w3_ref)):
                go(pltpu.make_async_copy(w.at[lax.rem(q, el), rows], wb.at[slot, :, pl.ds(i * f, f)], wsem.at[slot, i]))

    def fetch(b):
        block(b, lambda c: c.start())

    def ready(b):
        block(b, lambda c: c.wait())

    def pair(b):
        for j in range(2):
            fetch(b + NS - 2 + j)
        for j in range(2):
            ready(b + j)

    for b in range(NS - 2):
        fetch(b)
    for k in range(NK):
        pltpu.make_async_copy(x_ref.at[:, pl.ds(k * kw, kw)], xg.at[k, mine["o"]], xsem.at[k]).start()

    ne = el * 8
    row = lax.broadcasted_iota(jnp.int32, (ne, t), 0)
    chosen = jnp.zeros((ne, t), F32)
    gate = jnp.zeros((ne, t), F32)
    for j in range(ids_ref.shape[0]):
        hit = ids_ref[j:j + 1, :] == row
        chosen = jnp.where(hit, 1.0, chosen)
        gate = jnp.where(hit, gates_ref[j:j + 1, :], gate)
    before = (lax.broadcasted_iota(jnp.int32, (t, t), 0) < lax.broadcasted_iota(jnp.int32, (t, t), 1))
    rank = jnp.dot(chosen.astype(BF), before.astype(F32).astype(BF), preferred_element_type=F32)
    rank = jnp.where(chosen > 0.0, rank, -1.0)
    for d in range(8):
        mout[d, 0:el, :] = rank[d * el:(d + 1) * el]
        mout[d, el:2 * el, :] = gate[d * el:(d + 1) * el]

    barrier = pltpu.get_barrier_semaphore()
    others = [(a, b, c) for a in (0, 1) for b in (0, 1) for c in (0, 1) if a + b + c]

    def flip(o):
        return [lax.rem(v + s, 2) for v, s in zip((ey, ex, ec), o)]

    for o in others:
        y2, x2, c2 = flip(o)
        pl.semaphore_signal(barrier, inc=1, device_id=dict(ey=y2, ex=x2, ec=c2), device_id_type=MESH)
    pl.semaphore_wait(barrier, len(others))

    for k in range(NK):
        pltpu.make_async_copy(x_ref.at[:, pl.ds(k * kw, kw)], xg.at[k, mine["o"]], xsem.at[k]).wait()

    def remote(k, src, rows, chan, to):
        ref = xg.at[k, src, rows]
        return pltpu.make_async_remote_copy(ref, ref, ssem.at[k, chan], rsem.at[k, chan], device_id=dev[to],
                                            device_id_type=MESH)

    def direct(k):
        for chan, to in enumerate("xyp"):
            remote(k, mine["o"], full, chan, to).start()

    def relay(k):
        remote(k, mine["x"], full, 0, "x").wait_recv()
        remote(k, mine["x"], lo, 3, "y").start()
        remote(k, mine["x"], full, 5, "p").start()
        remote(k, mine["y"], full, 1, "y").wait_recv()
        remote(k, mine["y"], hi, 4, "x").start()
        remote(k, mine["y"], full, 6, "p").start()

    def corner(k):
        remote(k, mine["d"], lo, 3, "y").wait_recv()
        remote(k, mine["d"], lo, 7, "p").start()
        remote(k, mine["d"], hi, 4, "x").wait_recv()
        remote(k, mine["d"], hi, 8, "p").start()

    def arrived(k):
        remote(k, theirs["o"], full, 2, "p").wait_recv()
        remote(k, theirs["x"], full, 5, "p").wait_recv()
        remote(k, theirs["y"], full, 6, "p").wait_recv()
        remote(k, theirs["d"], lo, 7, "p").wait_recv()
        remote(k, theirs["d"], hi, 8, "p").wait_recv()

    def sent(k):
        for src, rows, chan, to in ((mine["o"], full, 0, "x"), (mine["o"], full, 1, "y"), (mine["o"], full, 2, "p"),
                                    (mine["x"], lo, 3, "y"), (mine["y"], hi, 4, "x"), (mine["x"], full, 5, "p"),
                                    (mine["y"], full, 6, "p"), (mine["d"], lo, 7, "p"), (mine["d"], hi, 8, "p")):
            remote(k, src, rows, chan, to).wait_send()

    def mcopy(o, back=False):
        y2, x2, c2 = flip(o)
        num = c2 * 4 + y2 * 2 + x2
        idx = y2 * 4 + x2 * 2 + c2
        src, dst = (meta.at[num], num) if back else (mout.at[idx], mine["o"])
        return pltpu.make_async_remote_copy(src, meta.at[dst], msend.at[num], mrecv.at[dst],
                                            device_id=dict(ey=y2, ex=x2, ec=c2), device_id_type=MESH)

    for o in others:
        mcopy(o).start()
    direct(0)

    for hf in range(2):
        acc[0, 0:t, :] = jnp.zeros((t, 2 * f), F32)

        def body(i, _):
            b = hf * NK + 2 * i
            pair(b)
            for at in [slice(v, v + SLAB) for v in range(0, 2 * f, SLAB)]:
                d = [jnp.dot(xg[2 * i + j, mine["o"]], wb[lax.rem(b + j, NS), :, at], preferred_element_type=F32)
                     for j in range(2)]
                acc[0, 0:t, at] += d[0] + d[1]
            return 0

        lax.fori_loop(0, NK // 2, body, 0)
        for v in range(0, f, 128):
            hst[hf, 0:t, v:v + 128] = silu_mul(acc[0, 0:t, v:v + 128], acc[0, 0:t, f + v:f + v + 128])
        pltpu.make_async_copy(hst.at[hf, 0:t], sh_ref.at[hf], osem.at[hf]).start()
        if hf == 0:
            relay(0)
            direct(1)


    meta[mine["o"]] = mout[ey * 4 + ex * 2 + ec]
    for o in others:
        mcopy(o, True).wait_recv()
    keep = pltpu.make_async_copy(meta, meta_ref, csem)
    keep.start()
    slots = lax.broadcasted_iota(jnp.int32, (cap, t), 0).astype(F32)

    def build(s, _):
        for e in range(el):
            sel = meta[s, e:e + 1, :] == slots
            disp[s, e * cap:(e + 1) * cap, :] = jnp.where(sel, 1.0, 0.0).astype(BF)
        return 0

    lax.fori_loop(0, 8, build, 0)

    def gather(k):
        def body(s, _):
            r = jnp.dot(disp[s], xg[k, s], preferred_element_type=F32).astype(BF)
            for e in range(el):
                xe[e, s] = r[e * cap:(e + 1) * cap]
            return 0

        lax.fori_loop(0, 8, body, 0)

    def products(k, i, use):
        b = nsh + k * el + 2 * i
        pair(b)
        for j in range(2):
            slot = lax.rem(b + j, NS)
            u = xe[2 * i + j].reshape(8 * cap, kw)
            use(2 * i + j, lambda at, u=u, slot=slot: jnp.dot(u, wb[slot, :, at], preferred_element_type=F32))

    def slabs(w):
        return [slice(i, min(i + w, 2 * f)) for i in range(0, 2 * f, w)]

    def start_acc(i, _):
        def use(e, part):
            for at in slabs(SLAB):
                acc[e, :, at] = part(at)
        products(0, i, use)
        return 0

    corner(0)
    arrived(0)
    gather(0)
    lax.fori_loop(0, el // 8, start_acc, 0)
    relay(1)
    direct(2)
    lax.fori_loop(el // 8, el // 2 - el // 8, start_acc, 0)
    corner(1)
    lax.fori_loop(el // 2 - el // 8, el // 2, start_acc, 0)

    def more(k, _):
        arrived(k)
        gather(k)

        def add(i, _):
            def use(e, part):
                for at in slabs(SLAB):
                    acc[e, :, at] += part(at)
            products(k, i, use)
            return 0

        lax.fori_loop(0, el // 8, add, 0)
        relay(k + 1)

        @pl.when(k < NK - 2)
        def _():
            direct(k + 2)
        lax.fori_loop(el // 8, el // 2 - el // 8, add, 0)
        corner(k + 1)
        lax.fori_loop(el // 2 - el // 8, el // 2, add, 0)
        return 0

    lax.fori_loop(1, NK - 1, more, 0)

    arrived(NK - 1)
    gather(NK - 1)
    for hf in range(2):
        pltpu.make_async_copy(hst.at[hf, 0:t], sh_ref.at[hf], osem.at[hf]).wait()

    def last(i, _):
        @pl.when(i >= 1)
        def _():
            for j in range(2):
                pltpu.make_async_copy(hst.at[j], h_ref.at[2 * i - 2 + j], osem.at[j]).wait()

        def use(e, part):
            slot = lax.rem(e, 2)
            nt = f // 128
            live = {}
            order = [nt // 2] + [v for i in range(nt // 2) for v in (i, nt // 2 + 1 + i)]
            for i in order:
                at = slice(i * 256, i * 256 + 256)
                d = acc[e, :, at] + part(at)
                for j in (2 * i, 2 * i + 1):
                    live[j] = d[:, (j - 2 * i) * 128:(j - 2 * i) * 128 + 128]
                    if j == nt - 1:
                        acc[e, :, j * 128:j * 128 + 128] = live.pop(j)
                for j in [v for v in live if v < nt and v + nt in live]:
                    hst[slot, :, j * 128:j * 128 + 128] = silu_mul(live.pop(j), live.pop(j + nt))
                if 2 * nt - 1 in live:
                    j = nt - 1
                    hst[slot, :, j * 128:j * 128 + 128] = silu_mul(acc[e, :, j * 128:j * 128 + 128], live.pop(2 * nt - 1))
            pltpu.make_async_copy(hst.at[slot], h_ref.at[e], osem.at[slot]).start()
        products(NK - 1, i, use)
        return 0

    lax.fori_loop(0, el // 2, last, 0)

    keep.wait()
    for e in (el - 2, el - 1):
        pltpu.make_async_copy(hst.at[e % 2], h_ref.at[e], osem.at[e % 2]).wait()
    for o in others:
        mcopy(o).wait_send()
    for k in range(NK):
        sent(k)


def second(el, cap, h_ref, sh_ref, meta_ref, x_ref, w2_ref, ws2_ref, y_ref,
           hv, shv, wcv, meta, xv, wb, o3, part, give, pr, sb, rv, res, yst,
           hsem, csem, xsem, wsem, ysem, psend, precv, ssem, rsem, esend, erecv):
    ey, ex, ec, dev, chip = place()
    t, hd = x_ref.shape
    nc = hd // CW
    f = w2_ref.shape[1]
    half = t // 2
    lo, hi = pl.ds(0, half), pl.ds(half, half)
    per = el + 2
    nb = nc * per
    n = el * cap

    def block(b, go):
        c, j = b // per, lax.rem(b, per)
        cols = pl.ds(pl.multiple_of(c * CW, CW), CW)
        slot = lax.rem(b, NW)

        @pl.when((j < el) & (b < nb))
        def _():
            go(pltpu.make_async_copy(w2_ref.at[j, :, cols], wb.at[slot], wsem.at[slot]))

        @pl.when((j >= el) & (b < nb))
        def _():
            rows = pl.ds(pl.multiple_of((j - el) * f, 128), f)
            go(pltpu.make_async_copy(ws2_ref.at[rows, cols], wb.at[slot], wsem.at[slot]))

    def fetch(b):
        block(b, lambda c: c.start())

    def ready(b):
        block(b, lambda c: c.wait())

    def hcopy(e):
        return pltpu.make_async_copy(h_ref.at[e], hv.at[e], hsem.at[e])

    hcopy(0).start()
    for b in range(NW - 1):
        fetch(b)
    for e in range(1, el):
        hcopy(e).start()
    loads = [pltpu.make_async_copy(sh_ref, shv, xsem.at[0]), pltpu.make_async_copy(x_ref, xv, xsem.at[1]),
             ]
    m = pltpu.make_async_copy(meta_ref, meta, csem)
    m.start()

    barrier = pltpu.get_barrier_semaphore()
    for to in "xyp":
        pl.semaphore_signal(barrier, inc=1, device_id=dev[to], device_id_type=MESH)
    pl.semaphore_wait(barrier, 3)

    m.wait()
    slots = lax.broadcasted_iota(jnp.int32, (cap, t), 0).astype(F32)

    def build(s, _):
        parts = [jnp.where(meta[s, e:e + 1, :] == slots, meta[s, el + e:el + e + 1, :], 0.0) for e in range(el)]
        w = jnp.concatenate(parts, axis=0).T
        for i in range(3):
            p = w.astype(BF)
            wcv[s, :, i * n:(i + 1) * n] = p
            w = w - p.astype(F32)
        return 0

    lax.fori_loop(0, 8, build, 0)

    def swap(c, i):
        ch = chip["dxyo"[i]]
        return pltpu.make_async_remote_copy(give.at[lax.rem(c, 2), ch], pr.at[c, ch], psend.at[c, i], precv.at[c, i],
                                            device_id=dev["p"], device_id_type=MESH)

    def ship(c, i, a, b, k=None):
        send, recv = (ssem.at[c, i], rsem.at[c, i]) if k is None else (esend.at[k, i], erecv.at[k, i])
        at = pl.ds(a, b - a)
        return pltpu.make_async_remote_copy(sb.at[i, c, at], rv.at[i, c, at], send, recv, device_id=dev["xy"[i]],
                                            device_id_type=MESH)

    def dispatch(c, op):
        for i in range(2):
            pl.when(c < 2)(lambda: op(ship(c, i, 0, 2)))
            pl.when((c >= 2) & (c < nc - 1))(lambda: op(ship(c, i, 0, 3)))
            pl.when(c == nc - 1)(lambda: op(ship(c, i, 0, 1)))

    def weigh(c, ch, core):
        s = core * 4 + chip[ch]
        return jnp.dot(wcv[s], o3[s], preferred_element_type=F32)

    def stage1(c):
        d, x, y, o = (chip[ch] for ch in "dxyo")
        swap(c, 0).wait_recv()
        sb[0, c, 0] = part[c, d, 0:half] + pr[c, d, 0:half]
        sb[1, c, 0] = part[c, d, half:t] + pr[c, d, half:t]
        swap(c, 1).wait_recv()
        sb[0, c, 1] = part[c, x, 0:half] + pr[c, x, 0:half]
        part[c, x, half:t] += pr[c, x, half:t]
        swap(c, 2).wait_recv()
        part[c, y, 0:half] += pr[c, y, 0:half]
        sb[1, c, 1] = part[c, y, half:t] + pr[c, y, half:t]
        swap(c, 3).wait_recv()
        part[c, o] += pr[c, o]

    def stage2(c, into):
        sb[1, into, 2] = part[c, chip["y"], 0:half] + rv[0, c, 0]
        sb[0, into, 2] = part[c, chip["x"], half:t] + rv[1, c, 0]

    def send(c):
        @pl.when(c >= 2)
        def _():
            dispatch(c - 2, lambda d: d.wait_recv())
            stage2(c - 2, c)
        stage1(c)
        dispatch(c, lambda d: d.start())

    def compute(c):
        def expert(e, _):
            b = c * per + e
            fetch(b + NW - 1)

            @pl.when(c == 0)
            def _():
                hcopy(e).wait()
            ready(b)
            o = jnp.dot(hv[e], wb[lax.rem(b, NW)], preferred_element_type=F32).astype(BF)
            for s in range(8):
                for i in range(3):
                    o3[s, pl.ds(pl.multiple_of(i * n + e * cap, 16), cap), :] = o[s * cap:(s + 1) * cap]
            return 0

        lax.fori_loop(0, el, expert, 0)

        @pl.when(c >= 2)
        def _():
            send(c - 1)

        @pl.when(c == 0)
        def _():
            for d in loads:
                d.start()

        @pl.when(c >= 2)
        def _():
            for i in range(4):
                swap(c - 2, i).wait_send()
        for i, ch in enumerate("dxyo"):
            give[lax.rem(c, 2), chip[ch]] = weigh(c, ch, 1 - ec)
            swap(c, i).start()
        for ch in "dxyo":
            part[c, chip[ch]] = weigh(c, ch, ec)

    def shared(c):
        @pl.when(c == 0)
        def _():
            for d in loads:
                d.wait()
        s = None
        for i in range(2):
            b = c * per + el + i
            fetch(b + NW - 1)
            ready(b)
            p = jnp.dot(shv[i], wb[lax.rem(b, NW)], preferred_element_type=F32)
            s = p if s is None else s + p
        cols = pl.ds(pl.multiple_of(c * CW, CW), CW)
        res[c] = xv[:, cols].astype(F32) + s.astype(BF).astype(F32)

    def ycopy(c):
        cols = pl.ds(pl.multiple_of(c * CW, CW), CW)
        return pltpu.make_async_copy(yst.at[lax.rem(c, 2)], y_ref.at[:, cols], ysem.at[lax.rem(c, 2)])

    def stage3(c):
        n2 = lax.rem(c + 2, nc)

        @pl.when(c >= 2)
        def _():
            ycopy(c - 2).wait()
        own = res[c] + part[c, chip["o"]]
        yst[lax.rem(c, 2), 0:half] = (own[0:half] + rv[0, c, 1] + rv[1, n2, 2]).astype(BF)
        yst[lax.rem(c, 2), half:t] = (own[half:t] + rv[0, n2, 2] + rv[1, c, 1]).astype(BF)
        ycopy(c).start()

    def step(c, _):
        compute(c)

        @pl.when(c == 0)
        def _():
            send(0)
        shared(c)

        @pl.when(c == nc - 1)
        def _():
            send(nc - 1)
            for i in range(2):
                ship(nc - 1, i, 1, 3, 0).start()

        @pl.when(c >= 5)
        def _():
            stage3(c - 5)
        return 0

    lax.fori_loop(0, nc, step, 0)
    stage3(nc - 5)
    for i in range(2):
        ship(nc - 2, i, 0, 3).wait_recv()
    stage2(nc - 2, 0)
    for i in range(2):
        ship(0, i, 2, 3, 1).start()
    stage3(nc - 4)
    for i in range(2):
        ship(nc - 1, i, 0, 1).wait_recv()
    stage2(nc - 1, 1)
    for i in range(2):
        ship(1, i, 2, 3, 2).start()
    for i in range(2):
        ship(nc - 1, i, 1, 3, 0).wait_recv()
    stage3(nc - 3)
    for k in range(2):
        for i in range(2):
            ship(k, i, 2, 3, k + 1).wait_recv()
        stage3(nc - 2 + k)
    for c in (nc - 2, nc - 1):
        ycopy(c).wait()
        for i in range(4):
            swap(c, i).wait_send()
    for i in range(2):
        ship(nc - 1, i, 1, 3, 0).wait_send()
        for k in range(2):
            ship(k, i, 2, 3, k + 1).wait_send()

    def drain(c, _):
        dispatch(c, lambda d: d.wait_send())
        return 0

    lax.fori_loop(0, nc, drain, 0)


def solution(mesh):
    pg = mesh.shape["ey"] * mesh.shape["ex"] * mesh.shape["ec"]

    def local(x, ids, gates, w1, w3, w2, ws1, ws3, ws2):
        t, hd = x.shape
        top = ids.shape[1]
        el, _, f = w1.shape
        ne = el * pg
        cap = min(t, 2 * ((t * top + ne - 1) // ne))
        n = el * cap
        kw = hd // NK
        nc = hd // CW
        dma = pltpu.SemaphoreType.DMA
        h, sh, meta = pl.pallas_call(
            functools.partial(first, el, cap),
            out_shape=(jax.ShapeDtypeStruct((el, pg * cap, f), BF), jax.ShapeDtypeStruct((2, t, f), BF),
                       jax.ShapeDtypeStruct((pg, 2 * el, t), F32)),
            in_specs=[VM, VM] + [ANY] * 5, out_specs=(ANY,) * 3,
            scratch_shapes=[
                pltpu.VMEM((NK, pg, t, kw), BF), pltpu.VMEM((el, pg * cap, 2 * f), F32), pltpu.VMEM((NS, kw, 2 * f), BF),
                pltpu.VMEM((pg, n, t), BF), pltpu.VMEM((el, pg, cap, kw), BF), pltpu.VMEM((2, pg * cap, f), BF),
                pltpu.VMEM((pg, 2 * el, t), F32), pltpu.VMEM((pg, 2 * el, t), F32),
                dma((NK,)), dma((NS, 2)), dma((2,)), dma, dma((8,)), dma((8,)), dma((NK, 9)), dma((NK, 9))],
            compiler_params=pltpu.CompilerParams(collective_id=0, has_side_effects=True, vmem_limit_bytes=VLIM),
        )(ids.T, gates.T, x, w1, w3, ws1, ws3)
        return pl.pallas_call(
            functools.partial(second, el, cap),
            out_shape=jax.ShapeDtypeStruct((t, hd), BF),
            in_specs=[ANY] * 6, out_specs=ANY,
            scratch_shapes=[
                pltpu.VMEM((el, pg * cap, f), BF), pltpu.VMEM((2, t, f), BF), pltpu.VMEM((pg, t, 3 * n), BF), pltpu.VMEM((pg, 2 * el, t), F32),
                pltpu.VMEM((t, hd), BF), pltpu.VMEM((NW, f, CW), BF), pltpu.VMEM((pg, 3 * n, CW), BF),
                pltpu.VMEM((nc, 4, t, CW), F32), pltpu.VMEM((2, 4, t, CW), F32), pltpu.VMEM((nc, 4, t, CW), F32),
                pltpu.VMEM((2, nc, 3, t // 2, CW), F32), pltpu.VMEM((2, nc, 3, t // 2, CW), F32),
                pltpu.VMEM((nc, t, CW), F32), pltpu.VMEM((2, t, CW), BF),
                dma((el,)), dma, dma((2,)), dma((NW,)), dma((2,)), dma((nc, 4)), dma((nc, 4)), dma((nc, 2)), dma((nc, 2)),
                dma((3, 2)), dma((3, 2))],
            compiler_params=pltpu.CompilerParams(collective_id=1, has_side_effects=True, vmem_limit_bytes=VLIM),
        )(h, sh, meta, x, w2, ws2)

    return jax.shard_map(local, mesh=mesh,
                         in_specs=(P(ALL), P(ALL), P(ALL), P(EXP), P(EXP), P(EXP), P(), P(), P()),
                         out_specs=P(ALL), check_vma=False)
```

```python
import functools

import jax
import jax.numpy as jnp
from jax import lax
from jax.experimental import pallas as pl
from jax.experimental.pallas import tpu as pltpu
from jax.sharding import PartitionSpec as P

EXP = ("ey", "ex", "ec")
ALL = ("dp", "ey", "ex", "ec")
MESH = pl.DeviceIdType.MESH
ANY = pl.BlockSpec(memory_space=pl.ANY)
VM = pl.BlockSpec(memory_space=pltpu.VMEM)
BF = jnp.bfloat16
F32 = jnp.float32
VLIM = 67043328

NK = 4
NS = 5
CW = 256
NW = 8
SLAB = 256


def place():
    ey, ex, ec = (lax.axis_index(a) for a in EXP)
    dev = {"x": dict(ey=ey, ex=1 - ex, ec=ec), "y": dict(ey=1 - ey, ex=ex, ec=ec), "p": dict(ey=ey, ex=ex, ec=1 - ec)}
    chip = {"o": ey * 2 + ex, "x": ey * 2 + 1 - ex, "y": (1 - ey) * 2 + ex, "d": (1 - ey) * 2 + 1 - ex}
    return ey, ex, ec, dev, chip


def silu_mul(a, b):
    return (a * jax.nn.sigmoid(a) * b).astype(BF)


def first(el, cap, ids_ref, gates_ref, x_ref, w1_ref, w3_ref, ws1_ref, ws3_ref, h_ref, sh_ref, meta_ref,
          xg, acc, wb, disp, xe, hst, mout, meta,
          xsem, wsem, osem, csem, msend, mrecv, ssem, rsem):
    ey, ex, ec, dev, chip = place()
    t = x_ref.shape[0]
    kw = x_ref.shape[1] // NK
    f = w1_ref.shape[2]
    half = t // 2
    lo, hi, full = pl.ds(0, half), pl.ds(half, half), pl.ds(0, t)
    mine = {c: ec * 4 + chip[c] for c in "oxyd"}
    theirs = {c: (1 - ec) * 4 + chip[c] for c in "oxyd"}
    nsh = 2 * NK
    nb = nsh + NK * el

    def block(b, go):
        slot = lax.rem(b, NS)

        @pl.when(b < nsh)
        def _():
            rows = pl.ds(pl.multiple_of(lax.rem(b, NK) * kw, kw), kw)
            cols = pl.ds(pl.multiple_of((b // NK) * f, 128), f)
            for i, w in enumerate((ws1_ref, ws3_ref)):
                go(pltpu.make_async_copy(w.at[rows, cols], wb.at[slot, :, pl.ds(i * f, f)], wsem.at[slot, i]))

        @pl.when((b >= nsh) & (b < nb))
        def _():
            q = b - nsh
            rows = pl.ds(pl.multiple_of((q // el) * kw, kw), kw)
            for i, w in enumerate((w1_ref, w3_ref)):
                go(pltpu.make_async_copy(w.at[lax.rem(q, el), rows], wb.at[slot, :, pl.ds(i * f, f)], wsem.at[slot, i]))

    def fetch(b):
        block(b, lambda c: c.start())

    def ready(b):
        block(b, lambda c: c.wait())

    def pair(b):
        for j in range(2):
            fetch(b + NS - 2 + j)
        for j in range(2):
            ready(b + j)

    for b in range(NS - 2):
        fetch(b)
    for k in range(NK):
        pltpu.make_async_copy(x_ref.at[:, pl.ds(k * kw, kw)], xg.at[k, mine["o"]], xsem.at[k]).start()

    ne = el * 8
    row = lax.broadcasted_iota(jnp.int32, (ne, t), 0)
    chosen = jnp.zeros((ne, t), F32)
    gate = jnp.zeros((ne, t), F32)
    for j in range(ids_ref.shape[0]):
        hit = ids_ref[j:j + 1, :] == row
        chosen = jnp.where(hit, 1.0, chosen)
        gate = jnp.where(hit, gates_ref[j:j + 1, :], gate)
    before = (lax.broadcasted_iota(jnp.int32, (t, t), 0) < lax.broadcasted_iota(jnp.int32, (t, t), 1))
    rank = jnp.dot(chosen.astype(BF), before.astype(F32).astype(BF), preferred_element_type=F32)
    rank = jnp.where(chosen > 0.0, rank, -1.0)
    for d in range(8):
        mout[d, 0:el, :] = rank[d * el:(d + 1) * el]
        mout[d, el:2 * el, :] = gate[d * el:(d + 1) * el]

    barrier = pltpu.get_barrier_semaphore()
    others = [(a, b, c) for a in (0, 1) for b in (0, 1) for c in (0, 1) if a + b + c]

    def flip(o):
        return [lax.rem(v + s, 2) for v, s in zip((ey, ex, ec), o)]

    for o in others:
        y2, x2, c2 = flip(o)
        pl.semaphore_signal(barrier, inc=1, device_id=dict(ey=y2, ex=x2, ec=c2), device_id_type=MESH)
    pl.semaphore_wait(barrier, len(others))

    for k in range(NK):
        pltpu.make_async_copy(x_ref.at[:, pl.ds(k * kw, kw)], xg.at[k, mine["o"]], xsem.at[k]).wait()

    def remote(k, src, rows, chan, to):
        ref = xg.at[k, src, rows]
        return pltpu.make_async_remote_copy(ref, ref, ssem.at[k, chan], rsem.at[k, chan], device_id=dev[to],
                                            device_id_type=MESH)

    def direct(k):
        for chan, to in enumerate("xyp"):
            remote(k, mine["o"], full, chan, to).start()

    def relay(k):
        remote(k, mine["x"], full, 0, "x").wait_recv()
        remote(k, mine["x"], lo, 3, "y").start()
        remote(k, mine["x"], full, 5, "p").start()
        remote(k, mine["y"], full, 1, "y").wait_recv()
        remote(k, mine["y"], hi, 4, "x").start()
        remote(k, mine["y"], full, 6, "p").start()

    def corner(k):
        remote(k, mine["d"], lo, 3, "y").wait_recv()
        remote(k, mine["d"], lo, 7, "p").start()
        remote(k, mine["d"], hi, 4, "x").wait_recv()
        remote(k, mine["d"], hi, 8, "p").start()

    def arrived(k):
        remote(k, theirs["o"], full, 2, "p").wait_recv()
        remote(k, theirs["x"], full, 5, "p").wait_recv()
        remote(k, theirs["y"], full, 6, "p").wait_recv()
        remote(k, theirs["d"], lo, 7, "p").wait_recv()
        remote(k, theirs["d"], hi, 8, "p").wait_recv()

    def sent(k):
        for src, rows, chan, to in ((mine["o"], full, 0, "x"), (mine["o"], full, 1, "y"), (mine["o"], full, 2, "p"),
                                    (mine["x"], lo, 3, "y"), (mine["y"], hi, 4, "x"), (mine["x"], full, 5, "p"),
                                    (mine["y"], full, 6, "p"), (mine["d"], lo, 7, "p"), (mine["d"], hi, 8, "p")):
            remote(k, src, rows, chan, to).wait_send()

    def mcopy(o, back=False):
        y2, x2, c2 = flip(o)
        num = c2 * 4 + y2 * 2 + x2
        idx = y2 * 4 + x2 * 2 + c2
        src, dst = (meta.at[num], num) if back else (mout.at[idx], mine["o"])
        return pltpu.make_async_remote_copy(src, meta.at[dst], msend.at[num], mrecv.at[dst],
                                            device_id=dict(ey=y2, ex=x2, ec=c2), device_id_type=MESH)

    for o in others:
        mcopy(o).start()
    direct(0)

    for hf in range(2):
        acc[0, 0:t, :] = jnp.zeros((t, 2 * f), F32)

        def body(i, _):
            b = hf * NK + 2 * i
            pair(b)
            for at in [slice(v, v + SLAB) for v in range(0, 2 * f, SLAB)]:
                d = [jnp.dot(xg[2 * i + j, mine["o"]], wb[lax.rem(b + j, NS), :, at], preferred_element_type=F32)
                     for j in range(2)]
                acc[0, 0:t, at] += d[0] + d[1]
            return 0

        lax.fori_loop(0, NK // 2, body, 0)
        for v in range(0, f, 128):
            hst[hf, 0:t, v:v + 128] = silu_mul(acc[0, 0:t, v:v + 128], acc[0, 0:t, f + v:f + v + 128])
        pltpu.make_async_copy(hst.at[hf, 0:t], sh_ref.at[hf], osem.at[hf]).start()
        if hf == 0:
            relay(0)
            direct(1)


    meta[mine["o"]] = mout[ey * 4 + ex * 2 + ec]
    for o in others:
        mcopy(o, True).wait_recv()
    keep = pltpu.make_async_copy(meta, meta_ref, csem)
    keep.start()
    slots = lax.broadcasted_iota(jnp.int32, (cap, t), 0).astype(F32)

    def build(s, _):
        for e in range(el):
            sel = meta[s, e:e + 1, :] == slots
            disp[s, e * cap:(e + 1) * cap, :] = jnp.where(sel, 1.0, 0.0).astype(BF)
        return 0

    lax.fori_loop(0, 8, build, 0)

    def gather(k):
        def body(s, _):
            r = jnp.dot(disp[s], xg[k, s], preferred_element_type=F32).astype(BF)
            for e in range(el):
                xe[e, s] = r[e * cap:(e + 1) * cap]
            return 0

        lax.fori_loop(0, 8, body, 0)

    def products(k, i, use):
        b = nsh + k * el + 2 * i
        pair(b)
        for j in range(2):
            slot = lax.rem(b + j, NS)
            u = xe[2 * i + j].reshape(8 * cap, kw)
            use(2 * i + j, lambda at, u=u, slot=slot: jnp.dot(u, wb[slot, :, at], preferred_element_type=F32))

    def slabs(w):
        return [slice(i, min(i + w, 2 * f)) for i in range(0, 2 * f, w)]

    def start_acc(i, _):
        def use(e, part):
            for at in slabs(SLAB):
                acc[e, :, at] = part(at)
        products(0, i, use)
        return 0

    corner(0)
    arrived(0)
    gather(0)
    lax.fori_loop(0, el // 8, start_acc, 0)
    relay(1)
    direct(2)
    lax.fori_loop(el // 8, el // 2 - el // 8, start_acc, 0)
    corner(1)
    lax.fori_loop(el // 2 - el // 8, el // 2, start_acc, 0)

    def more(k, _):
        arrived(k)
        gather(k)

        def add(i, _):
            def use(e, part):
                for at in slabs(SLAB):
                    acc[e, :, at] += part(at)
            products(k, i, use)
            return 0

        lax.fori_loop(0, el // 8, add, 0)
        relay(k + 1)

        @pl.when(k < NK - 2)
        def _():
            direct(k + 2)
        lax.fori_loop(el // 8, el // 2 - el // 8, add, 0)
        corner(k + 1)
        lax.fori_loop(el // 2 - el // 8, el // 2, add, 0)
        return 0

    lax.fori_loop(1, NK - 1, more, 0)

    arrived(NK - 1)
    gather(NK - 1)
    for hf in range(2):
        pltpu.make_async_copy(hst.at[hf, 0:t], sh_ref.at[hf], osem.at[hf]).wait()

    def last(i, _):
        @pl.when(i >= 1)
        def _():
            for j in range(2):
                pltpu.make_async_copy(hst.at[j], h_ref.at[2 * i - 2 + j], osem.at[j]).wait()

        def use(e, part):
            slot = lax.rem(e, 2)
            nt = f // 128
            live = {}
            order = [nt // 2] + [v for i in range(nt // 2) for v in (i, nt // 2 + 1 + i)]
            for i in order:
                at = slice(i * 256, i * 256 + 256)
                d = acc[e, :, at] + part(at)
                for j in (2 * i, 2 * i + 1):
                    live[j] = d[:, (j - 2 * i) * 128:(j - 2 * i) * 128 + 128]
                    if j == nt - 1:
                        acc[e, :, j * 128:j * 128 + 128] = live.pop(j)
                for j in [v for v in live if v < nt and v + nt in live]:
                    hst[slot, :, j * 128:j * 128 + 128] = silu_mul(live.pop(j), live.pop(j + nt))
                if 2 * nt - 1 in live:
                    j = nt - 1
                    hst[slot, :, j * 128:j * 128 + 128] = silu_mul(acc[e, :, j * 128:j * 128 + 128], live.pop(2 * nt - 1))
            pltpu.make_async_copy(hst.at[slot], h_ref.at[e], osem.at[slot]).start()
        products(NK - 1, i, use)
        return 0

    lax.fori_loop(0, el // 2, last, 0)

    keep.wait()
    for e in (el - 2, el - 1):
        pltpu.make_async_copy(hst.at[e % 2], h_ref.at[e], osem.at[e % 2]).wait()
    for o in others:
        mcopy(o).wait_send()
    for k in range(NK):
        sent(k)


def second(el, cap, h_ref, sh_ref, meta_ref, x_ref, w2_ref, ws2_ref, y_ref,
           hv, shv, wcv, meta, xv, wb, wd, o3, part, give, pr, sb, rv, res, yst,
           hsem, csem, xsem, wsem, dsem, ysem, psend, precv, ssem, rsem, esend, erecv):
    ey, ex, ec, dev, chip = place()
    t, hd = x_ref.shape
    nc = hd // CW
    f = w2_ref.shape[1]
    half = t // 2
    lo, hi = pl.ds(0, half), pl.ds(half, half)
    per = el
    nb = nc * per
    f = w2_ref.shape[1]
    n = el * cap

    def block(b, go):
        c, j = b // per, lax.rem(b, per)
        cols = pl.ds(pl.multiple_of(c * CW, CW), CW)
        slot = lax.rem(b, NW)

        @pl.when(b < nb)
        def _():
            go(pltpu.make_async_copy(w2_ref.at[j, :, cols], wb.at[slot], wsem.at[slot]))

    def down(c):
        cols = pl.ds(pl.multiple_of(c * CW, CW), CW)
        return pltpu.make_async_copy(ws2_ref.at[:, cols], wd.at[lax.rem(c, 2)], dsem.at[lax.rem(c, 2)])

    def fetch(b):
        block(b, lambda c: c.start())

    def ready(b):
        block(b, lambda c: c.wait())

    def hcopy(e):
        return pltpu.make_async_copy(h_ref.at[e], hv.at[e], hsem.at[e])

    hcopy(0).start()
    for b in range(NW):
        fetch(b)
    for e in range(1, el):
        hcopy(e).start()
    loads = [pltpu.make_async_copy(sh_ref, shv, xsem.at[0]), pltpu.make_async_copy(x_ref, xv, xsem.at[1]),
             ]
    m = pltpu.make_async_copy(meta_ref, meta, csem)
    m.start()

    barrier = pltpu.get_barrier_semaphore()
    for to in "xyp":
        pl.semaphore_signal(barrier, inc=1, device_id=dev[to], device_id_type=MESH)
    pl.semaphore_wait(barrier, 3)

    m.wait()
    slots = lax.broadcasted_iota(jnp.int32, (cap, t), 0).astype(F32)

    def build(s, _):
        parts = [jnp.where(meta[s, e:e + 1, :] == slots, meta[s, el + e:el + e + 1, :], 0.0) for e in range(el)]
        w = jnp.concatenate(parts, axis=0).T
        for i in range(3):
            p = w.astype(BF)
            wcv[s, :, i * n:(i + 1) * n] = p
            w = w - p.astype(F32)
        return 0

    lax.fori_loop(0, 8, build, 0)

    def swap(c, i):
        ch = chip["dxyo"[i]]
        return pltpu.make_async_remote_copy(give.at[lax.rem(c, 2), ch], pr.at[c, ch], psend.at[c, i], precv.at[c, i],
                                            device_id=dev["p"], device_id_type=MESH)

    def ship(c, i, a, b, k=None):
        send, recv = (ssem.at[c, i], rsem.at[c, i]) if k is None else (esend.at[k, i], erecv.at[k, i])
        at = pl.ds(a, b - a)
        return pltpu.make_async_remote_copy(sb.at[i, c, at], rv.at[i, c, at], send, recv, device_id=dev["xy"[i]],
                                            device_id_type=MESH)

    def dispatch(c, op):
        for i in range(2):
            pl.when(c < 2)(lambda: op(ship(c, i, 0, 2)))
            pl.when((c >= 2) & (c < nc - 1))(lambda: op(ship(c, i, 0, 3)))
            pl.when(c == nc - 1)(lambda: op(ship(c, i, 0, 1)))

    def weigh(c, ch, core):
        s = core * 4 + chip[ch]
        return jnp.dot(wcv[s], o3[s], preferred_element_type=F32)

    def compute(c):
        def expert(i, _):
            for e in (2 * i, 2 * i + 1):
                @pl.when(c == 0)
                def _():
                    hcopy(e).wait()
                ready(c * per + e)
            for e in (2 * i, 2 * i + 1):
                o = jnp.dot(hv[e], wb[lax.rem(c * per + e, NW)], preferred_element_type=F32).astype(BF)
                for s in range(8):
                    for j in range(3):
                        o3[s, pl.ds(pl.multiple_of(j * n + e * cap, 16), cap), :] = o[s * cap:(s + 1) * cap]
            for e in (2 * i, 2 * i + 1):
                fetch(c * per + e + NW)
            return 0

        lax.fori_loop(0, el // 2, expert, 0)

        @pl.when(c == 1)
        def _():
            for d in loads + [down(0), down(1)]:
                d.start()

        @pl.when(c >= 2)
        def _():
            for i in range(4):
                swap(c - 2, i).wait_send()
        for i, ch in enumerate("dxyo"):
            give[lax.rem(c, 2), chip[ch]] = weigh(c, ch, 1 - ec)
            swap(c, i).start()
        for ch in "dxyo":
            part[c, chip[ch]] = weigh(c, ch, ec)

    def shared(c):
        down(c).wait()
        p = [jnp.dot(shv[i], wd[lax.rem(c, 2), i * f:(i + 1) * f], preferred_element_type=F32) for i in range(2)]
        cols = pl.ds(pl.multiple_of(c * CW, CW), CW)
        res[c] = xv[:, cols].astype(F32) + (p[0] + p[1]).astype(BF).astype(F32)
        pl.when(c + 2 < nc)(lambda: down(c + 2).start())

    def stage1(c):
        d, x, y, o = (chip[ch] for ch in "dxyo")
        swap(c, 0).wait_recv()
        sb[0, c, 0] = part[c, d, 0:half] + pr[c, d, 0:half]
        sb[1, c, 0] = part[c, d, half:t] + pr[c, d, half:t]
        swap(c, 1).wait_recv()
        sb[0, c, 1] = part[c, x, 0:half] + pr[c, x, 0:half]
        part[c, x, half:t] += pr[c, x, half:t]
        swap(c, 2).wait_recv()
        part[c, y, 0:half] += pr[c, y, 0:half]
        sb[1, c, 1] = part[c, y, half:t] + pr[c, y, half:t]
        swap(c, 3).wait_recv()
        part[c, o] += pr[c, o]

    def stage2(c, into):
        sb[1, into, 2] = part[c, chip["y"], 0:half] + rv[0, c, 0]
        sb[0, into, 2] = part[c, chip["x"], half:t] + rv[1, c, 0]

    def ycopy(c):
        cols = pl.ds(pl.multiple_of(c * CW, CW), CW)
        return pltpu.make_async_copy(yst.at[lax.rem(c, 2)], y_ref.at[:, cols], ysem.at[lax.rem(c, 2)])

    def stage3(c):
        n2 = lax.rem(c + 2, nc)

        @pl.when(c >= 2)
        def _():
            ycopy(c - 2).wait()
        own = res[c] + part[c, chip["o"]]
        yst[lax.rem(c, 2), 0:half] = (own[0:half] + rv[0, c, 1] + rv[1, n2, 2]).astype(BF)
        yst[lax.rem(c, 2), half:t] = (own[half:t] + rv[0, n2, 2] + rv[1, c, 1]).astype(BF)
        ycopy(c).start()

    def step(c, _):
        compute(c)

        @pl.when(c >= 2)
        def _():
            dispatch(c - 2, lambda d: d.wait_recv())
            stage2(c - 2, c)
        stage1(c)
        dispatch(c, lambda d: d.start())

        @pl.when(c == nc - 1)
        def _():
            for i in range(2):
                ship(nc - 1, i, 1, 3, 0).start()
        @pl.when(c == 2)
        def _():
            for d in loads:
                d.wait()

        @pl.when(c >= 2)
        def _():
            shared(c - 2)

        @pl.when(c >= 4)
        def _():
            stage3(c - 4)
        return 0

    lax.fori_loop(0, nc, step, 0)
    lax.fori_loop(nc - 2, nc, lambda c, v: (shared(c), v)[1], 0)
    for i in range(2):
        ship(nc - 2, i, 0, 3).wait_recv()
    stage2(nc - 2, 0)
    for i in range(2):
        ship(0, i, 2, 3, 1).start()
    stage3(nc - 4)
    for i in range(2):
        ship(nc - 1, i, 0, 1).wait_recv()
    stage2(nc - 1, 1)
    for i in range(2):
        ship(1, i, 2, 3, 2).start()
    for i in range(2):
        ship(nc - 1, i, 1, 3, 0).wait_recv()
    stage3(nc - 3)
    for k in range(2):
        for i in range(2):
            ship(k, i, 2, 3, k + 1).wait_recv()
        stage3(nc - 2 + k)
    for c in (nc - 2, nc - 1):
        ycopy(c).wait()
        for i in range(4):
            swap(c, i).wait_send()
    for i in range(2):
        ship(nc - 1, i, 1, 3, 0).wait_send()
        for k in range(2):
            ship(k, i, 2, 3, k + 1).wait_send()

    def drain(c, _):
        dispatch(c, lambda d: d.wait_send())
        return 0

    lax.fori_loop(0, nc, drain, 0)


def solution(mesh):
    pg = mesh.shape["ey"] * mesh.shape["ex"] * mesh.shape["ec"]

    def local(x, ids, gates, w1, w3, w2, ws1, ws3, ws2):
        t, hd = x.shape
        top = ids.shape[1]
        el, _, f = w1.shape
        ne = el * pg
        cap = min(t, 2 * ((t * top + ne - 1) // ne))
        n = el * cap
        kw = hd // NK
        nc = hd // CW
        dma = pltpu.SemaphoreType.DMA
        h, sh, meta = pl.pallas_call(
            functools.partial(first, el, cap),
            out_shape=(jax.ShapeDtypeStruct((el, pg * cap, f), BF), jax.ShapeDtypeStruct((2, t, f), BF),
                       jax.ShapeDtypeStruct((pg, 2 * el, t), F32)),
            in_specs=[VM, VM] + [ANY] * 5, out_specs=(ANY,) * 3,
            scratch_shapes=[
                pltpu.VMEM((NK, pg, t, kw), BF), pltpu.VMEM((el, pg * cap, 2 * f), F32), pltpu.VMEM((NS, kw, 2 * f), BF),
                pltpu.VMEM((pg, n, t), BF), pltpu.VMEM((el, pg, cap, kw), BF), pltpu.VMEM((2, pg * cap, f), BF),
                pltpu.VMEM((pg, 2 * el, t), F32), pltpu.VMEM((pg, 2 * el, t), F32),
                dma((NK,)), dma((NS, 2)), dma((2,)), dma, dma((8,)), dma((8,)), dma((NK, 9)), dma((NK, 9))],
            compiler_params=pltpu.CompilerParams(collective_id=0, has_side_effects=True, vmem_limit_bytes=VLIM),
        )(ids.T, gates.T, x, w1, w3, ws1, ws3)
        return pl.pallas_call(
            functools.partial(second, el, cap),
            out_shape=jax.ShapeDtypeStruct((t, hd), BF),
            in_specs=[ANY] * 6, out_specs=ANY,
            scratch_shapes=[
                pltpu.VMEM((el, pg * cap, f), BF), pltpu.VMEM((2, t, f), BF), pltpu.VMEM((pg, t, 3 * n), BF), pltpu.VMEM((pg, 2 * el, t), F32),
                pltpu.VMEM((t, hd), BF), pltpu.VMEM((NW, f, CW), BF), pltpu.VMEM((2, 2 * f, CW), BF), pltpu.VMEM((pg, 3 * n, CW), BF),
                pltpu.VMEM((nc, 4, t, CW), F32), pltpu.VMEM((2, 4, t, CW), F32), pltpu.VMEM((nc, 4, t, CW), F32),
                pltpu.VMEM((2, nc, 3, t // 2, CW), F32), pltpu.VMEM((2, nc, 3, t // 2, CW), F32),
                pltpu.VMEM((nc, t, CW), F32), pltpu.VMEM((2, t, CW), BF),
                dma((el,)), dma, dma((2,)), dma((NW,)), dma((2,)), dma((2,)), dma((nc, 4)), dma((nc, 4)), dma((nc, 2)), dma((nc, 2)),
                dma((3, 2)), dma((3, 2))],
            compiler_params=pltpu.CompilerParams(collective_id=1, has_side_effects=True, vmem_limit_bytes=VLIM),
        )(h, sh, meta, x, w2, ws2)

    return jax.shard_map(local, mesh=mesh,
                         in_specs=(P(ALL), P(ALL), P(ALL), P(EXP), P(EXP), P(EXP), P(), P(), P()),
                         out_specs=P(ALL), check_vma=False)
```

```python
import functools

import jax
import jax.numpy as jnp
from jax import lax
from jax.experimental import pallas as pl
from jax.experimental.pallas import tpu as pltpu
from jax.sharding import PartitionSpec as P

EXP = ("ey", "ex", "ec")
ALL = ("dp", "ey", "ex", "ec")
MESH = pl.DeviceIdType.MESH
ANY = pl.BlockSpec(memory_space=pl.ANY)
VM = pl.BlockSpec(memory_space=pltpu.VMEM)
BF = jnp.bfloat16
F32 = jnp.float32
VLIM = 67043328

NK = 4
NS = 5
CW = 256
NW = 8
SLAB = 256


def place():
    ey, ex, ec = (lax.axis_index(a) for a in EXP)
    dev = {"x": dict(ey=ey, ex=1 - ex, ec=ec), "y": dict(ey=1 - ey, ex=ex, ec=ec), "p": dict(ey=ey, ex=ex, ec=1 - ec)}
    chip = {"o": ey * 2 + ex, "x": ey * 2 + 1 - ex, "y": (1 - ey) * 2 + ex, "d": (1 - ey) * 2 + 1 - ex}
    return ey, ex, ec, dev, chip


def silu_mul(a, b):
    return (a * jax.nn.sigmoid(a) * b).astype(BF)


def first(el, cap, ids_ref, gates_ref, x_ref, w1_ref, w3_ref, ws1_ref, ws3_ref, h_ref, sh_ref, meta_ref,
          xg, acc, wb, disp, xe, hst, mout, meta,
          xsem, wsem, osem, csem, msend, mrecv, ssem, rsem):
    ey, ex, ec, dev, chip = place()
    t = x_ref.shape[0]
    kw = x_ref.shape[1] // NK
    f = w1_ref.shape[2]
    half = t // 2
    lo, hi, full = pl.ds(0, half), pl.ds(half, half), pl.ds(0, t)
    mine = {c: ec * 4 + chip[c] for c in "oxyd"}
    theirs = {c: (1 - ec) * 4 + chip[c] for c in "oxyd"}
    nsh = 2 * NK
    nb = nsh + NK * el

    def block(b, go):
        slot = lax.rem(b, NS)

        @pl.when(b < nsh)
        def _():
            rows = pl.ds(pl.multiple_of(lax.rem(b, NK) * kw, kw), kw)
            cols = pl.ds(pl.multiple_of((b // NK) * f, 128), f)
            for i, w in enumerate((ws1_ref, ws3_ref)):
                go(pltpu.make_async_copy(w.at[rows, cols], wb.at[slot, :, pl.ds(i * f, f)], wsem.at[slot, i]))

        @pl.when((b >= nsh) & (b < nb))
        def _():
            q = b - nsh
            rows = pl.ds(pl.multiple_of((q // el) * kw, kw), kw)
            for i, w in enumerate((w1_ref, w3_ref)):
                go(pltpu.make_async_copy(w.at[lax.rem(q, el), rows], wb.at[slot, :, pl.ds(i * f, f)], wsem.at[slot, i]))

    def fetch(b):
        block(b, lambda c: c.start())

    def ready(b):
        block(b, lambda c: c.wait())

    def pair(b):
        for j in range(2):
            fetch(b + NS - 2 + j)
        for j in range(2):
            ready(b + j)

    for k in range(NK):
        pltpu.make_async_copy(x_ref.at[:, pl.ds(k * kw, kw)], xg.at[k, mine["o"]], xsem.at[k]).start()
    for b in range(NS - 2):
        fetch(b)

    ne = el * 8
    row = lax.broadcasted_iota(jnp.int32, (ne, t), 0)
    chosen = jnp.zeros((ne, t), F32)
    gate = jnp.zeros((ne, t), F32)
    for j in range(ids_ref.shape[0]):
        hit = ids_ref[j:j + 1, :] == row
        chosen = jnp.where(hit, 1.0, chosen)
        gate = jnp.where(hit, gates_ref[j:j + 1, :], gate)
    before = (lax.broadcasted_iota(jnp.int32, (t, t), 0) < lax.broadcasted_iota(jnp.int32, (t, t), 1))
    rank = jnp.dot(chosen.astype(BF), before.astype(F32).astype(BF), preferred_element_type=F32)
    rank = jnp.where(chosen > 0.0, rank, -1.0)
    for d in range(8):
        mout[d, 0:el, :] = rank[d * el:(d + 1) * el]
        mout[d, el:2 * el, :] = gate[d * el:(d + 1) * el]

    barrier = pltpu.get_barrier_semaphore()
    others = [(a, b, c) for a in (0, 1) for b in (0, 1) for c in (0, 1) if a + b + c]

    def flip(o):
        return [lax.rem(v + s, 2) for v, s in zip((ey, ex, ec), o)]

    for o in others:
        y2, x2, c2 = flip(o)
        pl.semaphore_signal(barrier, inc=1, device_id=dict(ey=y2, ex=x2, ec=c2), device_id_type=MESH)
    pl.semaphore_wait(barrier, len(others))

    for k in range(NK):
        pltpu.make_async_copy(x_ref.at[:, pl.ds(k * kw, kw)], xg.at[k, mine["o"]], xsem.at[k]).wait()

    def remote(k, src, rows, chan, to):
        ref = xg.at[k, src, rows]
        return pltpu.make_async_remote_copy(ref, ref, ssem.at[k, chan], rsem.at[k, chan], device_id=dev[to],
                                            device_id_type=MESH)

    def direct(k):
        for rows, chan, to in ((lo, 0, "x"), (hi, 1, "y"), (hi, 9, "x"), (lo, 10, "y"), (full, 2, "p")):
            remote(k, mine["o"], rows, chan, to).start()

    def relay(k):
        remote(k, mine["x"], lo, 0, "x").wait_recv()
        remote(k, mine["x"], lo, 3, "y").start()
        remote(k, mine["y"], hi, 1, "y").wait_recv()
        remote(k, mine["y"], hi, 4, "x").start()

    def corner(k):
        remote(k, mine["x"], hi, 9, "x").wait_recv()
        remote(k, mine["x"], full, 5, "p").start()
        remote(k, mine["y"], lo, 10, "y").wait_recv()
        remote(k, mine["y"], full, 6, "p").start()
        remote(k, mine["d"], lo, 3, "y").wait_recv()
        remote(k, mine["d"], lo, 7, "p").start()
        remote(k, mine["d"], hi, 4, "x").wait_recv()
        remote(k, mine["d"], hi, 8, "p").start()

    def arrived(k):
        remote(k, theirs["o"], full, 2, "p").wait_recv()
        remote(k, theirs["x"], full, 5, "p").wait_recv()
        remote(k, theirs["y"], full, 6, "p").wait_recv()
        remote(k, theirs["d"], lo, 7, "p").wait_recv()
        remote(k, theirs["d"], hi, 8, "p").wait_recv()

    def sent(k):
        for src, rows, chan, to in ((mine["o"], lo, 0, "x"), (mine["o"], hi, 9, "x"), (mine["o"], hi, 1, "y"),
                                    (mine["o"], lo, 10, "y"), (mine["o"], full, 2, "p"),
                                    (mine["x"], lo, 3, "y"), (mine["y"], hi, 4, "x"), (mine["x"], full, 5, "p"),
                                    (mine["y"], full, 6, "p"), (mine["d"], lo, 7, "p"), (mine["d"], hi, 8, "p")):
            remote(k, src, rows, chan, to).wait_send()

    def mcopy(o, back=False):
        y2, x2, c2 = flip(o)
        num = c2 * 4 + y2 * 2 + x2
        idx = y2 * 4 + x2 * 2 + c2
        src, dst = (meta.at[num], num) if back else (mout.at[idx], mine["o"])
        return pltpu.make_async_remote_copy(src, meta.at[dst], msend.at[num], mrecv.at[dst],
                                            device_id=dict(ey=y2, ex=x2, ec=c2), device_id_type=MESH)

    for o in others:
        mcopy(o).start()
    direct(0)

    for hf in range(2):
        acc[0, 0:t, :] = jnp.zeros((t, 2 * f), F32)

        def body(i, _):
            b = hf * NK + 2 * i
            pair(b)
            for at in [slice(v, v + SLAB) for v in range(0, 2 * f, SLAB)]:
                d = [jnp.dot(xg[2 * i + j, mine["o"]], wb[lax.rem(b + j, NS), :, at], preferred_element_type=F32)
                     for j in range(2)]
                acc[0, 0:t, at] += d[0] + d[1]
            return 0

        lax.fori_loop(0, NK // 2, body, 0)
        for v in range(0, f, 128):
            hst[hf, 0:t, v:v + 128] = silu_mul(acc[0, 0:t, v:v + 128], acc[0, 0:t, f + v:f + v + 128])
        pltpu.make_async_copy(hst.at[hf, 0:t], sh_ref.at[hf], osem.at[hf]).start()
        if hf == 0:
            relay(0)
            direct(1)


    meta[mine["o"]] = mout[ey * 4 + ex * 2 + ec]
    for o in others:
        mcopy(o, True).wait_recv()
    keep = pltpu.make_async_copy(meta, meta_ref, csem)
    keep.start()
    slots = lax.broadcasted_iota(jnp.int32, (cap, t), 0).astype(F32)

    def build(s, _):
        for e in range(el):
            sel = meta[s, e:e + 1, :] == slots
            disp[s, e * cap:(e + 1) * cap, :] = jnp.where(sel, 1.0, 0.0).astype(BF)
        return 0

    lax.fori_loop(0, 8, build, 0)

    def gather(k):
        def body(s, _):
            r = jnp.dot(disp[s], xg[k, s], preferred_element_type=F32).astype(BF)
            for e in range(el):
                xe[e, s] = r[e * cap:(e + 1) * cap]
            return 0

        lax.fori_loop(0, 8, body, 0)

    def products(k, i, use):
        b = nsh + k * el + 2 * i
        pair(b)
        for j in range(2):
            slot = lax.rem(b + j, NS)
            u = xe[2 * i + j].reshape(8 * cap, kw)
            use(2 * i + j, lambda at, u=u, slot=slot: jnp.dot(u, wb[slot, :, at], preferred_element_type=F32))

    def slabs(w):
        return [slice(i, min(i + w, 2 * f)) for i in range(0, 2 * f, w)]

    def start_acc(i, _):
        def use(e, part):
            for at in slabs(SLAB):
                acc[e, :, at] = part(at)
        products(0, i, use)
        return 0

    corner(0)
    arrived(0)
    gather(0)
    lax.fori_loop(0, el // 8, start_acc, 0)
    relay(1)
    direct(2)
    lax.fori_loop(el // 8, el // 2 - el // 8, start_acc, 0)
    corner(1)
    lax.fori_loop(el // 2 - el // 8, el // 2, start_acc, 0)

    def more(k, _):
        arrived(k)
        gather(k)

        def add(i, _):
            def use(e, part):
                for at in slabs(SLAB):
                    acc[e, :, at] += part(at)
            products(k, i, use)
            return 0

        lax.fori_loop(0, el // 8, add, 0)
        relay(k + 1)

        @pl.when(k < NK - 2)
        def _():
            direct(k + 2)
        lax.fori_loop(el // 8, el // 2 - el // 8, add, 0)
        corner(k + 1)
        lax.fori_loop(el // 2 - el // 8, el // 2, add, 0)
        return 0

    lax.fori_loop(1, NK - 1, more, 0)

    arrived(NK - 1)
    gather(NK - 1)
    for hf in range(2):
        pltpu.make_async_copy(hst.at[hf, 0:t], sh_ref.at[hf], osem.at[hf]).wait()

    def last(i, _):
        @pl.when(i >= 1)
        def _():
            for j in range(2):
                pltpu.make_async_copy(hst.at[j], h_ref.at[2 * i - 2 + j], osem.at[j]).wait()

        def use(e, part):
            slot = lax.rem(e, 2)
            nt = f // 128
            live = {}
            order = [nt // 2] + [v for i in range(nt // 2) for v in (i, nt // 2 + 1 + i)]
            for i in order:
                at = slice(i * 256, i * 256 + 256)
                d = acc[e, :, at] + part(at)
                for j in (2 * i, 2 * i + 1):
                    live[j] = d[:, (j - 2 * i) * 128:(j - 2 * i) * 128 + 128]
                    if j == nt - 1:
                        acc[e, :, j * 128:j * 128 + 128] = live.pop(j)
                for j in [v for v in live if v < nt and v + nt in live]:
                    hst[slot, :, j * 128:j * 128 + 128] = silu_mul(live.pop(j), live.pop(j + nt))
                if 2 * nt - 1 in live:
                    j = nt - 1
                    hst[slot, :, j * 128:j * 128 + 128] = silu_mul(acc[e, :, j * 128:j * 128 + 128], live.pop(2 * nt - 1))
            pltpu.make_async_copy(hst.at[slot], h_ref.at[e], osem.at[slot]).start()
        products(NK - 1, i, use)
        return 0

    lax.fori_loop(0, el // 2, last, 0)

    keep.wait()
    for e in (el - 2, el - 1):
        pltpu.make_async_copy(hst.at[e % 2], h_ref.at[e], osem.at[e % 2]).wait()
    for o in others:
        mcopy(o).wait_send()
    for k in range(NK):
        sent(k)


def second(el, cap, h_ref, sh_ref, meta_ref, x_ref, w2_ref, ws2_ref, y_ref,
           hv, shv, wcv, meta, xv, wb, wd, o3, part, give, pr, sb, rv, res, yst,
           hsem, csem, xsem, wsem, dsem, ysem, psend, precv, ssem, rsem, esend, erecv):
    ey, ex, ec, dev, chip = place()
    t, hd = x_ref.shape
    nc = hd // CW
    f = w2_ref.shape[1]
    half = t // 2
    lo, hi = pl.ds(0, half), pl.ds(half, half)
    per = el
    nb = nc * per
    f = w2_ref.shape[1]
    n = el * cap

    def block(b, go):
        c, j = b // per, lax.rem(b, per)
        cols = pl.ds(pl.multiple_of(c * CW, CW), CW)
        slot = lax.rem(b, NW)

        @pl.when(b < nb)
        def _():
            go(pltpu.make_async_copy(w2_ref.at[j, :, cols], wb.at[slot], wsem.at[slot]))

    def down(c):
        cols = pl.ds(pl.multiple_of(c * CW, CW), CW)
        return pltpu.make_async_copy(ws2_ref.at[:, cols], wd.at[lax.rem(c, 2)], dsem.at[lax.rem(c, 2)])

    def fetch(b):
        block(b, lambda c: c.start())

    def ready(b):
        block(b, lambda c: c.wait())

    def hcopy(e):
        return pltpu.make_async_copy(h_ref.at[e], hv.at[e], hsem.at[e])

    m = pltpu.make_async_copy(meta_ref, meta, csem)
    m.start()
    hcopy(0).start()
    for b in range(NW):
        fetch(b)
    for e in range(1, el):
        hcopy(e).start()
    loads = [pltpu.make_async_copy(sh_ref, shv, xsem.at[0]), pltpu.make_async_copy(x_ref, xv, xsem.at[1]),
             ]

    barrier = pltpu.get_barrier_semaphore()
    for to in "xyp":
        pl.semaphore_signal(barrier, inc=1, device_id=dev[to], device_id_type=MESH)
    pl.semaphore_wait(barrier, 3)

    m.wait()
    slots = lax.broadcasted_iota(jnp.int32, (cap, t), 0).astype(F32)

    def build(s, _):
        parts = [jnp.where(meta[s, e:e + 1, :] == slots, meta[s, el + e:el + e + 1, :], 0.0) for e in range(el)]
        w = jnp.concatenate(parts, axis=0).T
        for i in range(3):
            p = w.astype(BF)
            wcv[s, :, i * n:(i + 1) * n] = p
            w = w - p.astype(F32)
        return 0

    lax.fori_loop(0, 8, build, 0)

    def swap(c, i):
        ch = chip["dxyo"[i]]
        return pltpu.make_async_remote_copy(give.at[lax.rem(c, 2), ch], pr.at[c, ch], psend.at[c, i], precv.at[c, i],
                                            device_id=dev["p"], device_id_type=MESH)

    def ship(c, i, a, b, k=None):
        send, recv = (ssem.at[c, i], rsem.at[c, i]) if k is None else (esend.at[k, i], erecv.at[k, i])
        at = pl.ds(a, b - a)
        return pltpu.make_async_remote_copy(sb.at[i, c, at], rv.at[i, c, at], send, recv, device_id=dev["xy"[i]],
                                            device_id_type=MESH)

    def dispatch(c, op):
        for i in range(2):
            pl.when(c < 2)(lambda: op(ship(c, i, 0, 2)))
            pl.when((c >= 2) & (c < nc - 1))(lambda: op(ship(c, i, 0, 3)))
            pl.when(c == nc - 1)(lambda: op(ship(c, i, 0, 1)))

    def weigh(c, ch, core):
        s = core * 4 + chip[ch]
        return jnp.dot(wcv[s], o3[s], preferred_element_type=F32)

    def compute(c):
        def expert(i, _):
            for e in (2 * i, 2 * i + 1):
                @pl.when(c == 0)
                def _():
                    hcopy(e).wait()
                ready(c * per + e)
            for e in (2 * i, 2 * i + 1):
                o = jnp.dot(hv[e], wb[lax.rem(c * per + e, NW)], preferred_element_type=F32).astype(BF)
                for s in range(8):
                    for j in range(3):
                        o3[s, pl.ds(pl.multiple_of(j * n + e * cap, 16), cap), :] = o[s * cap:(s + 1) * cap]
            for e in (2 * i, 2 * i + 1):
                fetch(c * per + e + NW)
            return 0

        lax.fori_loop(0, el // 2, expert, 0)

        @pl.when(c == 1)
        def _():
            for d in loads + [down(0), down(1)]:
                d.start()

        @pl.when(c >= 2)
        def _():
            for i in range(4):
                swap(c - 2, i).wait_send()
        for i, ch in enumerate("dxyo"):
            give[lax.rem(c, 2), chip[ch]] = weigh(c, ch, 1 - ec)
            swap(c, i).start()
        for ch in "dxyo":
            part[c, chip[ch]] = weigh(c, ch, ec)

    def shared(c):
        down(c).wait()
        p = [jnp.dot(shv[i], wd[lax.rem(c, 2), i * f:(i + 1) * f], preferred_element_type=F32) for i in range(2)]
        cols = pl.ds(pl.multiple_of(c * CW, CW), CW)
        res[c] = xv[:, cols].astype(F32) + (p[0] + p[1]).astype(BF).astype(F32)
        pl.when(c + 2 < nc)(lambda: down(c + 2).start())

    def stage1(c):
        d, x, y, o = (chip[ch] for ch in "dxyo")
        swap(c, 0).wait_recv()
        sb[0, c, 0] = part[c, d, 0:half] + pr[c, d, 0:half]
        sb[1, c, 0] = part[c, d, half:t] + pr[c, d, half:t]
        swap(c, 1).wait_recv()
        sb[0, c, 1] = part[c, x, 0:half] + pr[c, x, 0:half]
        part[c, x, half:t] += pr[c, x, half:t]
        swap(c, 2).wait_recv()
        part[c, y, 0:half] += pr[c, y, 0:half]
        sb[1, c, 1] = part[c, y, half:t] + pr[c, y, half:t]
        swap(c, 3).wait_recv()
        part[c, o] += pr[c, o]

    def stage2(c, into):
        sb[1, into, 2] = part[c, chip["y"], 0:half] + rv[0, c, 0]
        sb[0, into, 2] = part[c, chip["x"], half:t] + rv[1, c, 0]

    def ycopy(c):
        cols = pl.ds(pl.multiple_of(c * CW, CW), CW)
        return pltpu.make_async_copy(yst.at[lax.rem(c, 2)], y_ref.at[:, cols], ysem.at[lax.rem(c, 2)])

    def stage3(c):
        n2 = lax.rem(c + 2, nc)

        @pl.when(c >= 2)
        def _():
            ycopy(c - 2).wait()
        own = res[c] + part[c, chip["o"]]
        yst[lax.rem(c, 2), 0:half] = (own[0:half] + rv[0, c, 1] + rv[1, n2, 2]).astype(BF)
        yst[lax.rem(c, 2), half:t] = (own[half:t] + rv[0, n2, 2] + rv[1, c, 1]).astype(BF)
        ycopy(c).start()

    def step(c, _):
        compute(c)

        @pl.when(c >= 2)
        def _():
            dispatch(c - 2, lambda d: d.wait_recv())
            stage2(c - 2, c)
        stage1(c)
        dispatch(c, lambda d: d.start())

        @pl.when(c == nc - 1)
        def _():
            for i in range(2):
                ship(nc - 1, i, 1, 3, 0).start()
        @pl.when(c == 2)
        def _():
            for d in loads:
                d.wait()

        @pl.when(c >= 2)
        def _():
            shared(c - 2)

        @pl.when(c >= 4)
        def _():
            stage3(c - 4)
        return 0

    lax.fori_loop(0, nc, step, 0)
    lax.fori_loop(nc - 2, nc, lambda c, v: (shared(c), v)[1], 0)
    for i in range(2):
        ship(nc - 2, i, 0, 3).wait_recv()
    stage2(nc - 2, 0)
    for i in range(2):
        ship(0, i, 2, 3, 1).start()
    stage3(nc - 4)
    for i in range(2):
        ship(nc - 1, i, 0, 1).wait_recv()
    stage2(nc - 1, 1)
    for i in range(2):
        ship(1, i, 2, 3, 2).start()
    for i in range(2):
        ship(nc - 1, i, 1, 3, 0).wait_recv()
    stage3(nc - 3)
    for k in range(2):
        for i in range(2):
            ship(k, i, 2, 3, k + 1).wait_recv()
        stage3(nc - 2 + k)
    for c in (nc - 2, nc - 1):
        ycopy(c).wait()
        for i in range(4):
            swap(c, i).wait_send()
    for i in range(2):
        ship(nc - 1, i, 1, 3, 0).wait_send()
        for k in range(2):
            ship(k, i, 2, 3, k + 1).wait_send()

    def drain(c, _):
        dispatch(c, lambda d: d.wait_send())
        return 0

    lax.fori_loop(0, nc, drain, 0)


def solution(mesh):
    pg = mesh.shape["ey"] * mesh.shape["ex"] * mesh.shape["ec"]

    def local(x, ids, gates, w1, w3, w2, ws1, ws3, ws2):
        t, hd = x.shape
        top = ids.shape[1]
        el, _, f = w1.shape
        ne = el * pg
        cap = min(t, 2 * ((t * top + ne - 1) // ne))
        n = el * cap
        kw = hd // NK
        nc = hd // CW
        dma = pltpu.SemaphoreType.DMA
        h, sh, meta = pl.pallas_call(
            functools.partial(first, el, cap),
            out_shape=(jax.ShapeDtypeStruct((el, pg * cap, f), BF), jax.ShapeDtypeStruct((2, t, f), BF),
                       jax.ShapeDtypeStruct((pg, 2 * el, t), F32)),
            in_specs=[VM, VM] + [ANY] * 5, out_specs=(ANY,) * 3,
            scratch_shapes=[
                pltpu.VMEM((NK, pg, t, kw), BF), pltpu.VMEM((el, pg * cap, 2 * f), F32), pltpu.VMEM((NS, kw, 2 * f), BF),
                pltpu.VMEM((pg, n, t), BF), pltpu.VMEM((el, pg, cap, kw), BF), pltpu.VMEM((2, pg * cap, f), BF),
                pltpu.VMEM((pg, 2 * el, t), F32), pltpu.VMEM((pg, 2 * el, t), F32),
                dma((NK,)), dma((NS, 2)), dma((2,)), dma, dma((8,)), dma((8,)), dma((NK, 11)), dma((NK, 11))],
            compiler_params=pltpu.CompilerParams(collective_id=0, has_side_effects=True, vmem_limit_bytes=VLIM),
        )(ids.T, gates.T, x, w1, w3, ws1, ws3)
        return pl.pallas_call(
            functools.partial(second, el, cap),
            out_shape=jax.ShapeDtypeStruct((t, hd), BF),
            in_specs=[ANY] * 6, out_specs=ANY,
            scratch_shapes=[
                pltpu.VMEM((el, pg * cap, f), BF), pltpu.VMEM((2, t, f), BF), pltpu.VMEM((pg, t, 3 * n), BF), pltpu.VMEM((pg, 2 * el, t), F32),
                pltpu.VMEM((t, hd), BF), pltpu.VMEM((NW, f, CW), BF), pltpu.VMEM((2, 2 * f, CW), BF), pltpu.VMEM((pg, 3 * n, CW), BF),
                pltpu.VMEM((nc, 4, t, CW), F32), pltpu.VMEM((2, 4, t, CW), F32), pltpu.VMEM((nc, 4, t, CW), F32),
                pltpu.VMEM((2, nc, 3, t // 2, CW), F32), pltpu.VMEM((2, nc, 3, t // 2, CW), F32),
                pltpu.VMEM((nc, t, CW), F32), pltpu.VMEM((2, t, CW), BF),
                dma((el,)), dma, dma((2,)), dma((NW,)), dma((2,)), dma((2,)), dma((nc, 4)), dma((nc, 4)), dma((nc, 2)), dma((nc, 2)),
                dma((3, 2)), dma((3, 2))],
            compiler_params=pltpu.CompilerParams(collective_id=1, has_side_effects=True, vmem_limit_bytes=VLIM),
        )(h, sh, meta, x, w2, ws2)

    return jax.shard_map(local, mesh=mesh,
                         in_specs=(P(ALL), P(ALL), P(ALL), P(EXP), P(EXP), P(EXP), P(), P(), P()),
                         out_specs=P(ALL), check_vma=False)
```

```python
import functools

import jax
import jax.numpy as jnp
from jax import lax
from jax.experimental import pallas as pl
from jax.experimental.pallas import tpu as pltpu
from jax.sharding import PartitionSpec as P

EXP = ("ey", "ex", "ec")
ALL = ("dp", "ey", "ex", "ec")
MESH = pl.DeviceIdType.MESH
ANY = pl.BlockSpec(memory_space=pl.ANY)
VM = pl.BlockSpec(memory_space=pltpu.VMEM)
BF = jnp.bfloat16
F32 = jnp.float32
VLIM = 67043328

NK = 4
NS = 5
CW = 256
NW = 8
SLAB = 256


def place():
    ey, ex, ec = (lax.axis_index(a) for a in EXP)
    dev = {"x": dict(ey=ey, ex=1 - ex, ec=ec), "y": dict(ey=1 - ey, ex=ex, ec=ec), "p": dict(ey=ey, ex=ex, ec=1 - ec)}
    chip = {"o": ey * 2 + ex, "x": ey * 2 + 1 - ex, "y": (1 - ey) * 2 + ex, "d": (1 - ey) * 2 + 1 - ex}
    return ey, ex, ec, dev, chip


def silu_mul(a, b):
    return (a * jax.nn.sigmoid(a) * b).astype(BF)


def first(el, cap, ids_ref, gates_ref, x_ref, w1_ref, w3_ref, ws1_ref, ws3_ref, h_ref, sh_ref, meta_ref,
          xg, acc, wb, disp, xe, hst, mout, meta,
          xsem, wsem, osem, csem, msend, mrecv, ssem, rsem):
    ey, ex, ec, dev, chip = place()
    t = x_ref.shape[0]
    kw = x_ref.shape[1] // NK
    f = w1_ref.shape[2]
    half = t // 2
    lo, hi, full = pl.ds(0, half), pl.ds(half, half), pl.ds(0, t)
    mine = {c: ec * 4 + chip[c] for c in "oxyd"}
    theirs = {c: (1 - ec) * 4 + chip[c] for c in "oxyd"}
    nsh = 2 * NK
    nb = nsh + NK * el

    def block(b, go):
        slot = lax.rem(b, NS)

        @pl.when(b < nsh)
        def _():
            rows = pl.ds(pl.multiple_of(lax.rem(b, NK) * kw, kw), kw)
            cols = pl.ds(pl.multiple_of((b // NK) * f, 128), f)
            for i, w in enumerate((ws1_ref, ws3_ref)):
                go(pltpu.make_async_copy(w.at[rows, cols], wb.at[slot, :, pl.ds(i * f, f)], wsem.at[slot, i]))

        @pl.when((b >= nsh) & (b < nb))
        def _():
            q = b - nsh
            rows = pl.ds(pl.multiple_of((q // el) * kw, kw), kw)
            for i, w in enumerate((w1_ref, w3_ref)):
                go(pltpu.make_async_copy(w.at[lax.rem(q, el), rows], wb.at[slot, :, pl.ds(i * f, f)], wsem.at[slot, i]))

    def fetch(b):
        block(b, lambda c: c.start())

    def ready(b):
        block(b, lambda c: c.wait())

    def pair(b):
        for j in range(2):
            ready(b + j)

    for k in range(NK):
        pltpu.make_async_copy(x_ref.at[:, pl.ds(k * kw, kw)], xg.at[k, mine["o"]], xsem.at[k]).start()
    for b in range(NS):
        fetch(b)

    ne = el * 8
    row = lax.broadcasted_iota(jnp.int32, (ne, t), 0)
    chosen = jnp.zeros((ne, t), F32)
    gate = jnp.zeros((ne, t), F32)
    for j in range(ids_ref.shape[0]):
        hit = ids_ref[j:j + 1, :] == row
        chosen = jnp.where(hit, 1.0, chosen)
        gate = jnp.where(hit, gates_ref[j:j + 1, :], gate)
    before = (lax.broadcasted_iota(jnp.int32, (t, t), 0) < lax.broadcasted_iota(jnp.int32, (t, t), 1))
    rank = jnp.dot(chosen.astype(BF), before.astype(F32).astype(BF), preferred_element_type=F32)
    rank = jnp.where(chosen > 0.0, rank, -1.0)
    for d in range(8):
        mout[d, 0:el, :] = rank[d * el:(d + 1) * el]
        mout[d, el:2 * el, :] = gate[d * el:(d + 1) * el]

    barrier = pltpu.get_barrier_semaphore()
    others = [(a, b, c) for a in (0, 1) for b in (0, 1) for c in (0, 1) if a + b + c]

    def flip(o):
        return [lax.rem(v + s, 2) for v, s in zip((ey, ex, ec), o)]

    for o in others:
        y2, x2, c2 = flip(o)
        pl.semaphore_signal(barrier, inc=1, device_id=dict(ey=y2, ex=x2, ec=c2), device_id_type=MESH)
    pl.semaphore_wait(barrier, len(others))

    for k in range(NK):
        pltpu.make_async_copy(x_ref.at[:, pl.ds(k * kw, kw)], xg.at[k, mine["o"]], xsem.at[k]).wait()

    def remote(k, src, rows, chan, to):
        ref = xg.at[k, src, rows]
        return pltpu.make_async_remote_copy(ref, ref, ssem.at[k, chan], rsem.at[k, chan], device_id=dev[to],
                                            device_id_type=MESH)

    def direct(k):
        for rows, chan, to in ((lo, 0, "x"), (hi, 1, "y"), (hi, 9, "x"), (lo, 10, "y"), (full, 2, "p")):
            remote(k, mine["o"], rows, chan, to).start()

    def relay(k):
        remote(k, mine["x"], lo, 0, "x").wait_recv()
        remote(k, mine["x"], lo, 3, "y").start()
        remote(k, mine["y"], hi, 1, "y").wait_recv()
        remote(k, mine["y"], hi, 4, "x").start()

    def corner(k):
        remote(k, mine["x"], hi, 9, "x").wait_recv()
        remote(k, mine["x"], full, 5, "p").start()
        remote(k, mine["y"], lo, 10, "y").wait_recv()
        remote(k, mine["y"], full, 6, "p").start()
        remote(k, mine["d"], lo, 3, "y").wait_recv()
        remote(k, mine["d"], lo, 7, "p").start()
        remote(k, mine["d"], hi, 4, "x").wait_recv()
        remote(k, mine["d"], hi, 8, "p").start()

    def arrived(k):
        remote(k, theirs["o"], full, 2, "p").wait_recv()
        remote(k, theirs["x"], full, 5, "p").wait_recv()
        remote(k, theirs["y"], full, 6, "p").wait_recv()
        remote(k, theirs["d"], lo, 7, "p").wait_recv()
        remote(k, theirs["d"], hi, 8, "p").wait_recv()

    def sent(k):
        for src, rows, chan, to in ((mine["o"], lo, 0, "x"), (mine["o"], hi, 9, "x"), (mine["o"], hi, 1, "y"),
                                    (mine["o"], lo, 10, "y"), (mine["o"], full, 2, "p"),
                                    (mine["x"], lo, 3, "y"), (mine["y"], hi, 4, "x"), (mine["x"], full, 5, "p"),
                                    (mine["y"], full, 6, "p"), (mine["d"], lo, 7, "p"), (mine["d"], hi, 8, "p")):
            remote(k, src, rows, chan, to).wait_send()

    def mcopy(o, back=False):
        y2, x2, c2 = flip(o)
        num = c2 * 4 + y2 * 2 + x2
        idx = y2 * 4 + x2 * 2 + c2
        src, dst = (meta.at[num], num) if back else (mout.at[idx], mine["o"])
        return pltpu.make_async_remote_copy(src, meta.at[dst], msend.at[num], mrecv.at[dst],
                                            device_id=dict(ey=y2, ex=x2, ec=c2), device_id_type=MESH)

    for o in others:
        mcopy(o).start()
    direct(0)

    for hf in range(2):
        acc[0, 0:t, :] = jnp.zeros((t, 2 * f), F32)

        def body(i, _):
            b = hf * NK + 2 * i
            pair(b)
            for at in [slice(v, v + SLAB) for v in range(0, 2 * f, SLAB)]:
                d = [jnp.dot(xg[2 * i + j, mine["o"]], wb[lax.rem(b + j, NS), :, at], preferred_element_type=F32)
                     for j in range(2)]
                acc[0, 0:t, at] += d[0] + d[1]
            for j in range(2):
                fetch(b + NS + j)
            return 0

        lax.fori_loop(0, NK // 2, body, 0)
        for v in range(0, f, 128):
            hst[hf, 0:t, v:v + 128] = silu_mul(acc[0, 0:t, v:v + 128], acc[0, 0:t, f + v:f + v + 128])
        pltpu.make_async_copy(hst.at[hf, 0:t], sh_ref.at[hf], osem.at[hf]).start()
        if hf == 0:
            relay(0)
            direct(1)


    meta[mine["o"]] = mout[ey * 4 + ex * 2 + ec]
    for o in others:
        mcopy(o, True).wait_recv()
    keep = pltpu.make_async_copy(meta, meta_ref, csem)
    keep.start()
    slots = lax.broadcasted_iota(jnp.int32, (cap, t), 0).astype(F32)

    def build(s, _):
        for e in range(el):
            sel = meta[s, e:e + 1, :] == slots
            disp[s, e * cap:(e + 1) * cap, :] = jnp.where(sel, 1.0, 0.0).astype(BF)
        return 0

    lax.fori_loop(0, 8, build, 0)

    def gather(k):
        def body(s, _):
            r = jnp.dot(disp[s], xg[k, s], preferred_element_type=F32).astype(BF)
            for e in range(el):
                xe[e, s] = r[e * cap:(e + 1) * cap]
            return 0

        lax.fori_loop(0, 8, body, 0)

    def products(k, i, use):
        b = nsh + k * el + 2 * i
        pair(b)
        for j in range(2):
            slot = lax.rem(b + j, NS)
            u = xe[2 * i + j].reshape(8 * cap, kw)
            use(2 * i + j, lambda at, u=u, slot=slot: jnp.dot(u, wb[slot, :, at], preferred_element_type=F32))
            fetch(b + j + NS)

    def slabs(w):
        return [slice(i, min(i + w, 2 * f)) for i in range(0, 2 * f, w)]

    def start_acc(i, _):
        def use(e, part):
            for at in slabs(SLAB):
                acc[e, :, at] = part(at)
        products(0, i, use)
        return 0

    corner(0)
    arrived(0)
    gather(0)
    relay(1)
    direct(2)
    lax.fori_loop(0, el // 2 - el // 8, start_acc, 0)
    corner(1)
    lax.fori_loop(el // 2 - el // 8, el // 2, start_acc, 0)

    def more(k, _):
        arrived(k)
        gather(k)

        def add(i, _):
            def use(e, part):
                for at in slabs(SLAB):
                    acc[e, :, at] += part(at)
            products(k, i, use)
            return 0

        relay(k + 1)

        @pl.when(k < NK - 2)
        def _():
            direct(k + 2)
        lax.fori_loop(0, el // 2 - el // 8, add, 0)
        corner(k + 1)
        lax.fori_loop(el // 2 - el // 8, el // 2, add, 0)
        return 0

    lax.fori_loop(1, NK - 1, more, 0)

    arrived(NK - 1)
    gather(NK - 1)
    for hf in range(2):
        pltpu.make_async_copy(hst.at[hf, 0:t], sh_ref.at[hf], osem.at[hf]).wait()

    def last(i, _):
        @pl.when(i >= 1)
        def _():
            for j in range(2):
                pltpu.make_async_copy(hst.at[j], h_ref.at[2 * i - 2 + j], osem.at[j]).wait()

        def use(e, part):
            slot = lax.rem(e, 2)
            nt = f // 128
            live = {}
            order = [nt // 2] + [v for i in range(nt // 2) for v in (i, nt // 2 + 1 + i)]
            for i in order:
                at = slice(i * 256, i * 256 + 256)
                d = acc[e, :, at] + part(at)
                for j in (2 * i, 2 * i + 1):
                    live[j] = d[:, (j - 2 * i) * 128:(j - 2 * i) * 128 + 128]
                    if j == nt - 1:
                        acc[e, :, j * 128:j * 128 + 128] = live.pop(j)
                for j in [v for v in live if v < nt and v + nt in live]:
                    hst[slot, :, j * 128:j * 128 + 128] = silu_mul(live.pop(j), live.pop(j + nt))
                if 2 * nt - 1 in live:
                    j = nt - 1
                    hst[slot, :, j * 128:j * 128 + 128] = silu_mul(acc[e, :, j * 128:j * 128 + 128], live.pop(2 * nt - 1))
            pltpu.make_async_copy(hst.at[slot], h_ref.at[e], osem.at[slot]).start()
        products(NK - 1, i, use)
        return 0

    lax.fori_loop(0, el // 2, last, 0)

    keep.wait()
    for e in (el - 2, el - 1):
        pltpu.make_async_copy(hst.at[e % 2], h_ref.at[e], osem.at[e % 2]).wait()
    for o in others:
        mcopy(o).wait_send()
    for k in range(NK):
        sent(k)


def second(el, cap, h_ref, sh_ref, meta_ref, x_ref, w2_ref, ws2_ref, y_ref,
           hv, shv, wcv, meta, xv, wb, wd, o3, part, give, pr, sb, rv, res, yst,
           hsem, csem, xsem, wsem, dsem, ysem, psend, precv, ssem, rsem, esend, erecv):
    ey, ex, ec, dev, chip = place()
    t, hd = x_ref.shape
    nc = hd // CW
    f = w2_ref.shape[1]
    half = t // 2
    lo, hi = pl.ds(0, half), pl.ds(half, half)
    per = el
    nb = nc * per
    f = w2_ref.shape[1]
    n = el * cap

    def block(b, go):
        c, j = b // per, lax.rem(b, per)
        cols = pl.ds(pl.multiple_of(c * CW, CW), CW)
        slot = lax.rem(b, NW)

        @pl.when(b < nb)
        def _():
            go(pltpu.make_async_copy(w2_ref.at[j, :, cols], wb.at[slot], wsem.at[slot]))

    def down(c):
        cols = pl.ds(pl.multiple_of(c * CW, CW), CW)
        return pltpu.make_async_copy(ws2_ref.at[:, cols], wd.at[lax.rem(c, 2)], dsem.at[lax.rem(c, 2)])

    def fetch(b):
        block(b, lambda c: c.start())

    def ready(b):
        block(b, lambda c: c.wait())

    def hcopy(e):
        return pltpu.make_async_copy(h_ref.at[e], hv.at[e], hsem.at[e])

    m = pltpu.make_async_copy(meta_ref, meta, csem)
    m.start()
    hcopy(0).start()
    for b in range(NW):
        fetch(b)
    for e in range(1, el):
        hcopy(e).start()
    loads = [pltpu.make_async_copy(sh_ref, shv, xsem.at[0]), pltpu.make_async_copy(x_ref, xv, xsem.at[1]),
             ]

    barrier = pltpu.get_barrier_semaphore()
    for to in "xyp":
        pl.semaphore_signal(barrier, inc=1, device_id=dev[to], device_id_type=MESH)
    pl.semaphore_wait(barrier, 3)

    m.wait()
    slots = lax.broadcasted_iota(jnp.int32, (cap, t), 0).astype(F32)

    def build(s, _):
        parts = [jnp.where(meta[s, e:e + 1, :] == slots, meta[s, el + e:el + e + 1, :], 0.0) for e in range(el)]
        w = jnp.concatenate(parts, axis=0).T
        for i in range(3):
            p = w.astype(BF)
            wcv[s, :, i * n:(i + 1) * n] = p
            w = w - p.astype(F32)
        return 0

    lax.fori_loop(0, 8, build, 0)

    def swap(c, i):
        ch = chip["dxyo"[i]]
        return pltpu.make_async_remote_copy(give.at[lax.rem(c, 2), ch], pr.at[c, ch], psend.at[c, i], precv.at[c, i],
                                            device_id=dev["p"], device_id_type=MESH)

    def ship(c, i, a, b, k=None):
        send, recv = (ssem.at[c, i], rsem.at[c, i]) if k is None else (esend.at[k, i], erecv.at[k, i])
        at = pl.ds(a, b - a)
        return pltpu.make_async_remote_copy(sb.at[i, c, at], rv.at[i, c, at], send, recv, device_id=dev["xy"[i]],
                                            device_id_type=MESH)

    def dispatch(c, op):
        for i in range(2):
            pl.when(c < 2)(lambda: op(ship(c, i, 0, 2)))
            pl.when((c >= 2) & (c < nc - 1))(lambda: op(ship(c, i, 0, 3)))
            pl.when(c == nc - 1)(lambda: op(ship(c, i, 0, 1)))

    def weigh(c, ch, core):
        s = core * 4 + chip[ch]
        return jnp.dot(wcv[s], o3[s], preferred_element_type=F32)

    def compute(c):
        def expert(i, _):
            for e in (2 * i, 2 * i + 1):
                @pl.when(c == 0)
                def _():
                    hcopy(e).wait()
                ready(c * per + e)
            for e in (2 * i, 2 * i + 1):
                o = jnp.dot(hv[e], wb[lax.rem(c * per + e, NW)], preferred_element_type=F32).astype(BF)
                for s in range(8):
                    for j in range(3):
                        o3[s, pl.ds(pl.multiple_of(j * n + e * cap, 16), cap), :] = o[s * cap:(s + 1) * cap]
            for e in (2 * i, 2 * i + 1):
                fetch(c * per + e + NW)
            return 0

        lax.fori_loop(0, el // 2, expert, 0)

        @pl.when(c == 1)
        def _():
            for d in loads + [down(0), down(1)]:
                d.start()

        @pl.when(c >= 2)
        def _():
            for i in range(4):
                swap(c - 2, i).wait_send()
        for i, ch in enumerate("dxyo"):
            give[lax.rem(c, 2), chip[ch]] = weigh(c, ch, 1 - ec)
            swap(c, i).start()
        for ch in "dxyo":
            part[c, chip[ch]] = weigh(c, ch, ec)

    def shared(c):
        down(c).wait()
        p = [jnp.dot(shv[i], wd[lax.rem(c, 2), i * f:(i + 1) * f], preferred_element_type=F32) for i in range(2)]
        cols = pl.ds(pl.multiple_of(c * CW, CW), CW)
        res[c] = xv[:, cols].astype(F32) + (p[0] + p[1]).astype(BF).astype(F32)
        pl.when(c + 2 < nc)(lambda: down(c + 2).start())

    def stage1(c):
        d, x, y = (chip[ch] for ch in "dxy")
        swap(c, 0).wait_recv()
        sb[0, c, 0] = part[c, d, 0:half] + pr[c, d, 0:half]
        sb[1, c, 0] = part[c, d, half:t] + pr[c, d, half:t]
        swap(c, 1).wait_recv()
        sb[0, c, 1] = part[c, x, 0:half] + pr[c, x, 0:half]
        part[c, x, half:t] += pr[c, x, half:t]
        swap(c, 2).wait_recv()
        part[c, y, 0:half] += pr[c, y, 0:half]
        sb[1, c, 1] = part[c, y, half:t] + pr[c, y, half:t]

    def stage2(c, into):
        sb[1, into, 2] = part[c, chip["y"], 0:half] + rv[0, c, 0]
        sb[0, into, 2] = part[c, chip["x"], half:t] + rv[1, c, 0]

    def ycopy(c):
        cols = pl.ds(pl.multiple_of(c * CW, CW), CW)
        return pltpu.make_async_copy(yst.at[lax.rem(c, 2)], y_ref.at[:, cols], ysem.at[lax.rem(c, 2)])

    def stage3(c):
        n2 = lax.rem(c + 2, nc)

        @pl.when(c >= 2)
        def _():
            ycopy(c - 2).wait()
        swap(c, 3).wait_recv()
        own = res[c] + (part[c, chip["o"]] + pr[c, chip["o"]])
        yst[lax.rem(c, 2), 0:half] = (own[0:half] + rv[0, c, 1] + rv[1, n2, 2]).astype(BF)
        yst[lax.rem(c, 2), half:t] = (own[half:t] + rv[0, n2, 2] + rv[1, c, 1]).astype(BF)
        ycopy(c).start()

    def step(c, _):
        compute(c)

        @pl.when(c >= 2)
        def _():
            dispatch(c - 2, lambda d: d.wait_recv())
            stage2(c - 2, c)
        stage1(c)
        dispatch(c, lambda d: d.start())

        @pl.when(c == nc - 1)
        def _():
            for i in range(2):
                ship(nc - 1, i, 1, 3, 0).start()
        @pl.when(c == 2)
        def _():
            for d in loads:
                d.wait()

        @pl.when(c >= 2)
        def _():
            shared(c - 2)

        @pl.when(c >= 4)
        def _():
            stage3(c - 4)
        return 0

    lax.fori_loop(0, nc, step, 0)
    lax.fori_loop(nc - 2, nc, lambda c, v: (shared(c), v)[1], 0)
    for i in range(2):
        ship(nc - 2, i, 0, 3).wait_recv()
    stage2(nc - 2, 0)
    for i in range(2):
        ship(0, i, 2, 3, 1).start()
    stage3(nc - 4)
    for i in range(2):
        ship(nc - 1, i, 0, 1).wait_recv()
    stage2(nc - 1, 1)
    for i in range(2):
        ship(1, i, 2, 3, 2).start()
    for i in range(2):
        ship(nc - 1, i, 1, 3, 0).wait_recv()
    stage3(nc - 3)
    for k in range(2):
        for i in range(2):
            ship(k, i, 2, 3, k + 1).wait_recv()
        stage3(nc - 2 + k)
    for c in (nc - 2, nc - 1):
        ycopy(c).wait()
        for i in range(4):
            swap(c, i).wait_send()
    for i in range(2):
        ship(nc - 1, i, 1, 3, 0).wait_send()
        for k in range(2):
            ship(k, i, 2, 3, k + 1).wait_send()

    def drain(c, _):
        dispatch(c, lambda d: d.wait_send())
        return 0

    lax.fori_loop(0, nc, drain, 0)


def solution(mesh):
    pg = mesh.shape["ey"] * mesh.shape["ex"] * mesh.shape["ec"]

    def local(x, ids, gates, w1, w3, w2, ws1, ws3, ws2):
        t, hd = x.shape
        top = ids.shape[1]
        el, _, f = w1.shape
        ne = el * pg
        cap = min(t, 2 * ((t * top + ne - 1) // ne))
        n = el * cap
        kw = hd // NK
        nc = hd // CW
        dma = pltpu.SemaphoreType.DMA
        h, sh, meta = pl.pallas_call(
            functools.partial(first, el, cap),
            out_shape=(jax.ShapeDtypeStruct((el, pg * cap, f), BF), jax.ShapeDtypeStruct((2, t, f), BF),
                       jax.ShapeDtypeStruct((pg, 2 * el, t), F32)),
            in_specs=[VM, VM] + [ANY] * 5, out_specs=(ANY,) * 3,
            scratch_shapes=[
                pltpu.VMEM((NK, pg, t, kw), BF), pltpu.VMEM((el, pg * cap, 2 * f), F32), pltpu.VMEM((NS, kw, 2 * f), BF),
                pltpu.VMEM((pg, n, t), BF), pltpu.VMEM((el, pg, cap, kw), BF), pltpu.VMEM((2, pg * cap, f), BF),
                pltpu.VMEM((pg, 2 * el, t), F32), pltpu.VMEM((pg, 2 * el, t), F32),
                dma((NK,)), dma((NS, 2)), dma((2,)), dma, dma((8,)), dma((8,)), dma((NK, 11)), dma((NK, 11))],
            compiler_params=pltpu.CompilerParams(collective_id=0, has_side_effects=True, vmem_limit_bytes=VLIM),
        )(ids.T, gates.T, x, w1, w3, ws1, ws3)
        return pl.pallas_call(
            functools.partial(second, el, cap),
            out_shape=jax.ShapeDtypeStruct((t, hd), BF),
            in_specs=[ANY] * 6, out_specs=ANY,
            scratch_shapes=[
                pltpu.VMEM((el, pg * cap, f), BF), pltpu.VMEM((2, t, f), BF), pltpu.VMEM((pg, t, 3 * n), BF), pltpu.VMEM((pg, 2 * el, t), F32),
                pltpu.VMEM((t, hd), BF), pltpu.VMEM((NW, f, CW), BF), pltpu.VMEM((2, 2 * f, CW), BF), pltpu.VMEM((pg, 3 * n, CW), BF),
                pltpu.VMEM((nc, 4, t, CW), F32), pltpu.VMEM((2, 4, t, CW), F32), pltpu.VMEM((nc, 4, t, CW), F32),
                pltpu.VMEM((2, nc, 3, t // 2, CW), F32), pltpu.VMEM((2, nc, 3, t // 2, CW), F32),
                pltpu.VMEM((nc, t, CW), F32), pltpu.VMEM((2, t, CW), BF),
                dma((el,)), dma, dma((2,)), dma((NW,)), dma((2,)), dma((2,)), dma((nc, 4)), dma((nc, 4)), dma((nc, 2)), dma((nc, 2)),
                dma((3, 2)), dma((3, 2))],
            compiler_params=pltpu.CompilerParams(collective_id=1, has_side_effects=True, vmem_limit_bytes=VLIM),
        )(h, sh, meta, x, w2, ws2)

    return jax.shard_map(local, mesh=mesh,
                         in_specs=(P(ALL), P(ALL), P(ALL), P(EXP), P(EXP), P(EXP), P(), P(), P()),
                         out_specs=P(ALL), check_vma=False)
```

```python
import functools

import jax
import jax.numpy as jnp
from jax import lax
from jax.experimental import pallas as pl
from jax.experimental.pallas import tpu as pltpu
from jax.sharding import PartitionSpec as P

EXP = ("ey", "ex", "ec")
ALL = ("dp", "ey", "ex", "ec")
MESH = pl.DeviceIdType.MESH
ANY = pl.BlockSpec(memory_space=pl.ANY)
VM = pl.BlockSpec(memory_space=pltpu.VMEM)
BF = jnp.bfloat16
F32 = jnp.float32
VLIM = 67043328

NK = 4
NS = 5
CW = 256
NW = 8
SLAB = 256


def place():
    ey, ex, ec = (lax.axis_index(a) for a in EXP)
    dev = {"x": dict(ey=ey, ex=1 - ex, ec=ec), "y": dict(ey=1 - ey, ex=ex, ec=ec), "p": dict(ey=ey, ex=ex, ec=1 - ec)}
    chip = {"o": ey * 2 + ex, "x": ey * 2 + 1 - ex, "y": (1 - ey) * 2 + ex, "d": (1 - ey) * 2 + 1 - ex}
    return ey, ex, ec, dev, chip


def silu_mul(a, b):
    return (a * jax.nn.sigmoid(a) * b).astype(BF)


def first(el, cap, ids_ref, gates_ref, x_ref, w1_ref, w3_ref, ws1_ref, ws3_ref, h_ref, sh_ref, meta_ref,
          xg, acc, wb, disp, xe, hst, mout, meta,
          xsem, wsem, osem, csem, msend, mrecv, ssem, rsem):
    ey, ex, ec, dev, chip = place()
    t = x_ref.shape[0]
    kw = x_ref.shape[1] // NK
    f = w1_ref.shape[2]
    half = t // 2
    lo, hi, full = pl.ds(0, half), pl.ds(half, half), pl.ds(0, t)
    mine = {c: ec * 4 + chip[c] for c in "oxyd"}
    theirs = {c: (1 - ec) * 4 + chip[c] for c in "oxyd"}
    nsh = 2 * NK
    nb = nsh + NK * el

    def block(b, go):
        slot = lax.rem(b, NS)

        @pl.when(b < nsh)
        def _():
            rows = pl.ds(pl.multiple_of(lax.rem(b, NK) * kw, kw), kw)
            cols = pl.ds(pl.multiple_of((b // NK) * f, 128), f)
            for i, w in enumerate((ws1_ref, ws3_ref)):
                go(pltpu.make_async_copy(w.at[rows, cols], wb.at[slot, :, pl.ds(i * f, f)], wsem.at[slot, i]))

        @pl.when((b >= nsh) & (b < nb))
        def _():
            q = b - nsh
            rows = pl.ds(pl.multiple_of((q // el) * kw, kw), kw)
            for i, w in enumerate((w1_ref, w3_ref)):
                go(pltpu.make_async_copy(w.at[lax.rem(q, el), rows], wb.at[slot, :, pl.ds(i * f, f)], wsem.at[slot, i]))

    def fetch(b):
        block(b, lambda c: c.start())

    def ready(b):
        block(b, lambda c: c.wait())

    def pair(b):
        for j in range(2):
            fetch(b + NS - 2 + j)
        for j in range(2):
            ready(b + j)

    for k in range(NK):
        pltpu.make_async_copy(x_ref.at[:, pl.ds(k * kw, kw)], xg.at[k, mine["o"]], xsem.at[k]).start()
    for b in range(NS - 2):
        fetch(b)

    ne = el * 8
    row = lax.broadcasted_iota(jnp.int32, (ne, t), 0)
    chosen = jnp.zeros((ne, t), F32)
    gate = jnp.zeros((ne, t), F32)
    for j in range(ids_ref.shape[0]):
        hit = ids_ref[j:j + 1, :] == row
        chosen = jnp.where(hit, 1.0, chosen)
        gate = jnp.where(hit, gates_ref[j:j + 1, :], gate)
    before = (lax.broadcasted_iota(jnp.int32, (t, t), 0) < lax.broadcasted_iota(jnp.int32, (t, t), 1))
    rank = jnp.dot(chosen.astype(BF), before.astype(F32).astype(BF), preferred_element_type=F32)
    rank = jnp.where(chosen > 0.0, rank, -1.0)
    for d in range(8):
        mout[d, 0:el, :] = rank[d * el:(d + 1) * el]
        mout[d, el:2 * el, :] = gate[d * el:(d + 1) * el]

    barrier = pltpu.get_barrier_semaphore()
    others = [(a, b, c) for a in (0, 1) for b in (0, 1) for c in (0, 1) if a + b + c]

    def flip(o):
        return [lax.rem(v + s, 2) for v, s in zip((ey, ex, ec), o)]

    for o in others:
        y2, x2, c2 = flip(o)
        pl.semaphore_signal(barrier, inc=1, device_id=dict(ey=y2, ex=x2, ec=c2), device_id_type=MESH)
    pl.semaphore_wait(barrier, len(others))

    for k in range(NK):
        pltpu.make_async_copy(x_ref.at[:, pl.ds(k * kw, kw)], xg.at[k, mine["o"]], xsem.at[k]).wait()

    def remote(k, src, rows, chan, to):
        ref = xg.at[k, src, rows]
        return pltpu.make_async_remote_copy(ref, ref, ssem.at[k, chan], rsem.at[k, chan], device_id=dev[to],
                                            device_id_type=MESH)

    def direct(k):
        for rows, chan, to in ((lo, 0, "x"), (hi, 1, "y"), (hi, 9, "x"), (lo, 10, "y"), (full, 2, "p")):
            remote(k, mine["o"], rows, chan, to).start()

    def relay(k):
        remote(k, mine["x"], lo, 0, "x").wait_recv()
        remote(k, mine["x"], lo, 3, "y").start()
        remote(k, mine["y"], hi, 1, "y").wait_recv()
        remote(k, mine["y"], hi, 4, "x").start()

    def corner(k):
        remote(k, mine["x"], hi, 9, "x").wait_recv()
        remote(k, mine["x"], full, 5, "p").start()
        remote(k, mine["y"], lo, 10, "y").wait_recv()
        remote(k, mine["y"], full, 6, "p").start()
        remote(k, mine["d"], lo, 3, "y").wait_recv()
        remote(k, mine["d"], lo, 7, "p").start()
        remote(k, mine["d"], hi, 4, "x").wait_recv()
        remote(k, mine["d"], hi, 8, "p").start()

    def arrived(k):
        remote(k, theirs["o"], full, 2, "p").wait_recv()
        remote(k, theirs["x"], full, 5, "p").wait_recv()
        remote(k, theirs["y"], full, 6, "p").wait_recv()
        remote(k, theirs["d"], lo, 7, "p").wait_recv()
        remote(k, theirs["d"], hi, 8, "p").wait_recv()

    def sent(k):
        for src, rows, chan, to in ((mine["o"], lo, 0, "x"), (mine["o"], hi, 9, "x"), (mine["o"], hi, 1, "y"),
                                    (mine["o"], lo, 10, "y"), (mine["o"], full, 2, "p"),
                                    (mine["x"], lo, 3, "y"), (mine["y"], hi, 4, "x"), (mine["x"], full, 5, "p"),
                                    (mine["y"], full, 6, "p"), (mine["d"], lo, 7, "p"), (mine["d"], hi, 8, "p")):
            remote(k, src, rows, chan, to).wait_send()

    def mcopy(o, back=False):
        y2, x2, c2 = flip(o)
        num = c2 * 4 + y2 * 2 + x2
        idx = y2 * 4 + x2 * 2 + c2
        src, dst = (meta.at[num], num) if back else (mout.at[idx], mine["o"])
        return pltpu.make_async_remote_copy(src, meta.at[dst], msend.at[num], mrecv.at[dst],
                                            device_id=dict(ey=y2, ex=x2, ec=c2), device_id_type=MESH)

    for o in others:
        mcopy(o).start()
    direct(0)

    for hf in range(2):
        acc[0, 0:t, :] = jnp.zeros((t, 2 * f), F32)

        def body(i, _):
            b = hf * NK + 2 * i
            pair(b)
            for at in [slice(v, v + SLAB) for v in range(0, 2 * f, SLAB)]:
                d = [jnp.dot(xg[2 * i + j, mine["o"]], wb[lax.rem(b + j, NS), :, at], preferred_element_type=F32)
                     for j in range(2)]
                acc[0, 0:t, at] += d[0] + d[1]
            return 0

        lax.fori_loop(0, NK // 2, body, 0)
        for v in range(0, f, 128):
            hst[hf, 0:t, v:v + 128] = silu_mul(acc[0, 0:t, v:v + 128], acc[0, 0:t, f + v:f + v + 128])
        pltpu.make_async_copy(hst.at[hf, 0:t], sh_ref.at[hf], osem.at[hf]).start()
        if hf == 0:
            relay(0)
            direct(1)


    meta[mine["o"]] = mout[ey * 4 + ex * 2 + ec]
    for o in others:
        mcopy(o, True).wait_recv()
    keep = pltpu.make_async_copy(meta, meta_ref, csem)
    keep.start()
    slots = lax.broadcasted_iota(jnp.int32, (cap, t), 0).astype(F32)

    def build(s, _):
        for e in range(el):
            sel = meta[s, e:e + 1, :] == slots
            disp[s, e * cap:(e + 1) * cap, :] = jnp.where(sel, 1.0, 0.0).astype(BF)
        return 0

    lax.fori_loop(0, 8, build, 0)

    def gather(k):
        def body(s, _):
            r = jnp.dot(disp[s], xg[k, s], preferred_element_type=F32).astype(BF)
            for e in range(el):
                xe[e, s] = r[e * cap:(e + 1) * cap]
            return 0

        lax.fori_loop(0, 8, body, 0)

    def products(k, i, use):
        b = nsh + k * el + 2 * i
        pair(b)
        for j in range(2):
            slot = lax.rem(b + j, NS)
            u = xe[2 * i + j].reshape(8 * cap, kw)
            use(2 * i + j, lambda at, u=u, slot=slot: jnp.dot(u, wb[slot, :, at], preferred_element_type=F32))

    def slabs(w):
        return [slice(i, min(i + w, 2 * f)) for i in range(0, 2 * f, w)]

    def start_acc(i, _):
        def use(e, part):
            for at in slabs(SLAB):
                acc[e, :, at] = part(at)
        products(0, i, use)
        return 0

    corner(0)
    arrived(0)
    gather(0)
    lax.fori_loop(0, el // 8, start_acc, 0)
    relay(1)
    direct(2)
    lax.fori_loop(el // 8, el // 2 - el // 8, start_acc, 0)
    corner(1)
    lax.fori_loop(el // 2 - el // 8, el // 2, start_acc, 0)

    def more(k, _):
        arrived(k)
        gather(k)

        def add(i, _):
            def use(e, part):
                for at in slabs(SLAB):
                    acc[e, :, at] += part(at)
            products(k, i, use)
            return 0

        lax.fori_loop(0, el // 8, add, 0)
        relay(k + 1)

        @pl.when(k < NK - 2)
        def _():
            direct(k + 2)
        lax.fori_loop(el // 8, el // 2 - el // 8, add, 0)
        corner(k + 1)
        lax.fori_loop(el // 2 - el // 8, el // 2, add, 0)
        return 0

    lax.fori_loop(1, NK - 1, more, 0)

    arrived(NK - 1)
    gather(NK - 1)
    for hf in range(2):
        pltpu.make_async_copy(hst.at[hf, 0:t], sh_ref.at[hf], osem.at[hf]).wait()

    def last(i, _):
        @pl.when(i >= 1)
        def _():
            for j in range(2):
                pltpu.make_async_copy(hst.at[j], h_ref.at[2 * i - 2 + j], osem.at[j]).wait()

        def use(e, part):
            slot = lax.rem(e, 2)
            nt = f // 128
            live = {}
            order = [nt // 2] + [v for i in range(nt // 2) for v in (i, nt // 2 + 1 + i)]
            for i in order:
                at = slice(i * 256, i * 256 + 256)
                d = acc[e, :, at] + part(at)
                for j in (2 * i, 2 * i + 1):
                    live[j] = d[:, (j - 2 * i) * 128:(j - 2 * i) * 128 + 128]
                    if j == nt - 1:
                        acc[e, :, j * 128:j * 128 + 128] = live.pop(j)
                for j in [v for v in live if v < nt and v + nt in live]:
                    hst[slot, :, j * 128:j * 128 + 128] = silu_mul(live.pop(j), live.pop(j + nt))
                if 2 * nt - 1 in live:
                    j = nt - 1
                    hst[slot, :, j * 128:j * 128 + 128] = silu_mul(acc[e, :, j * 128:j * 128 + 128], live.pop(2 * nt - 1))
            pltpu.make_async_copy(hst.at[slot], h_ref.at[e], osem.at[slot]).start()
        products(NK - 1, i, use)
        return 0

    lax.fori_loop(0, el // 2, last, 0)

    keep.wait()
    for e in (el - 2, el - 1):
        pltpu.make_async_copy(hst.at[e % 2], h_ref.at[e], osem.at[e % 2]).wait()
    for o in others:
        mcopy(o).wait_send()
    for k in range(NK):
        sent(k)


def second(el, cap, h_ref, sh_ref, meta_ref, x_ref, w2_ref, ws2_ref, y_ref,
           hv, shv, wcv, meta, xv, wb, wd, o3, part, give, pr, sb, rv, res, yst,
           hsem, csem, xsem, wsem, dsem, ysem, psend, precv, ssem, rsem, esend, erecv):
    ey, ex, ec, dev, chip = place()
    t, hd = x_ref.shape
    nc = hd // CW
    f = w2_ref.shape[1]
    half = t // 2
    lo, hi = pl.ds(0, half), pl.ds(half, half)
    per = el
    nb = nc * per
    f = w2_ref.shape[1]
    n = el * cap

    def block(b, go):
        c, j = b // per, lax.rem(b, per)
        cols = pl.ds(pl.multiple_of(c * CW, CW), CW)
        slot = lax.rem(b, NW)

        @pl.when(b < nb)
        def _():
            go(pltpu.make_async_copy(w2_ref.at[j, :, cols], wb.at[slot], wsem.at[slot]))

    def down(c):
        cols = pl.ds(pl.multiple_of(c * CW, CW), CW)
        return pltpu.make_async_copy(ws2_ref.at[:, cols], wd.at[lax.rem(c, 2)], dsem.at[lax.rem(c, 2)])

    def fetch(b):
        block(b, lambda c: c.start())

    def ready(b):
        block(b, lambda c: c.wait())

    def hcopy(e):
        return pltpu.make_async_copy(h_ref.at[e], hv.at[e], hsem.at[e])

    m = pltpu.make_async_copy(meta_ref, meta, csem)
    m.start()
    hcopy(0).start()
    for b in range(NW):
        fetch(b)
    for e in range(1, el):
        hcopy(e).start()
    loads = [pltpu.make_async_copy(sh_ref, shv, xsem.at[0]), pltpu.make_async_copy(x_ref, xv, xsem.at[1]),
             ]

    barrier = pltpu.get_barrier_semaphore()
    for to in "xyp":
        pl.semaphore_signal(barrier, inc=1, device_id=dev[to], device_id_type=MESH)
    pl.semaphore_wait(barrier, 3)

    m.wait()
    slots = lax.broadcasted_iota(jnp.int32, (cap, t), 0).astype(F32)

    def build(s, _):
        parts = [jnp.where(meta[s, e:e + 1, :] == slots, meta[s, el + e:el + e + 1, :], 0.0) for e in range(el)]
        w = jnp.concatenate(parts, axis=0).T
        for i in range(3):
            p = w.astype(BF)
            wcv[s, :, i * n:(i + 1) * n] = p
            w = w - p.astype(F32)
        return 0

    lax.fori_loop(0, 8, build, 0)

    def swap(c, i):
        ch = chip["dxyo"[i]]
        return pltpu.make_async_remote_copy(give.at[lax.rem(c, 2), ch], pr.at[c, ch], psend.at[c, i], precv.at[c, i],
                                            device_id=dev["p"], device_id_type=MESH)

    def ship(c, i, a, b, k=None):
        send, recv = (ssem.at[c, i], rsem.at[c, i]) if k is None else (esend.at[k, i], erecv.at[k, i])
        at = pl.ds(a, b - a)
        return pltpu.make_async_remote_copy(sb.at[i, c, at], rv.at[i, c, at], send, recv, device_id=dev["xy"[i]],
                                            device_id_type=MESH)

    def dispatch(c, op):
        for i in range(2):
            pl.when(c < 2)(lambda: op(ship(c, i, 0, 2)))
            pl.when((c >= 2) & (c < nc - 1))(lambda: op(ship(c, i, 0, 3)))
            pl.when(c == nc - 1)(lambda: op(ship(c, i, 0, 1)))

    def weigh(c, ch, core):
        s = core * 4 + chip[ch]
        return jnp.dot(wcv[s], o3[s], preferred_element_type=F32)

    def compute(c):
        def expert(i, _):
            for e in (2 * i, 2 * i + 1):
                @pl.when(c == 0)
                def _():
                    hcopy(e).wait()
                ready(c * per + e)
            for e in (2 * i, 2 * i + 1):
                o = jnp.dot(hv[e], wb[lax.rem(c * per + e, NW)], preferred_element_type=F32).astype(BF)
                for s in range(8):
                    for j in range(3):
                        o3[s, pl.ds(pl.multiple_of(j * n + e * cap, 16), cap), :] = o[s * cap:(s + 1) * cap]
            for e in (2 * i, 2 * i + 1):
                fetch(c * per + e + NW)
            return 0

        lax.fori_loop(0, el // 2, expert, 0)

        @pl.when(c == 1)
        def _():
            for d in loads + [down(0), down(1)]:
                d.start()

        @pl.when(c >= 2)
        def _():
            for i in range(4):
                swap(c - 2, i).wait_send()
        for i, ch in enumerate("dxyo"):
            give[lax.rem(c, 2), chip[ch]] = weigh(c, ch, 1 - ec)
            swap(c, i).start()
        for ch in "dxyo":
            part[c, chip[ch]] = weigh(c, ch, ec)

    def shared(c):
        down(c).wait()
        p = [jnp.dot(shv[i], wd[lax.rem(c, 2), i * f:(i + 1) * f], preferred_element_type=F32) for i in range(2)]
        cols = pl.ds(pl.multiple_of(c * CW, CW), CW)
        res[c] = xv[:, cols].astype(F32) + (p[0] + p[1]).astype(BF).astype(F32)
        pl.when(c + 2 < nc)(lambda: down(c + 2).start())

    def stage1(c):
        d, x, y = (chip[ch] for ch in "dxy")
        swap(c, 0).wait_recv()
        sb[0, c, 0] = part[c, d, 0:half] + pr[c, d, 0:half]
        sb[1, c, 0] = part[c, d, half:t] + pr[c, d, half:t]
        swap(c, 1).wait_recv()
        sb[0, c, 1] = part[c, x, 0:half] + pr[c, x, 0:half]
        part[c, x, half:t] += pr[c, x, half:t]
        swap(c, 2).wait_recv()
        part[c, y, 0:half] += pr[c, y, 0:half]
        sb[1, c, 1] = part[c, y, half:t] + pr[c, y, half:t]

    def stage2(c, into):
        sb[1, into, 2] = part[c, chip["y"], 0:half] + rv[0, c, 0]
        sb[0, into, 2] = part[c, chip["x"], half:t] + rv[1, c, 0]

    def ycopy(c):
        cols = pl.ds(pl.multiple_of(c * CW, CW), CW)
        return pltpu.make_async_copy(yst.at[lax.rem(c, 2)], y_ref.at[:, cols], ysem.at[lax.rem(c, 2)])

    def stage3(c):
        n2 = lax.rem(c + 2, nc)

        @pl.when(c >= 2)
        def _():
            ycopy(c - 2).wait()
        swap(c, 3).wait_recv()
        own = res[c] + (part[c, chip["o"]] + pr[c, chip["o"]])
        yst[lax.rem(c, 2), 0:half] = (own[0:half] + rv[0, c, 1] + rv[1, n2, 2]).astype(BF)
        yst[lax.rem(c, 2), half:t] = (own[half:t] + rv[0, n2, 2] + rv[1, c, 1]).astype(BF)
        ycopy(c).start()

    def step(c, _):
        compute(c)

        @pl.when(c >= 2)
        def _():
            dispatch(c - 2, lambda d: d.wait_recv())
            stage2(c - 2, c)
        stage1(c)
        dispatch(c, lambda d: d.start())

        @pl.when(c == nc - 1)
        def _():
            for i in range(2):
                ship(nc - 1, i, 1, 3, 0).start()
        @pl.when(c == 2)
        def _():
            for d in loads:
                d.wait()

        @pl.when(c >= 2)
        def _():
            shared(c - 2)

        @pl.when(c >= 4)
        def _():
            stage3(c - 4)
        return 0

    lax.fori_loop(0, nc, step, 0)
    lax.fori_loop(nc - 2, nc, lambda c, v: (shared(c), v)[1], 0)
    for i in range(2):
        ship(nc - 2, i, 0, 3).wait_recv()
    stage2(nc - 2, 0)
    for i in range(2):
        ship(0, i, 2, 3, 1).start()
    stage3(nc - 4)
    for i in range(2):
        ship(nc - 1, i, 0, 1).wait_recv()
    stage2(nc - 1, 1)
    for i in range(2):
        ship(1, i, 2, 3, 2).start()
    for i in range(2):
        ship(nc - 1, i, 1, 3, 0).wait_recv()
    stage3(nc - 3)
    for k in range(2):
        for i in range(2):
            ship(k, i, 2, 3, k + 1).wait_recv()
        stage3(nc - 2 + k)
    for c in (nc - 2, nc - 1):
        ycopy(c).wait()
        for i in range(4):
            swap(c, i).wait_send()
    for i in range(2):
        ship(nc - 1, i, 1, 3, 0).wait_send()
        for k in range(2):
            ship(k, i, 2, 3, k + 1).wait_send()

    def drain(c, _):
        dispatch(c, lambda d: d.wait_send())
        return 0

    lax.fori_loop(0, nc, drain, 0)


def solution(mesh):
    pg = mesh.shape["ey"] * mesh.shape["ex"] * mesh.shape["ec"]

    def local(x, ids, gates, w1, w3, w2, ws1, ws3, ws2):
        t, hd = x.shape
        top = ids.shape[1]
        el, _, f = w1.shape
        ne = el * pg
        cap = min(t, 2 * ((t * top + ne - 1) // ne))
        n = el * cap
        kw = hd // NK
        nc = hd // CW
        dma = pltpu.SemaphoreType.DMA
        h, sh, meta = pl.pallas_call(
            functools.partial(first, el, cap),
            out_shape=(jax.ShapeDtypeStruct((el, pg * cap, f), BF), jax.ShapeDtypeStruct((2, t, f), BF),
                       jax.ShapeDtypeStruct((pg, 2 * el, t), F32)),
            in_specs=[VM, VM] + [ANY] * 5, out_specs=(ANY,) * 3,
            scratch_shapes=[
                pltpu.VMEM((NK, pg, t, kw), BF), pltpu.VMEM((el, pg * cap, 2 * f), F32), pltpu.VMEM((NS, kw, 2 * f), BF),
                pltpu.VMEM((pg, n, t), BF), pltpu.VMEM((el, pg, cap, kw), BF), pltpu.VMEM((2, pg * cap, f), BF),
                pltpu.VMEM((pg, 2 * el, t), F32), pltpu.VMEM((pg, 2 * el, t), F32),
                dma((NK,)), dma((NS, 2)), dma((2,)), dma, dma((8,)), dma((8,)), dma((NK, 11)), dma((NK, 11))],
            compiler_params=pltpu.CompilerParams(collective_id=0, has_side_effects=True, vmem_limit_bytes=VLIM),
        )(ids.T, gates.T, x, w1, w3, ws1, ws3)
        return pl.pallas_call(
            functools.partial(second, el, cap),
            out_shape=jax.ShapeDtypeStruct((t, hd), BF),
            in_specs=[ANY] * 6, out_specs=ANY,
            scratch_shapes=[
                pltpu.VMEM((el, pg * cap, f), BF), pltpu.VMEM((2, t, f), BF), pltpu.VMEM((pg, t, 3 * n), BF), pltpu.VMEM((pg, 2 * el, t), F32),
                pltpu.VMEM((t, hd), BF), pltpu.VMEM((NW, f, CW), BF), pltpu.VMEM((2, 2 * f, CW), BF), pltpu.VMEM((pg, 3 * n, CW), BF),
                pltpu.VMEM((nc, 4, t, CW), F32), pltpu.VMEM((2, 4, t, CW), F32), pltpu.VMEM((nc, 4, t, CW), F32),
                pltpu.VMEM((2, nc, 3, t // 2, CW), F32), pltpu.VMEM((2, nc, 3, t // 2, CW), F32),
                pltpu.VMEM((nc, t, CW), F32), pltpu.VMEM((2, t, CW), BF),
                dma((el,)), dma, dma((2,)), dma((NW,)), dma((2,)), dma((2,)), dma((nc, 4)), dma((nc, 4)), dma((nc, 2)), dma((nc, 2)),
                dma((3, 2)), dma((3, 2))],
            compiler_params=pltpu.CompilerParams(collective_id=1, has_side_effects=True, vmem_limit_bytes=VLIM),
        )(h, sh, meta, x, w2, ws2)

    return jax.shard_map(local, mesh=mesh,
                         in_specs=(P(ALL), P(ALL), P(ALL), P(EXP), P(EXP), P(EXP), P(), P(), P()),
                         out_specs=P(ALL), check_vma=False)
```

```python
import functools

import jax
import jax.numpy as jnp
from jax import lax
from jax.experimental import pallas as pl
from jax.experimental.pallas import tpu as pltpu
from jax.sharding import PartitionSpec as P

EXP = ("ey", "ex", "ec")
ALL = ("dp", "ey", "ex", "ec")
MESH = pl.DeviceIdType.MESH
ANY = pl.BlockSpec(memory_space=pl.ANY)
VM = pl.BlockSpec(memory_space=pltpu.VMEM)
BF = jnp.bfloat16
F32 = jnp.float32
VLIM = 67043328

NK = 4
NS = 5
CW = 256
NW = 8
SLAB = 256


def place():
    ey, ex, ec = (lax.axis_index(a) for a in EXP)
    dev = {"x": dict(ey=ey, ex=1 - ex, ec=ec), "y": dict(ey=1 - ey, ex=ex, ec=ec), "p": dict(ey=ey, ex=ex, ec=1 - ec)}
    chip = {"o": ey * 2 + ex, "x": ey * 2 + 1 - ex, "y": (1 - ey) * 2 + ex, "d": (1 - ey) * 2 + 1 - ex}
    return ey, ex, ec, dev, chip


def silu_mul(a, b):
    return (a * jax.nn.sigmoid(a) * b).astype(BF)


def first(el, cap, ids_ref, gates_ref, x_ref, w1_ref, w3_ref, ws1_ref, ws3_ref, h_ref, sh_ref, meta_ref,
          xg, acc, wb, disp, xe, hst, mout, meta,
          xsem, wsem, osem, csem, msend, mrecv, ssem, rsem):
    ey, ex, ec, dev, chip = place()
    t = x_ref.shape[0]
    kw = x_ref.shape[1] // NK
    f = w1_ref.shape[2]
    half = t // 2
    lo, hi, full = pl.ds(0, half), pl.ds(half, half), pl.ds(0, t)
    mine = {c: ec * 4 + chip[c] for c in "oxyd"}
    theirs = {c: (1 - ec) * 4 + chip[c] for c in "oxyd"}
    nsh = 2 * NK
    nb = nsh + NK * el

    def block(b, go):
        slot = lax.rem(b, NS)

        @pl.when(b < nsh)
        def _():
            rows = pl.ds(pl.multiple_of(lax.rem(b, NK) * kw, kw), kw)
            cols = pl.ds(pl.multiple_of((b // NK) * f, 128), f)
            for i, w in enumerate((ws1_ref, ws3_ref)):
                go(pltpu.make_async_copy(w.at[rows, cols], wb.at[slot, :, pl.ds(i * f, f)], wsem.at[slot, i]))

        @pl.when((b >= nsh) & (b < nb))
        def _():
            q = b - nsh
            rows = pl.ds(pl.multiple_of((q // el) * kw, kw), kw)
            for i, w in enumerate((w1_ref, w3_ref)):
                go(pltpu.make_async_copy(w.at[lax.rem(q, el), rows], wb.at[slot, :, pl.ds(i * f, f)], wsem.at[slot, i]))

    def fetch(b):
        block(b, lambda c: c.start())

    def ready(b):
        block(b, lambda c: c.wait())

    def pair(b):
        for j in range(2):
            fetch(b + NS - 2 + j)
        for j in range(2):
            ready(b + j)

    for k in range(NK):
        pltpu.make_async_copy(x_ref.at[:, pl.ds(k * kw, kw)], xg.at[k, mine["o"]], xsem.at[k]).start()
    for b in range(NS - 2):
        fetch(b)

    barrier = pltpu.get_barrier_semaphore()
    others = [(a, b, c) for a in (0, 1) for b in (0, 1) for c in (0, 1) if a + b + c]

    def flip(o):
        return [lax.rem(v + s, 2) for v, s in zip((ey, ex, ec), o)]

    for o in others:
        y2, x2, c2 = flip(o)
        pl.semaphore_signal(barrier, inc=1, device_id=dict(ey=y2, ex=x2, ec=c2), device_id_type=MESH)
    ne = el * 8
    row = lax.broadcasted_iota(jnp.int32, (ne, t), 0)
    chosen = jnp.zeros((ne, t), F32)
    gate = jnp.zeros((ne, t), F32)
    for j in range(ids_ref.shape[0]):
        hit = ids_ref[j:j + 1, :] == row
        chosen = jnp.where(hit, 1.0, chosen)
        gate = jnp.where(hit, gates_ref[j:j + 1, :], gate)
    before = (lax.broadcasted_iota(jnp.int32, (t, t), 0) < lax.broadcasted_iota(jnp.int32, (t, t), 1))
    rank = jnp.dot(chosen.astype(BF), before.astype(F32).astype(BF), preferred_element_type=F32)
    rank = jnp.where(chosen > 0.0, rank, -1.0)
    for d in range(8):
        mout[d, 0:el, :] = rank[d * el:(d + 1) * el]
        mout[d, el:2 * el, :] = gate[d * el:(d + 1) * el]

    pl.semaphore_wait(barrier, len(others))

    for k in range(NK):
        pltpu.make_async_copy(x_ref.at[:, pl.ds(k * kw, kw)], xg.at[k, mine["o"]], xsem.at[k]).wait()

    def remote(k, src, rows, chan, to):
        ref = xg.at[k, src, rows]
        return pltpu.make_async_remote_copy(ref, ref, ssem.at[k, chan], rsem.at[k, chan], device_id=dev[to],
                                            device_id_type=MESH)

    def direct(k):
        for rows, chan, to in ((lo, 0, "x"), (hi, 1, "y"), (hi, 9, "x"), (lo, 10, "y"), (full, 2, "p")):
            remote(k, mine["o"], rows, chan, to).start()

    def relay(k):
        remote(k, mine["x"], lo, 0, "x").wait_recv()
        remote(k, mine["x"], lo, 3, "y").start()
        remote(k, mine["y"], hi, 1, "y").wait_recv()
        remote(k, mine["y"], hi, 4, "x").start()

    def corner(k):
        remote(k, mine["x"], hi, 9, "x").wait_recv()
        remote(k, mine["x"], full, 5, "p").start()
        remote(k, mine["y"], lo, 10, "y").wait_recv()
        remote(k, mine["y"], full, 6, "p").start()
        remote(k, mine["d"], lo, 3, "y").wait_recv()
        remote(k, mine["d"], lo, 7, "p").start()
        remote(k, mine["d"], hi, 4, "x").wait_recv()
        remote(k, mine["d"], hi, 8, "p").start()

    def arrived(k):
        remote(k, theirs["o"], full, 2, "p").wait_recv()
        remote(k, theirs["x"], full, 5, "p").wait_recv()
        remote(k, theirs["y"], full, 6, "p").wait_recv()
        remote(k, theirs["d"], lo, 7, "p").wait_recv()
        remote(k, theirs["d"], hi, 8, "p").wait_recv()

    def sent(k):
        for src, rows, chan, to in ((mine["o"], lo, 0, "x"), (mine["o"], hi, 9, "x"), (mine["o"], hi, 1, "y"),
                                    (mine["o"], lo, 10, "y"), (mine["o"], full, 2, "p"),
                                    (mine["x"], lo, 3, "y"), (mine["y"], hi, 4, "x"), (mine["x"], full, 5, "p"),
                                    (mine["y"], full, 6, "p"), (mine["d"], lo, 7, "p"), (mine["d"], hi, 8, "p")):
            remote(k, src, rows, chan, to).wait_send()

    def mcopy(o, back=False):
        y2, x2, c2 = flip(o)
        num = c2 * 4 + y2 * 2 + x2
        idx = y2 * 4 + x2 * 2 + c2
        src, dst = (meta.at[num], num) if back else (mout.at[idx], mine["o"])
        return pltpu.make_async_remote_copy(src, meta.at[dst], msend.at[num], mrecv.at[dst],
                                            device_id=dict(ey=y2, ex=x2, ec=c2), device_id_type=MESH)

    for o in others:
        mcopy(o).start()
    direct(0)

    for hf in range(2):
        acc[0, 0:t, :] = jnp.zeros((t, 2 * f), F32)

        def body(i, _):
            b = hf * NK + 2 * i
            pair(b)
            for at in [slice(v, v + SLAB) for v in range(0, 2 * f, SLAB)]:
                d = [jnp.dot(xg[2 * i + j, mine["o"]], wb[lax.rem(b + j, NS), :, at], preferred_element_type=F32)
                     for j in range(2)]
                acc[0, 0:t, at] += d[0] + d[1]
            return 0

        lax.fori_loop(0, NK // 2, body, 0)
        for v in range(0, f, 128):
            hst[hf, 0:t, v:v + 128] = silu_mul(acc[0, 0:t, v:v + 128], acc[0, 0:t, f + v:f + v + 128])
        pltpu.make_async_copy(hst.at[hf, 0:t], sh_ref.at[hf], osem.at[hf]).start()
        if hf == 0:
            relay(0)
            direct(1)


    meta[mine["o"]] = mout[ey * 4 + ex * 2 + ec]
    for o in others:
        mcopy(o, True).wait_recv()
    keep = pltpu.make_async_copy(meta, meta_ref, csem)
    keep.start()
    slots = lax.broadcasted_iota(jnp.int32, (cap, t), 0).astype(F32)

    def build(s, _):
        for e in range(el):
            sel = meta[s, e:e + 1, :] == slots
            disp[s, e * cap:(e + 1) * cap, :] = jnp.where(sel, 1.0, 0.0).astype(BF)
        return 0

    lax.fori_loop(0, 8, build, 0)

    def gather(k):
        def body(s, _):
            r = jnp.dot(disp[s], xg[k, s], preferred_element_type=F32).astype(BF)
            for e in range(el):
                xe[e, s] = r[e * cap:(e + 1) * cap]
            return 0

        lax.fori_loop(0, 8, body, 0)

    def products(k, i, use):
        b = nsh + k * el + 2 * i
        pair(b)
        for j in range(2):
            slot = lax.rem(b + j, NS)
            u = xe[2 * i + j].reshape(8 * cap, kw)
            use(2 * i + j, lambda at, u=u, slot=slot: jnp.dot(u, wb[slot, :, at], preferred_element_type=F32))

    def slabs(w):
        return [slice(i, min(i + w, 2 * f)) for i in range(0, 2 * f, w)]

    def start_acc(i, _):
        def use(e, part):
            for at in slabs(SLAB):
                acc[e, :, at] = part(at)
        products(0, i, use)
        return 0

    corner(0)
    arrived(0)
    gather(0)
    lax.fori_loop(0, el // 8, start_acc, 0)
    relay(1)
    direct(2)
    lax.fori_loop(el // 8, el // 2 - el // 8, start_acc, 0)
    corner(1)
    lax.fori_loop(el // 2 - el // 8, el // 2, start_acc, 0)

    def more(k, _):
        arrived(k)
        gather(k)

        def add(i, _):
            def use(e, part):
                for at in slabs(SLAB):
                    acc[e, :, at] += part(at)
            products(k, i, use)
            return 0

        lax.fori_loop(0, el // 8, add, 0)
        relay(k + 1)

        @pl.when(k < NK - 2)
        def _():
            direct(k + 2)
        lax.fori_loop(el // 8, el // 2 - el // 8, add, 0)
        corner(k + 1)
        lax.fori_loop(el // 2 - el // 8, el // 2, add, 0)
        return 0

    lax.fori_loop(1, NK - 1, more, 0)

    arrived(NK - 1)
    gather(NK - 1)
    for hf in range(2):
        pltpu.make_async_copy(hst.at[hf, 0:t], sh_ref.at[hf], osem.at[hf]).wait()

    def last(i, _):
        @pl.when(i >= 1)
        def _():
            for j in range(2):
                pltpu.make_async_copy(hst.at[j], h_ref.at[2 * i - 2 + j], osem.at[j]).wait()

        def use(e, part):
            slot = lax.rem(e, 2)
            nt = f // 128
            live = {}
            order = [nt // 2] + [v for i in range(nt // 2) for v in (i, nt // 2 + 1 + i)]
            for i in order:
                at = slice(i * 256, i * 256 + 256)
                d = acc[e, :, at] + part(at)
                for j in (2 * i, 2 * i + 1):
                    live[j] = d[:, (j - 2 * i) * 128:(j - 2 * i) * 128 + 128]
                    if j == nt - 1:
                        acc[e, :, j * 128:j * 128 + 128] = live.pop(j)
                for j in [v for v in live if v < nt and v + nt in live]:
                    hst[slot, :, j * 128:j * 128 + 128] = silu_mul(live.pop(j), live.pop(j + nt))
                if 2 * nt - 1 in live:
                    j = nt - 1
                    hst[slot, :, j * 128:j * 128 + 128] = silu_mul(acc[e, :, j * 128:j * 128 + 128], live.pop(2 * nt - 1))
            pltpu.make_async_copy(hst.at[slot], h_ref.at[e], osem.at[slot]).start()
        products(NK - 1, i, use)
        return 0

    lax.fori_loop(0, el // 2, last, 0)

    keep.wait()
    for e in (el - 2, el - 1):
        pltpu.make_async_copy(hst.at[e % 2], h_ref.at[e], osem.at[e % 2]).wait()
    for o in others:
        mcopy(o).wait_send()
    for k in range(NK):
        sent(k)


def second(el, cap, h_ref, sh_ref, meta_ref, x_ref, w2_ref, ws2_ref, y_ref,
           hv, shv, wcv, meta, xv, wb, wd, o3, part, give, pr, sb, rv, res, yst,
           hsem, csem, xsem, wsem, dsem, ysem, psend, precv, ssem, rsem, esend, erecv):
    ey, ex, ec, dev, chip = place()
    t, hd = x_ref.shape
    nc = hd // CW
    f = w2_ref.shape[1]
    half = t // 2
    lo, hi = pl.ds(0, half), pl.ds(half, half)
    per = el
    nb = nc * per
    assert NW == el
    f = w2_ref.shape[1]
    n = el * cap

    def block(b, go):
        c, j = b // per, lax.rem(b, per)
        cols = pl.ds(pl.multiple_of(c * CW, CW), CW)
        slot = lax.rem(b, NW)

        @pl.when(b < nb)
        def _():
            go(pltpu.make_async_copy(w2_ref.at[j, :, cols], wb.at[slot], wsem.at[slot]))

    def down(c):
        cols = pl.ds(pl.multiple_of(c * CW, CW), CW)
        return pltpu.make_async_copy(ws2_ref.at[:, cols], wd.at[lax.rem(c, 2)], dsem.at[lax.rem(c, 2)])

    def fetch(b):
        block(b, lambda c: c.start())

    def ready(b):
        block(b, lambda c: c.wait())

    def hcopy(e):
        return pltpu.make_async_copy(h_ref.at[e], hv.at[e], hsem.at[e])

    m = pltpu.make_async_copy(meta_ref, meta, csem)
    m.start()
    for e in range(el):
        hcopy(e).start()
        fetch(e)
    loads = [pltpu.make_async_copy(sh_ref, shv, xsem.at[0]), pltpu.make_async_copy(x_ref, xv, xsem.at[1]),
             ]

    barrier = pltpu.get_barrier_semaphore()
    for to in "xyp":
        pl.semaphore_signal(barrier, inc=1, device_id=dev[to], device_id_type=MESH)

    m.wait()
    slots = lax.broadcasted_iota(jnp.int32, (cap, t), 0).astype(F32)

    def build(s, _):
        parts = [jnp.where(meta[s, e:e + 1, :] == slots, meta[s, el + e:el + e + 1, :], 0.0) for e in range(el)]
        w = jnp.concatenate(parts, axis=0).T
        for i in range(3):
            p = w.astype(BF)
            wcv[s, :, i * n:(i + 1) * n] = p
            w = w - p.astype(F32)
        return 0

    lax.fori_loop(0, 8, build, 0)

    pl.semaphore_wait(barrier, 3)

    def swap(c, i):
        ch = chip["dxyo"[i]]
        return pltpu.make_async_remote_copy(give.at[lax.rem(c, 2), ch], pr.at[c, ch], psend.at[c, i], precv.at[c, i],
                                            device_id=dev["p"], device_id_type=MESH)

    def ship(c, i, a, b, k=None):
        send, recv = (ssem.at[c, i], rsem.at[c, i]) if k is None else (esend.at[k, i], erecv.at[k, i])
        at = pl.ds(a, b - a)
        return pltpu.make_async_remote_copy(sb.at[i, c, at], rv.at[i, c, at], send, recv, device_id=dev["xy"[i]],
                                            device_id_type=MESH)

    def dispatch(c, op):
        for i in range(2):
            pl.when(c < 2)(lambda: op(ship(c, i, 0, 2)))
            pl.when((c >= 2) & (c < nc - 1))(lambda: op(ship(c, i, 0, 3)))
            pl.when(c == nc - 1)(lambda: op(ship(c, i, 0, 1)))

    def weigh(c, ch, core):
        s = core * 4 + chip[ch]
        return jnp.dot(wcv[s], o3[s], preferred_element_type=F32)

    def compute(c):
        def expert(i, _):
            for e in (2 * i, 2 * i + 1):
                @pl.when(c == 0)
                def _():
                    hcopy(e).wait()
                ready(c * per + e)
            for e in (2 * i, 2 * i + 1):
                o = jnp.dot(hv[e], wb[lax.rem(c * per + e, NW)], preferred_element_type=F32).astype(BF)
                for s in range(8):
                    for j in range(3):
                        o3[s, pl.ds(pl.multiple_of(j * n + e * cap, 16), cap), :] = o[s * cap:(s + 1) * cap]
            for e in (2 * i, 2 * i + 1):
                fetch(c * per + e + NW)
            return 0

        lax.fori_loop(0, el // 2, expert, 0)

        @pl.when(c == 1)
        def _():
            for d in loads + [down(0), down(1)]:
                d.start()

        @pl.when(c >= 2)
        def _():
            for i in range(4):
                swap(c - 2, i).wait_send()
        for i, ch in enumerate("dxyo"):
            give[lax.rem(c, 2), chip[ch]] = weigh(c, ch, 1 - ec)
            swap(c, i).start()
        for ch in "dxyo":
            part[c, chip[ch]] = weigh(c, ch, ec)

    def shared(c):
        down(c).wait()
        p = [jnp.dot(shv[i], wd[lax.rem(c, 2), i * f:(i + 1) * f], preferred_element_type=F32) for i in range(2)]
        cols = pl.ds(pl.multiple_of(c * CW, CW), CW)
        res[c] = xv[:, cols].astype(F32) + (p[0] + p[1]).astype(BF).astype(F32)
        pl.when(c + 2 < nc)(lambda: down(c + 2).start())

    def stage1(c):
        d, x, y = (chip[ch] for ch in "dxy")
        swap(c, 0).wait_recv()
        sb[0, c, 0] = part[c, d, 0:half] + pr[c, d, 0:half]
        sb[1, c, 0] = part[c, d, half:t] + pr[c, d, half:t]
        swap(c, 1).wait_recv()
        sb[0, c, 1] = part[c, x, 0:half] + pr[c, x, 0:half]
        part[c, x, half:t] += pr[c, x, half:t]
        swap(c, 2).wait_recv()
        part[c, y, 0:half] += pr[c, y, 0:half]
        sb[1, c, 1] = part[c, y, half:t] + pr[c, y, half:t]

    def stage2(c, into):
        sb[1, into, 2] = part[c, chip["y"], 0:half] + rv[0, c, 0]
        sb[0, into, 2] = part[c, chip["x"], half:t] + rv[1, c, 0]

    def ycopy(c):
        cols = pl.ds(pl.multiple_of(c * CW, CW), CW)
        return pltpu.make_async_copy(yst.at[lax.rem(c, 2)], y_ref.at[:, cols], ysem.at[lax.rem(c, 2)])

    def stage3(c):
        n2 = lax.rem(c + 2, nc)

        @pl.when(c >= 2)
        def _():
            ycopy(c - 2).wait()
        swap(c, 3).wait_recv()
        own = res[c] + (part[c, chip["o"]] + pr[c, chip["o"]])
        yst[lax.rem(c, 2), 0:half] = (own[0:half] + rv[0, c, 1] + rv[1, n2, 2]).astype(BF)
        yst[lax.rem(c, 2), half:t] = (own[half:t] + rv[0, n2, 2] + rv[1, c, 1]).astype(BF)
        ycopy(c).start()

    def step(c, _):
        compute(c)

        @pl.when(c >= 2)
        def _():
            dispatch(c - 2, lambda d: d.wait_recv())
            stage2(c - 2, c)
        stage1(c)
        dispatch(c, lambda d: d.start())

        @pl.when(c == nc - 1)
        def _():
            for i in range(2):
                ship(nc - 1, i, 1, 3, 0).start()
        @pl.when(c == 2)
        def _():
            for d in loads:
                d.wait()

        @pl.when(c >= 2)
        def _():
            shared(c - 2)

        @pl.when(c >= 4)
        def _():
            stage3(c - 4)
        return 0

    lax.fori_loop(0, nc, step, 0)
    lax.fori_loop(nc - 2, nc, lambda c, v: (shared(c), v)[1], 0)
    for i in range(2):
        ship(nc - 2, i, 0, 3).wait_recv()
    stage2(nc - 2, 0)
    for i in range(2):
        ship(0, i, 2, 3, 1).start()
    stage3(nc - 4)
    for i in range(2):
        ship(nc - 1, i, 0, 1).wait_recv()
    stage2(nc - 1, 1)
    for i in range(2):
        ship(1, i, 2, 3, 2).start()
    for i in range(2):
        ship(nc - 1, i, 1, 3, 0).wait_recv()
    stage3(nc - 3)
    for k in range(2):
        for i in range(2):
            ship(k, i, 2, 3, k + 1).wait_recv()
        stage3(nc - 2 + k)
    for c in (nc - 2, nc - 1):
        ycopy(c).wait()
        for i in range(4):
            swap(c, i).wait_send()
    for i in range(2):
        ship(nc - 1, i, 1, 3, 0).wait_send()
        for k in range(2):
            ship(k, i, 2, 3, k + 1).wait_send()

    def drain(c, _):
        dispatch(c, lambda d: d.wait_send())
        return 0

    lax.fori_loop(0, nc, drain, 0)


def solution(mesh):
    pg = mesh.shape["ey"] * mesh.shape["ex"] * mesh.shape["ec"]

    def local(x, ids, gates, w1, w3, w2, ws1, ws3, ws2):
        t, hd = x.shape
        top = ids.shape[1]
        el, _, f = w1.shape
        ne = el * pg
        cap = min(t, 2 * ((t * top + ne - 1) // ne))
        n = el * cap
        kw = hd // NK
        nc = hd // CW
        dma = pltpu.SemaphoreType.DMA
        h, sh, meta = pl.pallas_call(
            functools.partial(first, el, cap),
            out_shape=(jax.ShapeDtypeStruct((el, pg * cap, f), BF), jax.ShapeDtypeStruct((2, t, f), BF),
                       jax.ShapeDtypeStruct((pg, 2 * el, t), F32)),
            in_specs=[VM, VM] + [ANY] * 5, out_specs=(ANY,) * 3,
            scratch_shapes=[
                pltpu.VMEM((NK, pg, t, kw), BF), pltpu.VMEM((el, pg * cap, 2 * f), F32), pltpu.VMEM((NS, kw, 2 * f), BF),
                pltpu.VMEM((pg, n, t), BF), pltpu.VMEM((el, pg, cap, kw), BF), pltpu.VMEM((2, pg * cap, f), BF),
                pltpu.VMEM((pg, 2 * el, t), F32), pltpu.VMEM((pg, 2 * el, t), F32),
                dma((NK,)), dma((NS, 2)), dma((2,)), dma, dma((8,)), dma((8,)), dma((NK, 11)), dma((NK, 11))],
            compiler_params=pltpu.CompilerParams(collective_id=0, has_side_effects=True, vmem_limit_bytes=VLIM),
        )(ids.T, gates.T, x, w1, w3, ws1, ws3)
        return pl.pallas_call(
            functools.partial(second, el, cap),
            out_shape=jax.ShapeDtypeStruct((t, hd), BF),
            in_specs=[ANY] * 6, out_specs=ANY,
            scratch_shapes=[
                pltpu.VMEM((el, pg * cap, f), BF), pltpu.VMEM((2, t, f), BF), pltpu.VMEM((pg, t, 3 * n), BF), pltpu.VMEM((pg, 2 * el, t), F32),
                pltpu.VMEM((t, hd), BF), pltpu.VMEM((NW, f, CW), BF), pltpu.VMEM((2, 2 * f, CW), BF), pltpu.VMEM((pg, 3 * n, CW), BF),
                pltpu.VMEM((nc, 4, t, CW), F32), pltpu.VMEM((2, 4, t, CW), F32), pltpu.VMEM((nc, 4, t, CW), F32),
                pltpu.VMEM((2, nc, 3, t // 2, CW), F32), pltpu.VMEM((2, nc, 3, t // 2, CW), F32),
                pltpu.VMEM((nc, t, CW), F32), pltpu.VMEM((2, t, CW), BF),
                dma((el,)), dma, dma((2,)), dma((NW,)), dma((2,)), dma((2,)), dma((nc, 4)), dma((nc, 4)), dma((nc, 2)), dma((nc, 2)),
                dma((3, 2)), dma((3, 2))],
            compiler_params=pltpu.CompilerParams(collective_id=1, has_side_effects=True, vmem_limit_bytes=VLIM),
        )(h, sh, meta, x, w2, ws2)

    return jax.shard_map(local, mesh=mesh,
                         in_specs=(P(ALL), P(ALL), P(ALL), P(EXP), P(EXP), P(EXP), P(), P(), P()),
                         out_specs=P(ALL), check_vma=False)
```
